128 devices in a mesh: gx: 8 (over x, core), gy: 16 (over y, z).
Axes of the slice: x: 4, y: 4, z: 4, core: 2. Of those that a mesh axis runs over, the one named last changes fastest.
Arguments:
- residual: float32 [2, 2097152], P(None, ('gx', 'gy')), may hold values from -15 to 15
- cam_jacobian: float32 [2, 9, 2097152], P(None, None, ('gx', 'gy')), may hold values from -0.3 to 0.3
- point_jacobian: float32 [2, 3, 2097152], P(None, None, ('gx', 'gy')), may hold values from -1.5 to 1.5
- obs_camera: int32 [2097152], P(('gx', 'gy')), may hold values from 0 to 16383
- obs_slot: int32 [2097152], P(('gx', 'gy')), may hold values from 0 to 127, as said below
- tile_offset: int32 [4096], P(('gx', 'gy')), may hold values from 0 to 1920, as said below
- damping: float32 [262144], P(('gx', 'gy')), may hold values from 0.3 to 3
- camera_slot: int32 [16384], replicated, may hold values from 0 to 16383, as said below
Outputs:
- reduced: float32 [9, 16384], P(None, ('gx', 'gy'))
- cost: float32 [], replicated
- grad_norm: float32 [], replicated
The draws below stay inside these ranges and needn't reach their ends.
Inputs may be any that keep to these rules, and one draw needn't show every extreme that they name: `obs_slot`: on each device observations are ordered by point; every observation's point lies in its tile's window of 128 points starting at tile_offset. `tile_offset`: windows lie within the device's 2048 points and do not fall from tile to tile. `camera_slot`: each position of the owners' layout is taken by exactly one camera.
All inputs are finite; a program needn't handle non-finite values.
Results may differ from the reference program's by a relative error of at most 0.000096.
Values sent between devices are 32-bit elements; how exact they have to be, the bound alone decides.
A program may use at most 64 MiB of HBM per device.

```python
import math
import jax
import jax.numpy as jnp
from jax import lax

OBS_DEV = 16384
TILE = 512
PW = 128
PTS_DEV = 2048
OBS = 2097152
PTS = 262144
CAMS = 16384


def layout_draw(key):
    local_key = jax.random.fold_in(key, 11)
    position_all = jnp.arange(OBS, dtype=jnp.int32)
    local_pos = position_all % OBS_DEV
    jitter = jax.random.randint(local_key, (OBS,), 0, 3, dtype=jnp.int32)
    point_index = jnp.minimum(local_pos * PTS_DEV // OBS_DEV + jitter, PTS_DEV - 1)
    point_index = lax.cummax(point_index.reshape(OBS // OBS_DEV, OBS_DEV), axis=1)
    tiled = point_index.reshape(-1, TILE)
    offsets = jnp.clip(tiled[:, -1] - (PW - 1), 0, PTS_DEV - PW).astype(jnp.int32)
    slot_values = (tiled - offsets[:, None]).astype(jnp.int32)
    return (slot_values.reshape(-1), offsets)


def camera_draw(key):
    base_key = jax.random.fold_in(key, 37)
    keys = jax.random.split(base_key, 3)
    perm = jax.random.permutation(keys[0], CAMS).astype(jnp.int32)
    inverse = jnp.zeros((CAMS,), jnp.int32).at[perm].set(jnp.arange(CAMS, dtype=jnp.int32))
    first = jax.random.randint(keys[1], (OBS,), 0, CAMS, dtype=jnp.int32)
    second = jax.random.randint(keys[2], (OBS,), 0, CAMS, dtype=jnp.int32)
    chosen = jnp.maximum(first, second)
    return (inverse[chosen].astype(jnp.int32), perm)


def draw_obs_camera(key, part):
    return camera_draw(key)[0]


def draw_camera_slot(key, part):
    return camera_draw(key)[1]


def draw_obs_slot(key, part):
    return layout_draw(key)[0]


def draw_tile_offset(key, part):
    return layout_draw(key)[1]


def draw_residual(key, part):
    keys = jax.random.split(jax.random.fold_in(key, 23), 2)
    spread = jnp.exp(jax.random.uniform(keys[1], (OBS,), jnp.float32) * math.log(10.0))
    device_pos = (jnp.arange(OBS, dtype=jnp.int32) // OBS_DEV).astype(jnp.float32)
    device_scale = 1.0 + 2.0 * device_pos / max(OBS // OBS_DEV - 1, 1)
    base = jax.random.truncated_normal(keys[0], -4.0, 4.0, (2, OBS), jnp.float32)
    return (base * (spread * device_scale / 8.0)[None, :]).astype(jnp.float32)


def levels(own_key, shape, shards, least, high):
    loudness = 1.0
    for dim, parts in shards:
        draws = jax.random.uniform(jax.random.fold_in(jax.random.fold_in(own_key, 6), dim), (parts,), jnp.float32, least / len(shards), high / len(shards))
        loudness = loudness * jnp.repeat(jnp.exp(draws), shape[dim] // parts).reshape((-1,) + (1,) * (len(shape) - 1 - dim))
    return loudness


def noise(own_key, shape, scale, bound, cuts=(), kind=jnp.bfloat16):
    factor_of = levels(own_key, shape, cuts, -0.22, 0.18) if cuts else 1.0
    values = jax.random.normal(own_key, shape, jnp.float32) * scale * factor_of
    return jnp.minimum(jnp.maximum(values, -bound), bound).astype(kind)


def setup_inputs(seed: int = 0) -> dict:
    key_list = jax.random.split(jax.random.key(seed), 9)
    residual = draw_residual(jax.random.fold_in(key_list[8], 71), 0)
    cam_jacobian = noise(key_list[1], (2, 9, OBS), 0.05, 0.3, ((2, 128),), jnp.float32)
    point_jacobian = noise(key_list[2], (2, 3, OBS), 0.25, 1.5, ((2, 128),), jnp.float32)
    obs_camera = draw_obs_camera(jax.random.fold_in(key_list[8], 71), 0)
    obs_slot = draw_obs_slot(jax.random.fold_in(key_list[8], 71), 0)
    tile_offset = draw_tile_offset(jax.random.fold_in(key_list[8], 71), 0)
    damping = jnp.clip(jnp.exp(math.log(3.0) - 2.3025851 * jax.random.uniform(key_list[6], (PTS,), jnp.float32) ** levels(key_list[6], (PTS,), ((0, 128),), -0.2, 0.2)), 0.3, 3.0)
    camera_slot = draw_camera_slot(jax.random.fold_in(key_list[8], 71), 0)
    return {"residual": residual, "cam_jacobian": cam_jacobian, "point_jacobian": point_jacobian, "obs_camera": obs_camera, "obs_slot": obs_slot, "tile_offset": tile_offset, "damping": damping, "camera_slot": camera_slot}


def block_solve(entries, rhs):
    comp_aa = entries[0]
    comp_ab = entries[1]
    comp_ac = entries[2]
    comp_bb = entries[3]
    comp_bc = entries[4]
    comp_cc = entries[5]
    cof_aa = comp_bb * comp_cc - comp_bc * comp_bc
    cof_ab = comp_ac * comp_bc - comp_ab * comp_cc
    cof_ac = comp_ab * comp_bc - comp_ac * comp_bb
    cof_bb = comp_aa * comp_cc - comp_ac * comp_ac
    cof_bc = comp_ab * comp_ac - comp_aa * comp_bc
    cof_cc = comp_aa * comp_bb - comp_ab * comp_ab
    determ = comp_aa * cof_aa + comp_ab * cof_ab + comp_ac * cof_ac
    first = (cof_aa * rhs[0] + cof_ab * rhs[1] + cof_ac * rhs[2]) / determ
    second = (cof_ab * rhs[0] + cof_bb * rhs[1] + cof_bc * rhs[2]) / determ
    third = (cof_ac * rhs[0] + cof_bc * rhs[1] + cof_cc * rhs[2]) / determ
    return jnp.stack([first, second, third])

def point_features(residual, point_jacobian):
    grad_obs = lax.optimization_barrier(jnp.sum(point_jacobian * residual[:, None, :], axis=0))
    pairs = [(0, 0), (0, 1), (0, 2), (1, 1), (1, 2), (2, 2)]
    products = [lax.optimization_barrier(jnp.sum(point_jacobian[:, left] * point_jacobian[:, right], axis=0)) for left, right in pairs]
    return jnp.concatenate([grad_obs, jnp.stack(products)], axis=0)

def reference(residual, cam_jacobian, point_jacobian, obs_camera, obs_slot, tile_offset, damping, camera_slot):
    position_all = jnp.arange(OBS, dtype=jnp.int32)
    device_of = position_all // OBS_DEV
    point_of = (device_of * PTS_DEV + tile_offset[position_all // TILE] + obs_slot).astype(jnp.int32)
    features = point_features(residual, point_jacobian)
    point_sums = jax.ops.segment_sum(features.T, point_of, num_segments=PTS).T
    point_grad = point_sums[:3]
    diag_mask = jnp.array([1.0, 0.0, 0.0, 1.0, 0.0, 1.0], jnp.float32)[:, None]
    entries = point_sums[3:] + diag_mask * damping[None, :]
    step_point = block_solve(entries, point_grad)
    step_obs = jnp.take(step_point, point_of, axis=1)
    moved = lax.optimization_barrier(jnp.sum(point_jacobian * step_obs[None, :, :], axis=1))
    position = camera_slot[obs_camera].astype(jnp.int32)
    grad_obs = lax.optimization_barrier(jnp.sum(cam_jacobian * residual[:, None, :], axis=0))
    coupling_obs = lax.optimization_barrier(jnp.sum(cam_jacobian * moved[:, None, :], axis=0))
    camera_grad = jax.ops.segment_sum(grad_obs.T, position, num_segments=CAMS).T
    coupling = jax.ops.segment_sum(coupling_obs.T, position, num_segments=CAMS).T
    reduced = coupling - camera_grad
    cost = jnp.sum(residual * residual) / (2.0 * OBS)
    total = jnp.sum(camera_grad * camera_grad) + jnp.sum(point_grad * point_grad)
    grad_norm = jnp.sqrt(total / (9.0 * CAMS + 3.0 * PTS) + 1e-06)
    return (reduced, cost, grad_norm)
```

```python
import functools

import jax
import jax.numpy as jnp
from jax import lax
from jax.experimental import pallas as pl
from jax.experimental.pallas import tpu as pltpu
from jax.sharding import Mesh
from jax.sharding import PartitionSpec as P

F32, BF16, I32 = jnp.float32, jnp.bfloat16, jnp.int32
NT = (((1,), (1,)), ((), ()))
LANES = 128
TILE = 512
CHUNK = 512


def halves(value):
    high = value.astype(BF16)
    return high, (value - high.astype(F32)).astype(BF16)


def thirds(value):
    high = value.astype(BF16)
    rest = value - high.astype(F32)
    middle = rest.astype(BF16)
    return high, middle, (rest - middle.astype(F32)).astype(BF16)


def row_of(ref, start, count):
    return jnp.concatenate([ref[pl.ds(start + k, 1), :] for k in range(count)], axis=1)


def local_kernel(
    offset_ref,
    res_ref,
    cam_ref,
    pt_ref,
    camera_ref,
    slot_ref,
    damp_ref,
    table_ref,
    out_ref,
    sums_ref,
    pos_ref,
    feat_ref,
    point_ref,
    step_ref,
    moved_ref,
    lhs_ref,
):
    n_obs = res_ref.shape[1]
    points = damp_ref.shape[0] * LANES
    tiles = n_obs // TILE

    camera = camera_ref[...]
    high_part, low_part = camera >> 7, camera & 127

    def look_up(k, found):
        line = jnp.broadcast_to(table_ref[pl.ds(k, 1), :], found.shape)
        return jnp.where(high_part == k, jnp.take_along_axis(line, low_part, axis=1), found)

    pos_ref[...] = lax.fori_loop(0, table_ref.shape[0], look_up, jnp.zeros_like(camera), unroll=4)

    point_ref[...] = jnp.zeros_like(point_ref)
    feat_ref[...] = jnp.zeros_like(feat_ref)
    window = lax.broadcasted_iota(I32, (2 * LANES, TILE), 0)

    def tile_onehot(t):
        offset = offset_ref[t]
        index = row_of(slot_ref, t * (TILE // LANES), TILE // LANES) + (offset & 127)
        base = pl.multiple_of((offset >> 7) * LANES, LANES)
        return (window == index).astype(F32).astype(BF16), base

    def add_points(t, _):
        cols = pl.ds(pl.multiple_of(t * TILE, TILE), TILE)
        onehot, base = tile_onehot(t)
        r0, r1 = res_ref[0:1, cols], res_ref[1:2, cols]
        j0, j1 = pt_ref[0, :, cols], pt_ref[1, :, cols]
        feat_ref[0:3, :] = j0 * r0 + j1 * r1
        feat_ref[3:6, :] = j0[0:1] * j0 + j1[0:1] * j1
        feat_ref[6:8, :] = j0[1:2] * j0[1:3] + j1[1:2] * j1[1:3]
        feat_ref[8:9, :] = j0[2:3] * j0[2:3] + j1[2:3] * j1[2:3]
        lhs = jnp.concatenate(thirds(feat_ref[...]), axis=0)
        dots = lax.dot_general(lhs, onehot, NT, preferred_element_type=F32)
        point_ref[:, pl.ds(base, 2 * LANES)] += (dots[32:48] + dots[16:32]) + dots[0:16]
        return 0

    lax.fori_loop(0, tiles, add_points, 0)

    damping = row_of(damp_ref, 0, points // LANES)
    g = [point_ref[k : k + 1, 0:points] for k in range(3)]
    aa, ab, ac, bb, bc, cc = [point_ref[k : k + 1, 0:points] for k in range(3, 9)]
    aa, bb, cc = aa + damping, bb + damping, cc + damping
    cof_aa = bb * cc - bc * bc
    cof_ab = ac * bc - ab * cc
    cof_ac = ab * bc - ac * bb
    cof_bb = aa * cc - ac * ac
    cof_bc = ab * ac - aa * bc
    cof_cc = aa * bb - ab * ab
    determ = aa * cof_aa + ab * cof_ab + ac * cof_ac
    steps = (
        (cof_aa * g[0] + cof_ab * g[1] + cof_ac * g[2]) / determ,
        (cof_ab * g[0] + cof_bb * g[1] + cof_bc * g[2]) / determ,
        (cof_ac * g[0] + cof_bc * g[1] + cof_cc * g[2]) / determ,
    )
    step_ref[...] = jnp.zeros_like(step_ref)
    for k in range(3):
        step_ref[k : k + 1, 0:points] = steps[k]
    point_square = jnp.sum(g[0] * g[0] + g[1] * g[1] + g[2] * g[2])
    residual = res_ref[...]
    cost = jnp.sum(residual * residual)
    lane = lax.broadcasted_iota(I32, sums_ref.shape, 1)
    sums_ref[...] = jnp.where(lane == 0, cost, jnp.where(lane == 1, point_square, 0.0))

    def take_steps(t, _):
        cols = pl.ds(pl.multiple_of(t * TILE, TILE), TILE)
        onehot, base = tile_onehot(t)
        lhs = jnp.concatenate(thirds(step_ref[:, pl.ds(base, 2 * LANES)]), axis=0)
        dots = jnp.dot(lhs, onehot, preferred_element_type=F32)
        step = (dots[16:24] + dots[8:16]) + dots[0:8]
        for a in range(2):
            jac = pt_ref[a, :, cols]
            moved_ref[a : a + 1, cols] = (
                jac[0:1] * step[0:1] + jac[1:2] * step[1:2] + jac[2:3] * step[2:3]
            )
        return 0

    lax.fori_loop(0, tiles, take_steps, 0)

    out_ref[...] = jnp.zeros_like(out_ref)
    hi_iota = lax.broadcasted_iota(I32, (64, CHUNK), 0)
    lo_iota = lax.broadcasted_iota(I32, (256, CHUNK), 0)

    def add_cameras(c, _):
        cols = pl.ds(pl.multiple_of(c * CHUNK, CHUNK), CHUNK)
        pos = row_of(pos_ref, c * (CHUNK // LANES), CHUNK // LANES)
        owner = pos >> 7
        hi = ((owner >> 5) << 4) + (owner & 15)
        lo = (((owner >> 4) & 1) << 7) + (pos & 127)
        hi_hot = (hi_iota == hi).astype(F32).astype(BF16)
        lo_hot = (lo_iota == lo).astype(F32).astype(BF16)
        c0, c1 = cam_ref[0, :, cols], cam_ref[1, :, cols]
        r0, r1 = res_ref[0:1, cols], res_ref[1:2, cols]
        m0, m1 = moved_ref[0:1, cols] - r0, moved_ref[1:2, cols] - r1
        for b, value in enumerate((c0 * r0 + c1 * r1, c0 * m0 + c1 * m1)):
            for p, part in enumerate(halves(value)):
                part = part.astype(F32)
                for m in range(9):
                    line = jnp.broadcast_to(part[m : m + 1], (64, CHUNK)).astype(BF16)
                    row = (b * 9 + m) * 64
                    lhs_ref[row : row + 64, p * CHUNK : (p + 1) * CHUNK] = line * hi_hot
        rhs = jnp.concatenate([lo_hot, lo_hot], axis=1)
        out_ref[...] += lax.dot_general(lhs_ref[...], rhs, NT, preferred_element_type=F32)
        return 0

    lax.fori_loop(0, n_obs // CHUNK, add_cameras, 0)


def local_sums(residual, cam_jacobian, point_jacobian, obs_camera, obs_slot, tile_offset, damping, camera_slot):
    n_obs = residual.shape[1]
    vmem = pl.BlockSpec(memory_space=pltpu.VMEM)
    grid_rows = lambda x: x.reshape(-1, LANES)
    points = damping.shape[0]
    return pl.pallas_call(
        local_kernel,
        out_shape=(
            jax.ShapeDtypeStruct((18 * 64, 256), F32),
            jax.ShapeDtypeStruct((8, LANES), F32),
        ),
        in_specs=[pl.BlockSpec(memory_space=pltpu.SMEM)] + [vmem] * 7,
        out_specs=(vmem, vmem),
        scratch_shapes=[
            pltpu.VMEM((n_obs // LANES, LANES), I32),
            pltpu.VMEM((16, TILE), F32),
            pltpu.VMEM((16, points + LANES), F32),
            pltpu.VMEM((8, points + LANES), F32),
            pltpu.VMEM((2, n_obs), F32),
            pltpu.VMEM((18 * 64, 2 * CHUNK), BF16),
        ],
    )(
        tile_offset,
        residual,
        cam_jacobian,
        point_jacobian,
        grid_rows(obs_camera),
        grid_rows(obs_slot),
        grid_rows(damping),
        grid_rows(camera_slot),
    )


GX_GY = ("gx_0", "gx_1", "gy_0", "gy_1")


def on_device(
    residual, cam_jacobian, point_jacobian, obs_camera, obs_slot, tile_offset, damping, camera_slot
):
    n_obs = residual.shape[1]
    devices = lax.axis_size(GX_GY)
    partial, sums = local_sums(
        residual, cam_jacobian, point_jacobian, obs_camera, obs_slot, tile_offset, damping, camera_slot
    )
    tiles = partial.reshape(18, 4, 16, 2, LANES)
    tiles = jnp.transpose(tiles, (1, 3, 2, 0, 4)).reshape(8, 4, 4, 18, LANES)
    own = lax.psum_scatter(tiles, ("gx_0", "gx_1"), scatter_dimension=0, tiled=False)
    own = lax.psum_scatter(own, "gy_0", scatter_dimension=0, tiled=False)
    own = lax.psum_scatter(own, "gy_1", scatter_dimension=0, tiled=False)
    grad_share, reduced = own[:9], own[9:]
    scalars = jnp.stack([sums[0, 0], sums[0, 1] + jnp.sum(grad_share * grad_share)])
    scalars = lax.psum(scalars, GX_GY)
    cost = scalars[0] / (2.0 * n_obs * devices)
    grad_norm = jnp.sqrt(
        scalars[1] / (9.0 * camera_slot.shape[0] + 3.0 * damping.shape[0] * devices) + 1e-06
    )
    return (reduced, cost, grad_norm)


def solution(mesh):
    finer = Mesh(mesh.devices.reshape(4, 2, 4, 4), GX_GY)
    in_specs = (
        P(None, GX_GY),
        P(None, None, GX_GY),
        P(None, None, GX_GY),
        P(GX_GY),
        P(GX_GY),
        P(GX_GY),
        P(GX_GY),
        P(),
    )
    out_specs = (P(None, GX_GY), P(), P())
    return jax.shard_map(
        on_device, mesh=finer, in_specs=in_specs, out_specs=out_specs, check_vma=False
    )
```

```python
import functools

import jax
import jax.numpy as jnp
from jax import lax
from jax.experimental import pallas as pl
from jax.experimental.pallas import tpu as pltpu
from jax.sharding import Mesh
from jax.sharding import PartitionSpec as P

F32, BF16, I32 = jnp.float32, jnp.bfloat16, jnp.int32
NT = (((1,), (1,)), ((), ()))
MESH = pl.DeviceIdType.MESH
LANES = 128
TILE = 512
CHUNK = 512


def halves(value):
    high = value.astype(BF16)
    return high, (value - high.astype(F32)).astype(BF16)


def thirds(value):
    high = value.astype(BF16)
    rest = value - high.astype(F32)
    middle = rest.astype(BF16)
    return high, middle, (rest - middle.astype(F32)).astype(BF16)


def row_of(ref, start, count):
    return jnp.concatenate([ref[pl.ds(start + k, 1), :] for k in range(count)], axis=1)


def local_kernel(
    offset_ref,
    res_ref,
    cam_ref,
    pt_ref,
    camera_ref,
    slot_ref,
    damp_ref,
    table_ref,
    out_ref,
    sums_ref,
    pos_ref,
    feat_ref,
    point_ref,
    step_ref,
    moved_ref,
    lhs_ref,
    total_ref,
):
    n_obs = res_ref.shape[1]
    points = damp_ref.shape[0] * LANES
    tiles = n_obs // TILE

    camera = camera_ref[...]
    high_part, low_part = camera >> 7, camera & 127

    def look_up(k, found):
        line = jnp.broadcast_to(table_ref[pl.ds(k, 1), :], found.shape)
        return jnp.where(high_part == k, jnp.take_along_axis(line, low_part, axis=1), found)

    pos_ref[...] = lax.fori_loop(0, table_ref.shape[0], look_up, jnp.zeros_like(camera), unroll=4)

    point_ref[...] = jnp.zeros_like(point_ref)
    feat_ref[...] = jnp.zeros_like(feat_ref)
    window = lax.broadcasted_iota(I32, (2 * LANES, TILE), 0)

    def tile_onehot(t):
        offset = offset_ref[t]
        index = row_of(slot_ref, t * (TILE // LANES), TILE // LANES) + (offset & 127)
        base = pl.multiple_of((offset >> 7) * LANES, LANES)
        return (window == index).astype(F32).astype(BF16), base

    def add_points(t, _):
        cols = pl.ds(pl.multiple_of(t * TILE, TILE), TILE)
        onehot, base = tile_onehot(t)
        r0, r1 = res_ref[0:1, cols], res_ref[1:2, cols]
        j0, j1 = pt_ref[0, :, cols], pt_ref[1, :, cols]
        feat_ref[0:3, :] = j0 * r0 + j1 * r1
        feat_ref[3:6, :] = j0[0:1] * j0 + j1[0:1] * j1
        feat_ref[6:8, :] = j0[1:2] * j0[1:3] + j1[1:2] * j1[1:3]
        feat_ref[8:9, :] = j0[2:3] * j0[2:3] + j1[2:3] * j1[2:3]
        lhs = jnp.concatenate(thirds(feat_ref[...]), axis=0)
        dots = lax.dot_general(lhs, onehot, NT, preferred_element_type=F32)
        point_ref[:, pl.ds(base, 2 * LANES)] += (dots[32:48] + dots[16:32]) + dots[0:16]
        return 0

    lax.fori_loop(0, tiles, add_points, 0)

    damping = row_of(damp_ref, 0, points // LANES)
    g = [point_ref[k : k + 1, 0:points] for k in range(3)]
    aa, ab, ac, bb, bc, cc = [point_ref[k : k + 1, 0:points] for k in range(3, 9)]
    aa, bb, cc = aa + damping, bb + damping, cc + damping
    cof_aa = bb * cc - bc * bc
    cof_ab = ac * bc - ab * cc
    cof_ac = ab * bc - ac * bb
    cof_bb = aa * cc - ac * ac
    cof_bc = ab * ac - aa * bc
    cof_cc = aa * bb - ab * ab
    determ = aa * cof_aa + ab * cof_ab + ac * cof_ac
    steps = (
        (cof_aa * g[0] + cof_ab * g[1] + cof_ac * g[2]) / determ,
        (cof_ab * g[0] + cof_bb * g[1] + cof_bc * g[2]) / determ,
        (cof_ac * g[0] + cof_bc * g[1] + cof_cc * g[2]) / determ,
    )
    step_ref[...] = jnp.zeros_like(step_ref)
    for k in range(3):
        step_ref[k : k + 1, 0:points] = steps[k]
    point_square = jnp.sum(g[0] * g[0] + g[1] * g[1] + g[2] * g[2])
    residual = res_ref[...]
    cost = jnp.sum(residual * residual)
    lane = lax.broadcasted_iota(I32, sums_ref.shape, 1)
    sums_ref[...] = jnp.where(lane == 0, cost, jnp.where(lane == 1, point_square, 0.0))

    def take_steps(t, _):
        cols = pl.ds(pl.multiple_of(t * TILE, TILE), TILE)
        onehot, base = tile_onehot(t)
        lhs = jnp.concatenate(thirds(step_ref[:, pl.ds(base, 2 * LANES)]), axis=0)
        dots = jnp.dot(lhs, onehot, preferred_element_type=F32)
        step = (dots[16:24] + dots[8:16]) + dots[0:8]
        for a in range(2):
            jac = pt_ref[a, :, cols]
            moved_ref[a : a + 1, cols] = (
                jac[0:1] * step[0:1] + jac[1:2] * step[1:2] + jac[2:3] * step[2:3]
            )
        return 0

    lax.fori_loop(0, tiles, take_steps, 0)

    total_ref[...] = jnp.zeros_like(total_ref)
    hi_iota = lax.broadcasted_iota(I32, (64, CHUNK), 0)
    lo_iota = lax.broadcasted_iota(I32, (256, CHUNK), 0)

    def add_cameras(c, _):
        cols = pl.ds(pl.multiple_of(c * CHUNK, CHUNK), CHUNK)
        pos = row_of(pos_ref, c * (CHUNK // LANES), CHUNK // LANES)
        owner = pos >> 7
        hi = ((owner >> 5) << 4) + (owner & 15)
        lo = (((owner >> 4) & 1) << 7) + (pos & 127)
        hi_hot = (hi_iota == hi).astype(F32).astype(BF16)
        lo_hot = (lo_iota == lo).astype(F32).astype(BF16)
        c0, c1 = cam_ref[0, :, cols], cam_ref[1, :, cols]
        r0, r1 = res_ref[0:1, cols], res_ref[1:2, cols]
        m0, m1 = moved_ref[0:1, cols] - r0, moved_ref[1:2, cols] - r1
        for b, value in enumerate((c0 * r0 + c1 * r1, c0 * m0 + c1 * m1)):
            for p, part in enumerate(halves(value)):
                part = part.astype(F32)
                for m in range(9):
                    line = jnp.broadcast_to(part[m : m + 1], (64, CHUNK)).astype(BF16)
                    row = (b * 9 + m) * 64
                    lhs_ref[row : row + 64, p * CHUNK : (p + 1) * CHUNK] = line * hi_hot
        rhs = jnp.concatenate([lo_hot, lo_hot], axis=1)
        dots = lax.dot_general(lhs_ref[...], rhs, NT, preferred_element_type=F32)
        total_ref[0] += dots[:, :LANES]
        total_ref[1] += dots[:, LANES:]
        return 0

    lax.fori_loop(0, n_obs // CHUNK, add_cameras, 0)

    def regroup(hi, _):
        for side in range(2):
            for g in range(3):
                rows = pl.ds(g * 6 * 64 + hi, 6, stride=64)
                out_ref[side, g, hi] = total_ref[side, rows, :]
        return 0

    lax.fori_loop(0, 64, regroup, 0, unroll=4)


def local_sums(residual, cam_jacobian, point_jacobian, obs_camera, obs_slot, tile_offset, damping, camera_slot):
    n_obs = residual.shape[1]
    vmem = pl.BlockSpec(memory_space=pltpu.VMEM)
    grid_rows = lambda x: x.reshape(-1, LANES)
    points = damping.shape[0]
    return pl.pallas_call(
        local_kernel,
        out_shape=(
            jax.ShapeDtypeStruct((2, 3, 64, 6, LANES), F32),
            jax.ShapeDtypeStruct((8, LANES), F32),
        ),
        in_specs=[pl.BlockSpec(memory_space=pltpu.SMEM)] + [vmem] * 7,
        out_specs=(vmem, vmem),
        scratch_shapes=[
            pltpu.VMEM((n_obs // LANES, LANES), I32),
            pltpu.VMEM((16, TILE), F32),
            pltpu.VMEM((16, points + LANES), F32),
            pltpu.VMEM((8, points + LANES), F32),
            pltpu.VMEM((2, n_obs), F32),
            pltpu.VMEM((18 * 64, 2 * CHUNK), BF16),
            pltpu.VMEM((2, 18 * 64, LANES), F32),
        ],
    )(
        tile_offset,
        residual,
        cam_jacobian,
        point_jacobian,
        grid_rows(obs_camera),
        grid_rows(obs_slot),
        grid_rows(damping),
        grid_rows(camera_slot),
    )


AXES = ("gx_0", "gx_1", "gy_0", "gy_1")
RINGS = ("gx_0", "gy_0", "gy_1")
ORDERS = ((0, 1, 2), (1, 2, 0), (2, 0, 1))


def neighbours(me, names, sizes):
    total = 1
    for name in names:
        total *= sizes[name]
    place = 0
    for name in names:
        place = place * sizes[name] + me[name]
    found = []
    for k in range(1, total):
        other = lax.rem(place + k, total)
        target = dict(me)
        for name in reversed(names):
            target[name] = lax.rem(other, sizes[name])
            other = other // sizes[name]
        found.append(tuple(target[name] for name in AXES))
    return found


def inside(position, index):
    return (slice(None),) * position + (index,)


def exchange_kernel(
    sizes,
    scale,
    part_ref,
    sums_ref,
    reduced_ref,
    cost_ref,
    norm_ref,
    pair_ref,
    whole_ref,
    in1_ref,
    sum1_ref,
    in2_ref,
    sum2_ref,
    in3_ref,
    mine_ref,
    far_ref,
    plane_ref,
    near_ref,
    pair_send,
    pair_recv,
    ring_send,
    ring_recv,
    far_send,
    far_recv,
    near_send,
    near_recv,
):
    me = {name: lax.axis_index(name) for name in AXES}
    far = neighbours(me, ("gx_0", "gx_1"), sizes)
    near = neighbours(me, ("gy_0", "gy_1"), sizes)
    rings = [neighbours(me, (name,), sizes) for name in RINGS]
    core = me["gx_1"]
    partner = (me["gx_0"], 1 - core, me["gy_0"], me["gy_1"])

    barrier = pltpu.get_barrier_semaphore()
    for target in far + near:
        pl.semaphore_signal(barrier, inc=1, device_id=target, device_id_type=MESH)
    pl.semaphore_wait(barrier, len(far) + len(near))

    started = []

    def send(source, target_ref, send_sem, recv_sem, device):
        copy = pltpu.make_async_remote_copy(
            src_ref=source,
            dst_ref=target_ref,
            send_sem=send_sem,
            recv_sem=recv_sem,
            device_id=device,
            device_id_type=MESH,
        )
        copy.start()
        started.append(copy)
        return copy

    def spread(source, inbox, group, phase, position):
        ring = ORDERS[group][phase]
        name = RINGS[ring]
        copies = []
        for k, device in enumerate(rings[ring]):
            there = device[AXES.index(name)]
            copies.append(
                send(
                    source.at[(group,) + inside(position, there)],
                    inbox.at[group, k],
                    ring_send.at[group, phase, k],
                    ring_recv.at[group, phase, k],
                    device,
                )
            )
        return copies

    def gather(source, inbox, copies, group, phase, position):
        for copy in copies:
            copy.wait_recv()
        here = me[RINGS[ORDERS[group][phase]]]
        kept = source[(group,) + inside(position, here)]
        return (kept + inbox[group, 1]) + (inbox[group, 0] + inbox[group, 2])

    pairs = [
        send(part_ref.at[1 - core, g], pair_ref.at[g], pair_send.at[g], pair_recv.at[g], partner)
        for g in range(3)
    ]
    first, second, third = [], [], []
    for g in range(3):
        pairs[g].wait_recv()
        whole_ref[g] = part_ref[core, g] + pair_ref[g]
        first.append(spread(whole_ref, in1_ref, g, 0, ORDERS[g][0]))
    spots = []
    for g in range(3):
        sum1_ref[g] = gather(whole_ref, in1_ref, first[g], g, 0, ORDERS[g][0])
        left = [d for d in range(3) if d != ORDERS[g][0]]
        spots.append(left.index(ORDERS[g][1]))
        second.append(spread(sum1_ref, in2_ref, g, 1, spots[g]))
    for g in range(3):
        sum2_ref[g] = gather(sum1_ref, in2_ref, second[g], g, 1, spots[g])
        third.append(spread(sum2_ref, in3_ref, g, 2, 0))
    own = [gather(sum2_ref, in3_ref, third[g], g, 2, 0) for g in range(3)]

    rows = jnp.concatenate(own, axis=0)
    half = rows.shape[0] // 2
    reduced_ref[...] = rows[half:]
    camera_square = jnp.sum(rows[:half] * rows[:half])
    lane = lax.broadcasted_iota(I32, mine_ref.shape, 1)
    mine_ref[...] = sums_ref[...] + jnp.where(lane == 1, camera_square, 0.0)
    arrivals = [
        send(mine_ref, far_ref.at[k], far_send.at[k], far_recv.at[k], device)
        for k, device in enumerate(far)
    ]
    for copy in arrivals:
        copy.wait_recv()
    plane_ref[...] = mine_ref[...] + jnp.sum(far_ref[...], axis=0)
    arrivals = [
        send(plane_ref, near_ref.at[k], near_send.at[k], near_recv.at[k], device)
        for k, device in enumerate(near)
    ]
    for copy in arrivals:
        copy.wait_recv()
    totals = plane_ref[...] + jnp.sum(near_ref[...], axis=0)
    first_row = lax.broadcasted_iota(I32, mine_ref.shape, 0) == 0
    cost = totals / scale[0]
    norm = jnp.sqrt(totals / scale[1] + 1e-06)
    cost_ref[0, 0] = jnp.sum(jnp.where(first_row & (lane == 0), cost, 0.0))
    norm_ref[0, 0] = jnp.sum(jnp.where(first_row & (lane == 1), norm, 0.0))
    for copy in started:
        copy.wait_send()


def exchange(partial, sums, sizes, scale):
    rows = partial.shape[-2]
    block = (rows, LANES)
    vmem = pl.BlockSpec(memory_space=pltpu.VMEM)
    smem = pl.BlockSpec(memory_space=pltpu.SMEM)
    buffer = lambda *lead: pltpu.VMEM(lead + block, F32)
    dma = pltpu.SemaphoreType.DMA
    far = sizes["gx_0"] * sizes["gx_1"] - 1
    near = sizes["gy_0"] * sizes["gy_1"] - 1
    return pl.pallas_call(
        functools.partial(exchange_kernel, sizes, scale),
        out_shape=(
            jax.ShapeDtypeStruct((3 * rows // 2, LANES), F32),
            jax.ShapeDtypeStruct((1, 1), F32),
            jax.ShapeDtypeStruct((1, 1), F32),
        ),
        in_specs=[vmem, vmem],
        out_specs=(vmem, smem, smem),
        scratch_shapes=[
            buffer(3, 4, 4, 4),
            buffer(3, 4, 4, 4),
            buffer(3, 3, 4, 4),
            buffer(3, 4, 4),
            buffer(3, 3, 4),
            buffer(3, 4),
            buffer(3, 3),
            pltpu.VMEM((8, LANES), F32),
            pltpu.VMEM((far, 8, LANES), F32),
            pltpu.VMEM((8, LANES), F32),
            pltpu.VMEM((near, 8, LANES), F32),
            dma((3,)),
            dma((3,)),
            dma((3, 3, 3)),
            dma((3, 3, 3)),
            dma((far,)),
            dma((far,)),
            dma((near,)),
            dma((near,)),
        ],
        compiler_params=pltpu.CompilerParams(collective_id=0, has_side_effects=True),
    )(partial, sums)


def on_device(
    residual, cam_jacobian, point_jacobian, obs_camera, obs_slot, tile_offset, damping, camera_slot
):
    n_obs = residual.shape[1]
    sizes = {name: lax.axis_size(name) for name in AXES}
    devices = lax.axis_size(AXES)
    partial, sums = local_sums(
        residual, cam_jacobian, point_jacobian, obs_camera, obs_slot, tile_offset, damping, camera_slot
    )
    partial = partial.reshape(2, 3, 4, 4, 4, 6, LANES)
    scale = (2.0 * n_obs * devices, 9.0 * camera_slot.shape[0] + 3.0 * damping.shape[0] * devices)
    reduced, cost, grad_norm = exchange(partial, sums, sizes, scale)
    return (reduced, cost.reshape(()), grad_norm.reshape(()))


def solution(mesh):
    finer = Mesh(mesh.devices.reshape(4, 2, 4, 4), AXES)
    in_specs = (
        P(None, AXES),
        P(None, None, AXES),
        P(None, None, AXES),
        P(AXES),
        P(AXES),
        P(AXES),
        P(AXES),
        P(),
    )
    out_specs = (P(None, AXES), P(), P())
    return jax.shard_map(
        on_device, mesh=finer, in_specs=in_specs, out_specs=out_specs, check_vma=False
    )
```

```python
import functools

import jax
import jax.numpy as jnp
from jax import lax
from jax.experimental import pallas as pl
from jax.experimental.pallas import tpu as pltpu
from jax.sharding import Mesh
from jax.sharding import PartitionSpec as P

F32, BF16, I32 = jnp.float32, jnp.bfloat16, jnp.int32
NT = (((1,), (1,)), ((), ()))
MESH = pl.DeviceIdType.MESH
LANES = 128
CAM = 9
BINS = 64


def thirds(value):
    high = value.astype(BF16)
    rest = value - high.astype(F32)
    middle = rest.astype(BF16)
    return high, middle, (rest - middle.astype(F32)).astype(BF16)


def row_of(ref, start, count):
    return jnp.concatenate([ref[pl.ds(start + k, 1), :] for k in range(count)], axis=1)


def pair_sum(product):
    return product + pltpu.roll(product, product.shape[0] - 1, 0)


def window_base(offset):
    return pl.multiple_of((offset >> 7) * LANES, LANES)


def one_hot(count, index):
    shape = (count, index.shape[1])
    return (lax.broadcasted_iota(I32, shape, 0) == index).astype(F32).astype(BF16)


def push_bins(tile, pos_ref):
    for unit in range(2):
        pos = row_of(pos_ref, tile * 4 + unit * 2, 2)
        lo = (((pos >> 11) & 1) << 7) + (pos & 127)
        pltpu.matmul_push_rhs(one_hot(2 * LANES, lo), 0, unit, transpose=True)


def split_lines(tile, factor, cam_ref, line_ref):
    rows = pl.ds(pl.multiple_of(tile * 8, 8), 8)
    for m in range(CAM):
        value = pair_sum(cam_ref[m, rows, :] * factor)
        high = value.astype(BF16).astype(F32)
        line_ref[0, m] = high
        line_ref[1, m] = value - high


def add_lines(tile, pos_ref, line_ref, accs):
    hots = []
    for unit in range(2):
        owner = row_of(pos_ref, tile * 4 + unit * 2, 2) >> 7
        hots.append(one_hot(BINS, ((owner >> 5) << 4) + (owner & 15)))
    for part in range(2):
        for m in range(CAM):
            for unit in range(2):
                pieces = []
                for q in range(2):
                    row = 2 * (2 * unit + q)
                    line = jnp.broadcast_to(line_ref[part, m, row : row + 1], (16, LANES)).astype(BF16)
                    hot = hots[unit][:, q * LANES : (q + 1) * LANES].reshape(BINS // 16, 16, LANES)
                    pieces.append((hot * line[None]).reshape(BINS, LANES))
                lhs = jnp.concatenate(pieces, axis=1)
                staged = 0 if part == 0 and m == 0 else None
                pltpu.matmul_acc_lhs(accs[unit * CAM + m], lhs, staged)


def empty_accs(accs):
    return [pltpu.matmul_pop(acc) for acc in accs]


def drain(accs, total_ref):
    for unit in range(2):
        pltpu.matmul_acc_lhs(accs[unit * CAM], jnp.zeros((BINS, 2 * LANES), BF16), 0)
    for m in range(CAM):
        total = pltpu.matmul_pop(accs[m]) + pltpu.matmul_pop(accs[CAM + m])
        total_ref[0, m * BINS : (m + 1) * BINS] = total[:, :LANES]
        total_ref[1, m * BINS : (m + 1) * BINS] = total[:, LANES:]


def regroup_into(out_ref, total_ref):
    def one(hi, _):
        for side in range(2):
            for g in range(3):
                rows = pl.ds(g * 3 * BINS + hi, 3, stride=BINS)
                out_ref[side, g, hi >> 4, (hi >> 2) & 3, hi & 3] = total_ref[side, rows, :]
        return 0

    lax.fori_loop(0, BINS, one, 0, unroll=4)


def solve_points(point_ref, damp_ref, step_ref):
    points = damp_ref.shape[0] * LANES
    damping = row_of(damp_ref, 0, points // LANES)
    g = [point_ref[k : k + 1, 0:points] for k in range(3)]
    aa, ab, ac, bb, bc, cc = [point_ref[k : k + 1, 0:points] for k in range(3, 9)]
    aa, bb, cc = aa + damping, bb + damping, cc + damping
    cof_aa = bb * cc - bc * bc
    cof_ab = ac * bc - ab * cc
    cof_ac = ab * bc - ac * bb
    cof_bb = aa * cc - ac * ac
    cof_bc = ab * ac - aa * bc
    cof_cc = aa * bb - ab * ab
    determ = aa * cof_aa + ab * cof_ab + ac * cof_ac
    steps = [
        (cof_aa * g[0] + cof_ab * g[1] + cof_ac * g[2]) / determ,
        (cof_ab * g[0] + cof_bb * g[1] + cof_bc * g[2]) / determ,
        (cof_ac * g[0] + cof_bc * g[1] + cof_cc * g[2]) / determ,
    ]
    step_ref[...] = jnp.zeros_like(step_ref)
    for k in range(3):
        for p, part in enumerate(thirds(steps[k])):
            step_ref[3 * p + k : 3 * p + k + 1, 0:points] = part.astype(F32)
    return jnp.sum(g[0] * g[0] + g[1] * g[1] + g[2] * g[2])


def first_kernel(
    offset_ref,
    res_ref,
    cam_ref,
    pt_ref,
    camera_ref,
    slot_ref,
    damp_ref,
    table_ref,
    grad_ref,
    pos_ref,
    index_ref,
    window_ref,
    sums_ref,
    step_ref,
    feat_ref,
    point_ref,
    line_ref,
    total_ref,
    *accs,
):
    tiles = res_ref.shape[0] // 8
    point_accs, accs = accs[:2], accs[2:]
    point_ref[...] = jnp.zeros_like(point_ref)
    feat_ref[...] = jnp.zeros_like(feat_ref)
    empty_accs(point_accs + accs)

    def find(tile):
        lines = pl.ds(pl.multiple_of(tile * 4, 4), 4)
        camera = camera_ref[lines, :]
        high, low = camera >> 7, camera & 127
        found = [jnp.zeros_like(camera)] * 4
        for k in range(table_ref.shape[0]):
            line = jnp.broadcast_to(table_ref[k : k + 1, :], camera.shape)
            taken = jnp.take_along_axis(line, low, axis=1, mode="promise_in_bounds")
            found[k % 4] = jnp.where(high == k, taken, found[k % 4])
        pos_ref[lines, :] = (found[0] + found[1]) + (found[2] + found[3])

    def residual_of(tile):
        return res_ref[pl.ds(pl.multiple_of(tile * 8, 8), 8), :]

    def add_points(tile):
        rows = pl.ds(pl.multiple_of(tile * 8, 8), 8)
        r = residual_of(tile)
        j = [pt_ref[k, rows, :] for k in range(3)]
        products = [j[0] * r, j[1] * r, j[2] * r]
        products += [j[0] * j[0], j[0] * j[1], j[0] * j[2]]
        products += [j[1] * j[1], j[1] * j[2], j[2] * j[2]]
        for f, product in enumerate(products):
            feat_ref[f * 8 : f * 8 + 8, :] = pair_sum(product)
        offset = offset_ref[tile]
        lines = pl.ds(pl.multiple_of(tile * 4, 4), 4)
        index_ref[lines, :] = slot_ref[lines, :] + (offset & 127)
        index, base = row_of(index_ref, tile * 4, 4), window_base(offset)
        for unit in range(2):
            columns = [feat_ref[pl.ds(4 * unit + 2 * q, 16, stride=8), :] for q in range(2)]
            lhs = jnp.concatenate(thirds(jnp.concatenate(columns, axis=1)), axis=0)
            hot = one_hot(2 * LANES, index[:, unit * 2 * LANES : (unit + 1) * 2 * LANES])
            pltpu.matmul_push_rhs(hot, 1, unit, transpose=True)
            pltpu.matmul_acc_lhs(point_accs[unit], lhs, 1)
        return base

    find(0)
    push_bins(0, pos_ref)
    split_lines(0, residual_of(0), cam_ref, line_ref.at[0])

    def one_tile(tile, now, later):
        ahead = jnp.minimum(tile + 1, tiles - 1)
        add_lines(tile, pos_ref, line_ref.at[now], accs)
        base = add_points(tile)
        find(ahead)
        push_bins(ahead, pos_ref)
        split_lines(ahead, residual_of(ahead), cam_ref, line_ref.at[later])
        dots = pltpu.matmul_pop(point_accs[0]) + pltpu.matmul_pop(point_accs[1])
        point_ref[:, pl.ds(base, 2 * LANES)] += (dots[32:48] + dots[16:32]) + dots[0:16]

    def two_tiles(k, _):
        one_tile(2 * k, 0, 1)
        one_tile(2 * k + 1, 1, 0)
        return 0

    lax.fori_loop(0, tiles // 2, two_tiles, 0)
    drain(accs, total_ref)
    regroup_into(grad_ref, total_ref)
    point_square = solve_points(point_ref, damp_ref, step_ref)

    def cut_window(tile, _):
        window_ref[tile] = step_ref[:, pl.ds(window_base(offset_ref[tile]), 2 * LANES)].astype(BF16)
        return 0

    lax.fori_loop(0, tiles, cut_window, 0, unroll=4)
    residual = res_ref[...]
    cost = jnp.sum(residual * residual)
    lane = lax.broadcasted_iota(I32, sums_ref.shape, 1)
    sums_ref[...] = jnp.where(lane == 0, cost, jnp.where(lane == 1, point_square, 0.0))


def move_start(tile, index_ref, window_ref, point_accs):
    index = row_of(index_ref, tile * 4, 4)
    lhs = window_ref[tile]
    for unit in range(2):
        hot = one_hot(2 * LANES, index[:, unit * 2 * LANES : (unit + 1) * 2 * LANES])
        pltpu.matmul_push_rhs(hot, 1, unit)
        pltpu.matmul_acc_lhs(point_accs[unit], lhs, 1)


def move_end(tile, pt_ref, res_ref, moved_ref, point_accs):
    for unit in range(2):
        dots = pltpu.matmul_pop(point_accs[unit])
        taken = (dots[6:9] + dots[3:6]) + dots[0:3]
        for q in range(2):
            piece = taken[:, q * LANES : (q + 1) * LANES]
            for a in range(2):
                row = tile * 8 + 2 * (2 * unit + q) + a
                jac = jnp.concatenate([pt_ref[k, pl.ds(row, 1), :] for k in range(3)], axis=0)
                moved = jnp.sum(jac * piece, axis=0, keepdims=True)
                moved_ref[pl.ds(row, 1), :] = moved - res_ref[pl.ds(row, 1), :]


def second_start(index_ref, window_ref, pt_ref, res_ref, moved_ref, pos_ref, cam_ref, line_ref, accs):
    point_accs, accs = accs[:2], accs[2:]
    empty_accs(point_accs + accs)
    for tile in range(2):
        move_start(tile, index_ref, window_ref, point_accs)
        move_end(tile, pt_ref, res_ref, moved_ref, point_accs)
    push_bins(0, pos_ref)
    split_lines(0, moved_ref[0:8, :], cam_ref, line_ref.at[0])


def second_tiles(
    first, last, index_ref, window_ref, pt_ref, res_ref, moved_ref, pos_ref, cam_ref, line_ref, accs
):
    tiles = res_ref.shape[0] // 8
    point_accs, accs = accs[:2], accs[2:]

    def one_tile(tile, now, later):
        ahead = jnp.minimum(tile + 1, tiles - 1)
        after = jnp.minimum(tile + 2, tiles - 1)
        add_lines(tile, pos_ref, line_ref.at[now], accs)
        move_start(after, index_ref, window_ref, point_accs)
        push_bins(ahead, pos_ref)
        factor = moved_ref[pl.ds(pl.multiple_of(ahead * 8, 8), 8), :]
        split_lines(ahead, factor, cam_ref, line_ref.at[later])
        move_end(after, pt_ref, res_ref, moved_ref, point_accs)

    def two_tiles(k, _):
        one_tile(2 * k, 0, 1)
        one_tile(2 * k + 1, 1, 0)
        return 0

    lax.fori_loop(first // 2, last // 2, two_tiles, 0)


def scoped(kernel, shapes):
    def whole(*refs):
        pl.run_scoped(lambda *accs: kernel(*refs, *accs), *shapes())

    return whole


def acc_shapes():
    points = [pltpu.ACC(unit)((48, 2 * LANES), F32) for unit in range(2)]
    return points + [pltpu.ACC(unit)((BINS, 2 * LANES), F32) for unit in range(2) for _ in range(CAM)]


def take_shapes():
    points = [pltpu.ACC(unit)((16, 2 * LANES), F32) for unit in range(2)]
    return points + acc_shapes()[2:]


def row_major(array):
    rows, n_obs = array.shape[1:-1], array.shape[-1]
    blocks = array.reshape(2, *rows, n_obs // LANES, LANES)
    blocks = jnp.moveaxis(blocks, 0, -2)
    return blocks.reshape(*rows, 2 * n_obs // LANES, LANES)


def first_half(residual, cam_jacobian, point_jacobian, obs_camera, obs_slot, tile_offset, damping, camera_slot):
    vmem = pl.BlockSpec(memory_space=pltpu.VMEM)
    points = damping.shape[0]
    return pl.pallas_call(
        scoped(first_kernel, acc_shapes),
        out_shape=(
            jax.ShapeDtypeStruct((2, 3, 4, 4, 4, 3, LANES), F32),
            jax.ShapeDtypeStruct(obs_camera.shape, I32),
            jax.ShapeDtypeStruct(obs_camera.shape, I32),
            jax.ShapeDtypeStruct((tile_offset.size, 16, 2 * LANES), BF16),
            jax.ShapeDtypeStruct((8, LANES), F32),
        ),
        in_specs=[pl.BlockSpec(memory_space=pltpu.SMEM)] + [vmem] * 7,
        out_specs=(vmem,) * 5,
        scratch_shapes=[
            pltpu.VMEM((16, damping.size + LANES), F32),
            pltpu.VMEM((16 * 8, LANES), F32),
            pltpu.VMEM((16, damping.size + LANES), F32),
            pltpu.VMEM((2, 2, CAM, 8, LANES), F32),
            pltpu.VMEM((2, CAM * BINS, LANES), F32),
        ],
    )(tile_offset, residual, cam_jacobian, point_jacobian, obs_camera, obs_slot, damping, camera_slot)


AXES = ("gx_0", "gx_1", "gy_0", "gy_1")
RINGS = ("gx_0", "gy_0", "gy_1")
ORDERS = ((0, 1, 2), (1, 2, 0), (2, 0, 1))
SPOTS = (0, 1, 0)


def neighbours(me, names, sizes):
    total = 1
    for name in names:
        total *= sizes[name]
    place = 0
    for name in names:
        place = place * sizes[name] + me[name]
    found = []
    for k in range(1, total):
        other = lax.rem(place + k, total)
        target = dict(me)
        for name in reversed(names):
            target[name] = lax.rem(other, sizes[name])
            other = other // sizes[name]
        found.append(tuple(target[name] for name in AXES))
    return found


def inside(position, index):
    return (slice(None),) * position + (index,)


def second_kernel(
    sizes,
    scale,
    res_ref,
    cam_ref,
    pt_ref,
    pos_ref,
    index_ref,
    window_ref,
    grad_ref,
    sums_ref,
    reduced_ref,
    cost_ref,
    norm_ref,
    moved_ref,
    line_ref,
    total_ref,
    move_ref,
    pair_ref,
    whole_ref,
    in1_ref,
    sum1_ref,
    in2_ref,
    sum2_ref,
    in3_ref,
    mine_ref,
    far_ref,
    plane_ref,
    near_ref,
    pair_send,
    pair_recv,
    ring_send,
    ring_recv,
    far_send,
    far_recv,
    near_send,
    near_recv,
    *accs,
):
    me = {name: lax.axis_index(name) for name in AXES}
    far = neighbours(me, ("gx_0", "gx_1"), sizes)
    near = neighbours(me, ("gy_0", "gy_1"), sizes)
    rings = [neighbours(me, (name,), sizes) for name in RINGS]
    core = me["gx_1"]
    partner = (me["gx_0"], 1 - core, me["gy_0"], me["gy_1"])

    barrier = pltpu.get_barrier_semaphore()
    for target in far + near:
        pl.semaphore_signal(barrier, inc=1, device_id=target, device_id_type=MESH)

    started = []

    def send(source, target_ref, send_sem, recv_sem, device):
        copy = pltpu.make_async_remote_copy(
            src_ref=source,
            dst_ref=target_ref,
            send_sem=send_sem,
            recv_sem=recv_sem,
            device_id=device,
            device_id_type=MESH,
        )
        copy.start()
        started.append(copy)
        return copy

    def spread(source, inbox, job, group, phase, position):
        ring = ORDERS[group][phase]
        name = RINGS[ring]
        copies = []
        for k, device in enumerate(rings[ring]):
            there = device[AXES.index(name)]
            copies.append(
                send(
                    source.at[(job, group) + inside(position, there)],
                    inbox.at[job, group, k],
                    ring_send.at[job, group, phase, k],
                    ring_recv.at[job, group, phase, k],
                    device,
                )
            )
        return copies

    def gather(source, inbox, copies, job, group, phase, position):
        for copy in copies:
            copy.wait_recv()
        here = me[RINGS[ORDERS[group][phase]]]
        kept = source[(job, group) + inside(position, here)]
        return (kept + inbox[job, group, 1]) + (inbox[job, group, 0] + inbox[job, group, 2])

    flight = {}

    def pairs(job, source):
        flight[job] = [
            send(
                source.at[1 - core, g],
                pair_ref.at[job, g],
                pair_send.at[job, g],
                pair_recv.at[job, g],
                partner,
            )
            for g in range(3)
        ]

    def phase_one(job, source):
        copies = flight[job]
        flight[job] = []
        for g in range(3):
            copies[g].wait_recv()
            whole_ref[job, g] = source[core, g] + pair_ref[job, g]
            flight[job].append(spread(whole_ref, in1_ref, job, g, 0, ORDERS[g][0]))

    def phase_two(job):
        copies = flight[job]
        flight[job] = []
        for g in range(3):
            sum1_ref[job, g] = gather(whole_ref, in1_ref, copies[g], job, g, 0, ORDERS[g][0])
            flight[job].append(spread(sum1_ref, in2_ref, job, g, 1, SPOTS[g]))

    def phase_three(job):
        copies = flight[job]
        flight[job] = []
        for g in range(3):
            sum2_ref[job, g] = gather(sum1_ref, in2_ref, copies[g], job, g, 1, SPOTS[g])
            flight[job].append(spread(sum2_ref, in3_ref, job, g, 2, 0))

    def finish(job):
        own = [gather(sum2_ref, in3_ref, flight[job][g], job, g, 2, 0) for g in range(3)]
        return jnp.concatenate(own, axis=0)

    refs = (index_ref, window_ref, pt_ref, res_ref, moved_ref, pos_ref, cam_ref, line_ref, accs)
    second_start(*refs)
    pl.semaphore_wait(barrier, len(far) + len(near))
    pairs(0, grad_ref)
    second_tiles(0, 4, *refs)
    phase_one(0, grad_ref)
    second_tiles(4, 12, *refs)
    phase_two(0)
    second_tiles(12, 18, *refs)
    phase_three(0)
    second_tiles(18, 24, *refs)
    grads = finish(0)
    lane = lax.broadcasted_iota(I32, mine_ref.shape, 1)
    mine_ref[...] = sums_ref[...] + jnp.where(lane == 1, jnp.sum(grads * grads), 0.0)
    arrivals = [
        send(mine_ref, far_ref.at[k], far_send.at[k], far_recv.at[k], device)
        for k, device in enumerate(far)
    ]
    second_tiles(24, 32, *refs)
    drain(accs[2:], total_ref)
    regroup_into(move_ref, total_ref)
    pairs(1, move_ref)
    for copy in arrivals:
        copy.wait_recv()
    plane_ref[...] = mine_ref[...] + jnp.sum(far_ref[...], axis=0)
    phase_one(1, move_ref)
    arrivals = [
        send(plane_ref, near_ref.at[k], near_send.at[k], near_recv.at[k], device)
        for k, device in enumerate(near)
    ]
    phase_two(1)
    phase_three(1)
    for copy in arrivals:
        copy.wait_recv()
    totals = plane_ref[...] + jnp.sum(near_ref[...], axis=0)
    first_row = lax.broadcasted_iota(I32, mine_ref.shape, 0) == 0
    cost = totals / scale[0]
    norm = jnp.sqrt(totals / scale[1] + 1e-06)
    cost_ref[0, 0] = jnp.sum(jnp.where(first_row & (lane == 0), cost, 0.0))
    norm_ref[0, 0] = jnp.sum(jnp.where(first_row & (lane == 1), norm, 0.0))
    reduced_ref[...] = finish(1)
    for copy in started:
        copy.wait_send()


def second_half(residual, cam_jacobian, point_jacobian, pos, index, window, grad, sums, sizes, scale):
    vmem = pl.BlockSpec(memory_space=pltpu.VMEM)
    smem = pl.BlockSpec(memory_space=pltpu.SMEM)
    rows = CAM // 3
    buffer = lambda *lead: pltpu.VMEM(lead + (rows, LANES), F32)
    dma = pltpu.SemaphoreType.DMA
    far = sizes["gx_0"] * sizes["gx_1"] - 1
    near = sizes["gy_0"] * sizes["gy_1"] - 1
    return pl.pallas_call(
        scoped(functools.partial(second_kernel, sizes, scale), take_shapes),
        out_shape=(
            jax.ShapeDtypeStruct((CAM, LANES), F32),
            jax.ShapeDtypeStruct((1, 1), F32),
            jax.ShapeDtypeStruct((1, 1), F32),
        ),
        in_specs=[vmem] * 8,
        out_specs=(vmem, smem, smem),
        scratch_shapes=[
            pltpu.VMEM(residual.shape, F32),
            pltpu.VMEM((2, 2, CAM, 8, LANES), F32),
            pltpu.VMEM((2, CAM * BINS, LANES), F32),
            buffer(2, 3, 4, 4, 4),
            buffer(2, 3, 4, 4, 4),
            buffer(2, 3, 4, 4, 4),
            buffer(2, 3, 3, 4, 4),
            buffer(2, 3, 4, 4),
            buffer(2, 3, 3, 4),
            buffer(2, 3, 4),
            buffer(2, 3, 3),
            pltpu.VMEM((8, LANES), F32),
            pltpu.VMEM((far, 8, LANES), F32),
            pltpu.VMEM((8, LANES), F32),
            pltpu.VMEM((near, 8, LANES), F32),
            dma((2, 3)),
            dma((2, 3)),
            dma((2, 3, 3, 3)),
            dma((2, 3, 3, 3)),
            dma((far,)),
            dma((far,)),
            dma((near,)),
            dma((near,)),
        ],
        compiler_params=pltpu.CompilerParams(collective_id=0, has_side_effects=True),
    )(residual, cam_jacobian, point_jacobian, pos, index, window, grad, sums)


def on_device(
    residual, cam_jacobian, point_jacobian, obs_camera, obs_slot, tile_offset, damping, camera_slot
):
    n_obs = residual.shape[1]
    sizes = {name: lax.axis_size(name) for name in AXES}
    devices = lax.axis_size(AXES)
    scale = (2.0 * n_obs * devices, 9.0 * camera_slot.shape[0] + 3.0 * damping.shape[0] * devices)
    lines = lambda array: array.reshape(-1, LANES)
    res, cam, pt = row_major(residual), row_major(cam_jacobian), row_major(point_jacobian)
    grad, pos, index, window, sums = first_half(
        res, cam, pt, lines(obs_camera), lines(obs_slot), tile_offset, lines(damping), lines(camera_slot)
    )
    reduced, cost, norm = second_half(res, cam, pt, pos, index, window, grad, sums, sizes, scale)
    return (reduced, cost.reshape(()), norm.reshape(()))


def solution(mesh):
    finer = Mesh(mesh.devices.reshape(4, 2, 4, 4), AXES)
    in_specs = (
        P(None, AXES),
        P(None, None, AXES),
        P(None, None, AXES),
        P(AXES),
        P(AXES),
        P(AXES),
        P(AXES),
        P(),
    )
    out_specs = (P(None, AXES), P(), P())
    return jax.shard_map(
        on_device, mesh=finer, in_specs=in_specs, out_specs=out_specs, check_vma=False
    )
```

```python
import functools

import jax
import jax.numpy as jnp
from jax import lax
from jax.experimental import pallas as pl
from jax.experimental.pallas import tpu as pltpu
from jax.sharding import Mesh
from jax.sharding import PartitionSpec as P

F32, BF16, I32 = jnp.float32, jnp.bfloat16, jnp.int32
NT = (((1,), (1,)), ((), ()))
MESH = pl.DeviceIdType.MESH
LANES = 128
CAM = 9
BINS = 64
UNROLL = 4


def thirds(value):
    high = value.astype(BF16)
    rest = value - high.astype(F32)
    middle = rest.astype(BF16)
    return high, middle, (rest - middle.astype(F32)).astype(BF16)


def row_of(ref, start, count):
    return jnp.concatenate([ref[pl.ds(start + k, 1), :] for k in range(count)], axis=1)


def pair_sum(product):
    return product + pltpu.roll(product, product.shape[0] - 1, 0)


def window_base(offset):
    return pl.multiple_of((offset >> 7) * LANES, LANES)


def one_hot(count, index):
    shape = (count, index.shape[1])
    return (lax.broadcasted_iota(I32, shape, 0) == index).astype(F32).astype(BF16)


def push_bins(tile, pos_ref):
    for unit in range(2):
        pos = row_of(pos_ref, tile * 4 + unit * 2, 2)
        lo = (((pos >> 11) & 1) << 7) + (pos & 127)
        pltpu.matmul_push_rhs(one_hot(2 * LANES, lo), 0, unit, transpose=True)


def split_lines(tile, factor, cam_ref, line_ref):
    rows = pl.ds(pl.multiple_of(tile * 8, 8), 8)
    for m in range(CAM):
        value = pair_sum(cam_ref[m, rows, :] * factor)
        high = value.astype(BF16).astype(F32)
        line_ref[0, m] = high
        line_ref[1, m] = value - high


def add_lines(tile, pos_ref, line_ref, accs):
    hots = []
    for unit in range(2):
        owner = row_of(pos_ref, tile * 4 + unit * 2, 2) >> 7
        hots.append(one_hot(BINS, ((owner >> 5) << 4) + (owner & 15)))
    for part in range(2):
        for m in range(CAM):
            for unit in range(2):
                pieces = []
                for q in range(2):
                    row = 2 * (2 * unit + q)
                    line = jnp.broadcast_to(line_ref[part, m, row : row + 1], (16, LANES)).astype(BF16)
                    hot = hots[unit][:, q * LANES : (q + 1) * LANES].reshape(BINS // 16, 16, LANES)
                    pieces.append((hot * line[None]).reshape(BINS, LANES))
                lhs = jnp.concatenate(pieces, axis=1)
                staged = 0 if part == 0 and m == 0 else None
                pltpu.matmul_acc_lhs(accs[unit * CAM + m], lhs, staged)


def empty_accs(accs):
    return [pltpu.matmul_pop(acc) for acc in accs]


def drain(accs, total_ref):
    for unit in range(2):
        pltpu.matmul_acc_lhs(accs[unit * CAM], jnp.zeros((BINS, 2 * LANES), BF16), 0)
    for m in range(CAM):
        total = pltpu.matmul_pop(accs[m]) + pltpu.matmul_pop(accs[CAM + m])
        total_ref[0, m * BINS : (m + 1) * BINS] = total[:, :LANES]
        total_ref[1, m * BINS : (m + 1) * BINS] = total[:, LANES:]


def regroup_into(out_ref, total_ref):
    def one(hi, _):
        for side in range(2):
            for g in range(3):
                rows = pl.ds(g * 3 * BINS + hi, 3, stride=BINS)
                out_ref[side, g, hi >> 4, (hi >> 2) & 3, hi & 3] = total_ref[side, rows, :]
        return 0

    lax.fori_loop(0, BINS, one, 0, unroll=4)


def solve_points(point_ref, damp_ref, step_ref):
    points = damp_ref.shape[0] * LANES
    damping = row_of(damp_ref, 0, points // LANES)
    g = [point_ref[k : k + 1, 0:points] for k in range(3)]
    aa, ab, ac, bb, bc, cc = [point_ref[k : k + 1, 0:points] for k in range(3, 9)]
    aa, bb, cc = aa + damping, bb + damping, cc + damping
    cof_aa = bb * cc - bc * bc
    cof_ab = ac * bc - ab * cc
    cof_ac = ab * bc - ac * bb
    cof_bb = aa * cc - ac * ac
    cof_bc = ab * ac - aa * bc
    cof_cc = aa * bb - ab * ab
    determ = aa * cof_aa + ab * cof_ab + ac * cof_ac
    steps = [
        (cof_aa * g[0] + cof_ab * g[1] + cof_ac * g[2]) / determ,
        (cof_ab * g[0] + cof_bb * g[1] + cof_bc * g[2]) / determ,
        (cof_ac * g[0] + cof_bc * g[1] + cof_cc * g[2]) / determ,
    ]
    step_ref[...] = jnp.zeros_like(step_ref)
    for k in range(3):
        for p, part in enumerate(thirds(steps[k])):
            step_ref[3 * p + k : 3 * p + k + 1, 0:points] = part.astype(F32)
    return jnp.sum(g[0] * g[0] + g[1] * g[1] + g[2] * g[2])


def first_kernel(
    offset_ref,
    res_ref,
    cam_ref,
    pt_ref,
    camera_ref,
    slot_ref,
    damp_ref,
    table_ref,
    grad_ref,
    pos_ref,
    index_ref,
    window_ref,
    sums_ref,
    step_ref,
    feat_ref,
    point_ref,
    line_ref,
    total_ref,
    *accs,
):
    tiles = res_ref.shape[0] // 8
    point_accs, accs = accs[:2], accs[2:]
    point_ref[...] = jnp.zeros_like(point_ref)
    feat_ref[...] = jnp.zeros_like(feat_ref)
    empty_accs(point_accs + accs)

    def find(tile):
        lines = pl.ds(pl.multiple_of(tile * 4, 4), 4)
        camera = camera_ref[lines, :]
        high, low = camera >> 7, camera & 127
        found = [jnp.zeros_like(camera)] * 4
        for k in range(table_ref.shape[0]):
            line = jnp.broadcast_to(table_ref[k : k + 1, :], camera.shape)
            taken = jnp.take_along_axis(line, low, axis=1, mode="promise_in_bounds")
            found[k % 4] = jnp.where(high == k, taken, found[k % 4])
        pos_ref[lines, :] = (found[0] + found[1]) + (found[2] + found[3])

    def residual_of(tile):
        return res_ref[pl.ds(pl.multiple_of(tile * 8, 8), 8), :]

    def add_points(tile):
        rows = pl.ds(pl.multiple_of(tile * 8, 8), 8)
        r = residual_of(tile)
        j = [pt_ref[k, rows, :] for k in range(3)]
        products = [j[0] * r, j[1] * r, j[2] * r]
        products += [j[0] * j[0], j[0] * j[1], j[0] * j[2]]
        products += [j[1] * j[1], j[1] * j[2], j[2] * j[2]]
        for f, product in enumerate(products):
            feat_ref[f * 8 : f * 8 + 8, :] = pair_sum(product)
        offset = offset_ref[tile]
        lines = pl.ds(pl.multiple_of(tile * 4, 4), 4)
        index_ref[lines, :] = slot_ref[lines, :] + (offset & 127)
        index, base = row_of(index_ref, tile * 4, 4), window_base(offset)
        for unit in range(2):
            columns = [feat_ref[pl.ds(4 * unit + 2 * q, 16, stride=8), :] for q in range(2)]
            lhs = jnp.concatenate(thirds(jnp.concatenate(columns, axis=1)), axis=0)
            hot = one_hot(2 * LANES, index[:, unit * 2 * LANES : (unit + 1) * 2 * LANES])
            pltpu.matmul_push_rhs(hot, 1, unit, transpose=True)
            pltpu.matmul_acc_lhs(point_accs[unit], lhs, 1)
        return base

    find(0)
    push_bins(0, pos_ref)
    split_lines(0, residual_of(0), cam_ref, line_ref.at[0])

    def one_tile(tile, now, later):
        ahead = jnp.minimum(tile + 1, tiles - 1)
        add_lines(tile, pos_ref, line_ref.at[now], accs)
        base = add_points(tile)
        find(ahead)
        push_bins(ahead, pos_ref)
        split_lines(ahead, residual_of(ahead), cam_ref, line_ref.at[later])
        dots = pltpu.matmul_pop(point_accs[0]) + pltpu.matmul_pop(point_accs[1])
        point_ref[:, pl.ds(base, 2 * LANES)] += (dots[32:48] + dots[16:32]) + dots[0:16]

    def some_tiles(k, _):
        for s in range(UNROLL):
            one_tile(UNROLL * k + s, s % 2, 1 - s % 2)
        return 0

    lax.fori_loop(0, tiles // UNROLL, some_tiles, 0)
    drain(accs, total_ref)
    regroup_into(grad_ref, total_ref)
    point_square = solve_points(point_ref, damp_ref, step_ref)

    def cut_window(tile, _):
        window_ref[tile] = step_ref[:, pl.ds(window_base(offset_ref[tile]), 2 * LANES)].astype(BF16)
        return 0

    lax.fori_loop(0, tiles, cut_window, 0, unroll=4)
    residual = res_ref[...]
    cost = jnp.sum(residual * residual)
    lane = lax.broadcasted_iota(I32, sums_ref.shape, 1)
    sums_ref[...] = jnp.where(lane == 0, cost, jnp.where(lane == 1, point_square, 0.0))


def move_start(tile, index_ref, window_ref, point_accs):
    index = row_of(index_ref, tile * 4, 4)
    lhs = window_ref[tile]
    for unit in range(2):
        hot = one_hot(2 * LANES, index[:, unit * 2 * LANES : (unit + 1) * 2 * LANES])
        pltpu.matmul_push_rhs(hot, 1, unit)
        pltpu.matmul_acc_lhs(point_accs[unit], lhs, 1)


def move_end(tile, pt_ref, res_ref, moved_ref, point_accs):
    for unit in range(2):
        dots = pltpu.matmul_pop(point_accs[unit])
        taken = (dots[6:9] + dots[3:6]) + dots[0:3]
        for q in range(2):
            piece = taken[:, q * LANES : (q + 1) * LANES]
            for a in range(2):
                row = tile * 8 + 2 * (2 * unit + q) + a
                jac = jnp.concatenate([pt_ref[k, pl.ds(row, 1), :] for k in range(3)], axis=0)
                moved = jnp.sum(jac * piece, axis=0, keepdims=True)
                moved_ref[pl.ds(row, 1), :] = moved - res_ref[pl.ds(row, 1), :]


def second_start(index_ref, window_ref, pt_ref, res_ref, moved_ref, pos_ref, cam_ref, line_ref, accs):
    point_accs, accs = accs[:2], accs[2:]
    empty_accs(point_accs + accs)
    for tile in range(2):
        move_start(tile, index_ref, window_ref, point_accs)
        move_end(tile, pt_ref, res_ref, moved_ref, point_accs)
    push_bins(0, pos_ref)
    split_lines(0, moved_ref[0:8, :], cam_ref, line_ref.at[0])


def second_tiles(
    first, last, index_ref, window_ref, pt_ref, res_ref, moved_ref, pos_ref, cam_ref, line_ref, accs
):
    tiles = res_ref.shape[0] // 8
    point_accs, accs = accs[:2], accs[2:]

    def one_tile(tile, now, later):
        ahead = jnp.minimum(tile + 1, tiles - 1)
        after = jnp.minimum(tile + 2, tiles - 1)
        add_lines(tile, pos_ref, line_ref.at[now], accs)
        move_start(after, index_ref, window_ref, point_accs)
        push_bins(ahead, pos_ref)
        factor = moved_ref[pl.ds(pl.multiple_of(ahead * 8, 8), 8), :]
        split_lines(ahead, factor, cam_ref, line_ref.at[later])
        move_end(after, pt_ref, res_ref, moved_ref, point_accs)

    def some_tiles(k, _):
        for s in range(UNROLL):
            one_tile(UNROLL * k + s, s % 2, 1 - s % 2)
        return 0

    lax.fori_loop(first // UNROLL, last // UNROLL, some_tiles, 0)


def scoped(kernel, shapes):
    def whole(*refs):
        pl.run_scoped(lambda *accs: kernel(*refs, *accs), *shapes())

    return whole


def acc_shapes():
    points = [pltpu.ACC(unit)((48, 2 * LANES), F32) for unit in range(2)]
    return points + [pltpu.ACC(unit)((BINS, 2 * LANES), F32) for unit in range(2) for _ in range(CAM)]


def take_shapes():
    points = [pltpu.ACC(unit)((16, 2 * LANES), F32) for unit in range(2)]
    return points + acc_shapes()[2:]


def row_major(array):
    rows, n_obs = array.shape[1:-1], array.shape[-1]
    blocks = array.reshape(2, *rows, n_obs // LANES, LANES)
    blocks = jnp.moveaxis(blocks, 0, -2)
    return blocks.reshape(*rows, 2 * n_obs // LANES, LANES)


def first_half(residual, cam_jacobian, point_jacobian, obs_camera, obs_slot, tile_offset, damping, camera_slot):
    vmem = pl.BlockSpec(memory_space=pltpu.VMEM)
    points = damping.shape[0]
    return pl.pallas_call(
        scoped(first_kernel, acc_shapes),
        out_shape=(
            jax.ShapeDtypeStruct((2, 3, 4, 4, 4, 3, LANES), F32),
            jax.ShapeDtypeStruct(obs_camera.shape, I32),
            jax.ShapeDtypeStruct(obs_camera.shape, I32),
            jax.ShapeDtypeStruct((tile_offset.size, 16, 2 * LANES), BF16),
            jax.ShapeDtypeStruct((8, LANES), F32),
        ),
        in_specs=[pl.BlockSpec(memory_space=pltpu.SMEM)] + [vmem] * 7,
        out_specs=(vmem,) * 5,
        scratch_shapes=[
            pltpu.VMEM((16, damping.size + LANES), F32),
            pltpu.VMEM((16 * 8, LANES), F32),
            pltpu.VMEM((16, damping.size + LANES), F32),
            pltpu.VMEM((2, 2, CAM, 8, LANES), F32),
            pltpu.VMEM((2, CAM * BINS, LANES), F32),
        ],
    )(tile_offset, residual, cam_jacobian, point_jacobian, obs_camera, obs_slot, damping, camera_slot)


AXES = ("gx_0", "gx_1", "gy_0", "gy_1")
RINGS = ("gx_0", "gy_0", "gy_1")
ORDERS = ((0, 1, 2), (1, 2, 0), (2, 0, 1))
SPOTS = (0, 1, 0)


def neighbours(me, names, sizes):
    total = 1
    for name in names:
        total *= sizes[name]
    place = 0
    for name in names:
        place = place * sizes[name] + me[name]
    found = []
    for k in range(1, total):
        other = lax.rem(place + k, total)
        target = dict(me)
        for name in reversed(names):
            target[name] = lax.rem(other, sizes[name])
            other = other // sizes[name]
        found.append(tuple(target[name] for name in AXES))
    return found


def inside(position, index):
    return (slice(None),) * position + (index,)


def second_kernel(
    sizes,
    scale,
    res_ref,
    cam_ref,
    pt_ref,
    pos_ref,
    index_ref,
    window_ref,
    grad_ref,
    sums_ref,
    reduced_ref,
    cost_ref,
    norm_ref,
    moved_ref,
    line_ref,
    total_ref,
    move_ref,
    pair_ref,
    whole_ref,
    in1_ref,
    sum1_ref,
    in2_ref,
    sum2_ref,
    in3_ref,
    mine_ref,
    far_ref,
    plane_ref,
    near_ref,
    pair_send,
    pair_recv,
    ring_send,
    ring_recv,
    far_send,
    far_recv,
    near_send,
    near_recv,
    *accs,
):
    me = {name: lax.axis_index(name) for name in AXES}
    far = neighbours(me, ("gx_0", "gx_1"), sizes)
    near = neighbours(me, ("gy_0", "gy_1"), sizes)
    rings = [neighbours(me, (name,), sizes) for name in RINGS]
    core = me["gx_1"]
    partner = (me["gx_0"], 1 - core, me["gy_0"], me["gy_1"])

    barrier = pltpu.get_barrier_semaphore()
    for target in far + near:
        pl.semaphore_signal(barrier, inc=1, device_id=target, device_id_type=MESH)

    started = []

    def send(source, target_ref, send_sem, recv_sem, device):
        copy = pltpu.make_async_remote_copy(
            src_ref=source,
            dst_ref=target_ref,
            send_sem=send_sem,
            recv_sem=recv_sem,
            device_id=device,
            device_id_type=MESH,
        )
        copy.start()
        started.append(copy)
        return copy

    def spread(source, inbox, job, group, phase, position):
        ring = ORDERS[group][phase]
        name = RINGS[ring]
        copies = []
        for k, device in enumerate(rings[ring]):
            there = device[AXES.index(name)]
            copies.append(
                send(
                    source.at[(job, group) + inside(position, there)],
                    inbox.at[job, group, k],
                    ring_send.at[job, group, phase, k],
                    ring_recv.at[job, group, phase, k],
                    device,
                )
            )
        return copies

    def gather(source, inbox, copies, job, group, phase, position):
        for copy in copies:
            copy.wait_recv()
        here = me[RINGS[ORDERS[group][phase]]]
        kept = source[(job, group) + inside(position, here)]
        return (kept + inbox[job, group, 1]) + (inbox[job, group, 0] + inbox[job, group, 2])

    flight = {}

    def pairs(job, source):
        flight[job] = [
            send(
                source.at[1 - core, g],
                pair_ref.at[job, g],
                pair_send.at[job, g],
                pair_recv.at[job, g],
                partner,
            )
            for g in range(3)
        ]

    def phase_one(job, source):
        copies = flight[job]
        flight[job] = []
        for g in range(3):
            copies[g].wait_recv()
            whole_ref[job, g] = source[core, g] + pair_ref[job, g]
            flight[job].append(spread(whole_ref, in1_ref, job, g, 0, ORDERS[g][0]))

    def phase_two(job):
        copies = flight[job]
        flight[job] = []
        for g in range(3):
            sum1_ref[job, g] = gather(whole_ref, in1_ref, copies[g], job, g, 0, ORDERS[g][0])
            flight[job].append(spread(sum1_ref, in2_ref, job, g, 1, SPOTS[g]))

    def phase_three(job):
        copies = flight[job]
        flight[job] = []
        for g in range(3):
            sum2_ref[job, g] = gather(sum1_ref, in2_ref, copies[g], job, g, 1, SPOTS[g])
            flight[job].append(spread(sum2_ref, in3_ref, job, g, 2, 0))

    def finish(job):
        own = [gather(sum2_ref, in3_ref, flight[job][g], job, g, 2, 0) for g in range(3)]
        return jnp.concatenate(own, axis=0)

    refs = (index_ref, window_ref, pt_ref, res_ref, moved_ref, pos_ref, cam_ref, line_ref, accs)
    lane = lax.broadcasted_iota(I32, mine_ref.shape, 1)
    second_start(*refs)
    second_tiles(0, 8, *refs)
    pl.semaphore_wait(barrier, len(far) + len(near))
    pairs(0, grad_ref)
    second_tiles(8, 16, *refs)
    phase_one(0, grad_ref)
    second_tiles(16, 24, *refs)
    phase_two(0)
    second_tiles(24, 32, *refs)
    drain(accs[2:], total_ref)
    regroup_into(move_ref, total_ref)
    pairs(1, move_ref)
    phase_three(0)
    phase_one(1, move_ref)
    grads = finish(0)
    mine_ref[...] = sums_ref[...] + jnp.where(lane == 1, jnp.sum(grads * grads), 0.0)
    arrivals = [
        send(mine_ref, far_ref.at[k], far_send.at[k], far_recv.at[k], device)
        for k, device in enumerate(far)
    ]
    phase_two(1)
    for copy in arrivals:
        copy.wait_recv()
    plane_ref[...] = mine_ref[...] + jnp.sum(far_ref[...], axis=0)
    arrivals = [
        send(plane_ref, near_ref.at[k], near_send.at[k], near_recv.at[k], device)
        for k, device in enumerate(near)
    ]
    phase_three(1)
    for copy in arrivals:
        copy.wait_recv()
    totals = plane_ref[...] + jnp.sum(near_ref[...], axis=0)
    first_row = lax.broadcasted_iota(I32, mine_ref.shape, 0) == 0
    cost = totals / scale[0]
    norm = jnp.sqrt(totals / scale[1] + 1e-06)
    cost_ref[0, 0] = jnp.sum(jnp.where(first_row & (lane == 0), cost, 0.0))
    norm_ref[0, 0] = jnp.sum(jnp.where(first_row & (lane == 1), norm, 0.0))
    reduced_ref[...] = finish(1)
    for copy in started:
        copy.wait_send()


def second_half(residual, cam_jacobian, point_jacobian, pos, index, window, grad, sums, sizes, scale):
    vmem = pl.BlockSpec(memory_space=pltpu.VMEM)
    smem = pl.BlockSpec(memory_space=pltpu.SMEM)
    rows = CAM // 3
    buffer = lambda *lead: pltpu.VMEM(lead + (rows, LANES), F32)
    dma = pltpu.SemaphoreType.DMA
    far = sizes["gx_0"] * sizes["gx_1"] - 1
    near = sizes["gy_0"] * sizes["gy_1"] - 1
    return pl.pallas_call(
        scoped(functools.partial(second_kernel, sizes, scale), take_shapes),
        out_shape=(
            jax.ShapeDtypeStruct((CAM, LANES), F32),
            jax.ShapeDtypeStruct((1, 1), F32),
            jax.ShapeDtypeStruct((1, 1), F32),
        ),
        in_specs=[vmem] * 8,
        out_specs=(vmem, smem, smem),
        scratch_shapes=[
            pltpu.VMEM(residual.shape, F32),
            pltpu.VMEM((2, 2, CAM, 8, LANES), F32),
            pltpu.VMEM((2, CAM * BINS, LANES), F32),
            buffer(2, 3, 4, 4, 4),
            buffer(2, 3, 4, 4, 4),
            buffer(2, 3, 4, 4, 4),
            buffer(2, 3, 3, 4, 4),
            buffer(2, 3, 4, 4),
            buffer(2, 3, 3, 4),
            buffer(2, 3, 4),
            buffer(2, 3, 3),
            pltpu.VMEM((8, LANES), F32),
            pltpu.VMEM((far, 8, LANES), F32),
            pltpu.VMEM((8, LANES), F32),
            pltpu.VMEM((near, 8, LANES), F32),
            dma((2, 3)),
            dma((2, 3)),
            dma((2, 3, 3, 3)),
            dma((2, 3, 3, 3)),
            dma((far,)),
            dma((far,)),
            dma((near,)),
            dma((near,)),
        ],
        compiler_params=pltpu.CompilerParams(collective_id=0, has_side_effects=True),
    )(residual, cam_jacobian, point_jacobian, pos, index, window, grad, sums)


def on_device(
    residual, cam_jacobian, point_jacobian, obs_camera, obs_slot, tile_offset, damping, camera_slot
):
    n_obs = residual.shape[1]
    sizes = {name: lax.axis_size(name) for name in AXES}
    devices = lax.axis_size(AXES)
    scale = (2.0 * n_obs * devices, 9.0 * camera_slot.shape[0] + 3.0 * damping.shape[0] * devices)
    lines = lambda array: array.reshape(-1, LANES)
    res, cam, pt = row_major(residual), row_major(cam_jacobian), row_major(point_jacobian)
    grad, pos, index, window, sums = first_half(
        res, cam, pt, lines(obs_camera), lines(obs_slot), tile_offset, lines(damping), lines(camera_slot)
    )
    reduced, cost, norm = second_half(res, cam, pt, pos, index, window, grad, sums, sizes, scale)
    return (reduced, cost.reshape(()), norm.reshape(()))


def solution(mesh):
    finer = Mesh(mesh.devices.reshape(4, 2, 4, 4), AXES)
    in_specs = (
        P(None, AXES),
        P(None, None, AXES),
        P(None, None, AXES),
        P(AXES),
        P(AXES),
        P(AXES),
        P(AXES),
        P(),
    )
    out_specs = (P(None, AXES), P(), P())
    return jax.shard_map(
        on_device, mesh=finer, in_specs=in_specs, out_specs=out_specs, check_vma=False
    )
```

```python
import functools

import jax
import jax.numpy as jnp
from jax import lax
from jax.experimental import pallas as pl
from jax.experimental.pallas import tpu as pltpu
from jax.sharding import Mesh
from jax.sharding import PartitionSpec as P

F32, BF16, I32 = jnp.float32, jnp.bfloat16, jnp.int32
NT = (((1,), (1,)), ((), ()))
MESH = pl.DeviceIdType.MESH
LANES = 128
CAM = 9
BINS = 64
UNROLL = 4


def thirds(value):
    high = value.astype(BF16)
    rest = value - high.astype(F32)
    middle = rest.astype(BF16)
    return high, middle, (rest - middle.astype(F32)).astype(BF16)


def row_of(ref, start, count):
    return jnp.concatenate([ref[pl.ds(start + k, 1), :] for k in range(count)], axis=1)


def pair_sum(product):
    return product + pltpu.roll(product, product.shape[0] - 1, 0)


def one_hot(count, index):
    shape = (count, index.shape[1])
    return (lax.broadcasted_iota(I32, shape, 0) == index).astype(F32).astype(BF16)


def push_bins(tile, pos_ref):
    for unit in range(2):
        pos = row_of(pos_ref, tile * 4 + unit * 2, 2)
        lo = (((pos >> 11) & 1) << 7) + (pos & 127)
        pltpu.matmul_push_rhs(one_hot(2 * LANES, lo), 0, unit, transpose=True)


def split_lines(tile, factor, cam_ref, line_ref):
    rows = pl.ds(pl.multiple_of(tile * 8, 8), 8)
    for m in range(CAM):
        value = pair_sum(cam_ref[m, rows, :] * factor)
        high = value.astype(BF16).astype(F32)
        line_ref[0, m] = high
        line_ref[1, m] = value - high


def add_lines(tile, pos_ref, line_ref, accs):
    hots = []
    for unit in range(2):
        owner = row_of(pos_ref, tile * 4 + unit * 2, 2) >> 7
        hots.append(one_hot(BINS, ((owner >> 5) << 4) + (owner & 15)))
    for part in range(2):
        for m in range(CAM):
            for unit in range(2):
                pieces = []
                for q in range(2):
                    row = 2 * (2 * unit + q)
                    line = jnp.broadcast_to(line_ref[part, m, row : row + 1], (16, LANES)).astype(BF16)
                    hot = hots[unit][:, q * LANES : (q + 1) * LANES].reshape(BINS // 16, 16, LANES)
                    pieces.append((hot * line[None]).reshape(BINS, LANES))
                lhs = jnp.concatenate(pieces, axis=1)
                staged = 0 if part == 0 and m == 0 else None
                pltpu.matmul_acc_lhs(accs[unit * CAM + m], lhs, staged)


def empty_accs(accs):
    return [pltpu.matmul_pop(acc) for acc in accs]


def drain(accs, total_ref):
    for unit in range(2):
        pltpu.matmul_acc_lhs(accs[unit * CAM], jnp.zeros((BINS, 2 * LANES), BF16), 0)
    for m in range(CAM):
        total = pltpu.matmul_pop(accs[m]) + pltpu.matmul_pop(accs[CAM + m])
        total_ref[0, m * BINS : (m + 1) * BINS] = total[:, :LANES]
        total_ref[1, m * BINS : (m + 1) * BINS] = total[:, LANES:]


def regroup_into(out_ref, total_ref):
    def one(hi, _):
        for side in range(2):
            for g in range(3):
                rows = pl.ds(g * 3 * BINS + hi, 3, stride=BINS)
                out_ref[side, g, hi >> 4, (hi >> 2) & 3, hi & 3] = total_ref[side, rows, :]
        return 0

    lax.fori_loop(0, BINS, one, 0, unroll=4)


def is_block(offset, count):
    block = jnp.full((16, LANES), offset >> 7, I32)
    return [block == b for b in range(count)]


def solve_points(point_ref, damp_ref, step_ref):
    blocks = damp_ref.shape[0]
    damping = row_of(damp_ref, 0, blocks)

    def row(k):
        return jnp.concatenate([point_ref[b, k : k + 1, :] for b in range(blocks)], axis=1)

    g = [row(k) for k in range(3)]
    aa, ab, ac, bb, bc, cc = [row(k) for k in range(3, 9)]
    aa, bb, cc = aa + damping, bb + damping, cc + damping
    cof_aa = bb * cc - bc * bc
    cof_ab = ac * bc - ab * cc
    cof_ac = ab * bc - ac * bb
    cof_bb = aa * cc - ac * ac
    cof_bc = ab * ac - aa * bc
    cof_cc = aa * bb - ab * ab
    determ = aa * cof_aa + ab * cof_ab + ac * cof_ac
    steps = [
        (cof_aa * g[0] + cof_ab * g[1] + cof_ac * g[2]) / determ,
        (cof_ab * g[0] + cof_bb * g[1] + cof_bc * g[2]) / determ,
        (cof_ac * g[0] + cof_bc * g[1] + cof_cc * g[2]) / determ,
    ]
    step_ref[...] = jnp.zeros_like(step_ref)
    for k in range(3):
        for p, part in enumerate(thirds(steps[k])):
            value = part.astype(F32)
            for b in range(blocks):
                step_ref[b, 3 * p + k : 3 * p + k + 1, :] = value[:, b * LANES : (b + 1) * LANES]
    return jnp.sum(g[0] * g[0] + g[1] * g[1] + g[2] * g[2])


def first_tiles(
    offset_ref,
    res_ref,
    cam_ref,
    pt_ref,
    camera_ref,
    slot_ref,
    table_ref,
    pos_ref,
    index_ref,
    feat_ref,
    point_ref,
    line_ref,
    point_accs,
    accs,
):
    tiles = res_ref.shape[0] // 8
    blocks = point_ref.shape[0]
    point_ref[...] = jnp.zeros_like(point_ref)
    feat_ref[...] = jnp.zeros_like(feat_ref)

    def find(tile):
        lines = pl.ds(pl.multiple_of(tile * 4, 4), 4)
        camera = camera_ref[lines, :]
        high, low = camera >> 7, camera & 127
        found = [jnp.zeros_like(camera)] * 4
        for k in range(table_ref.shape[0]):
            line = jnp.broadcast_to(table_ref[k : k + 1, :], camera.shape)
            taken = jnp.take_along_axis(line, low, axis=1, mode="promise_in_bounds")
            found[k % 4] = jnp.where(high == k, taken, found[k % 4])
        pos_ref[lines, :] = (found[0] + found[1]) + (found[2] + found[3])

    def residual_of(tile):
        return res_ref[pl.ds(pl.multiple_of(tile * 8, 8), 8), :]

    def add_points(tile):
        rows = pl.ds(pl.multiple_of(tile * 8, 8), 8)
        r = residual_of(tile)
        j = [pt_ref[k, rows, :] for k in range(3)]
        products = [j[0] * r, j[1] * r, j[2] * r]
        products += [j[0] * j[0], j[0] * j[1], j[0] * j[2]]
        products += [j[1] * j[1], j[1] * j[2], j[2] * j[2]]
        for f, product in enumerate(products):
            feat_ref[f * 8 : f * 8 + 8, :] = pair_sum(product)
        offset = offset_ref[tile]
        lines = pl.ds(pl.multiple_of(tile * 4, 4), 4)
        index_ref[lines, :] = slot_ref[lines, :] + (offset & 127)
        index = row_of(index_ref, tile * 4, 4)
        for unit in range(2):
            columns = [feat_ref[pl.ds(4 * unit + 2 * q, 16, stride=8), :] for q in range(2)]
            lhs = jnp.concatenate(thirds(jnp.concatenate(columns, axis=1)), axis=0)
            hot = one_hot(2 * LANES, index[:, unit * 2 * LANES : (unit + 1) * 2 * LANES])
            pltpu.matmul_push_rhs(hot, 1, unit, transpose=True)
            pltpu.matmul_acc_lhs(point_accs[unit], lhs, 1)
        return is_block(offset, blocks - 1)

    find(0)
    push_bins(0, pos_ref)
    split_lines(0, residual_of(0), cam_ref, line_ref.at[0])

    def one_tile(tile, now, later):
        ahead = jnp.minimum(tile + 1, tiles - 1)
        add_lines(tile, pos_ref, line_ref.at[now], accs)
        here = add_points(tile)
        find(ahead)
        push_bins(ahead, pos_ref)
        split_lines(ahead, residual_of(ahead), cam_ref, line_ref.at[later])
        dots = pltpu.matmul_pop(point_accs[0]) + pltpu.matmul_pop(point_accs[1])
        dots = (dots[32:48] + dots[16:32]) + dots[0:16]
        left, right = dots[:, :LANES], dots[:, LANES:]
        for b in range(blocks):
            part = jnp.where(here[b - 1], right, 0.0) if b else jnp.zeros_like(left)
            point_ref[b] += jnp.where(here[b], left, part) if b < blocks - 1 else part

    def some_tiles(k, _):
        for s in range(UNROLL):
            one_tile(UNROLL * k + s, s % 2, 1 - s % 2)
        return 0

    lax.fori_loop(0, tiles // UNROLL, some_tiles, 0)


def move_start(tile, offset_ref, index_ref, step_ref, point_accs):
    index = row_of(index_ref, tile * 4, 4)
    blocks = step_ref.shape[0]
    here = is_block(offset_ref[tile], blocks - 1)
    left = right = jnp.zeros((16, LANES), F32)
    for b in range(blocks - 1):
        left = jnp.where(here[b], step_ref[b], left)
        right = jnp.where(here[b], step_ref[b + 1], right)
    lhs = jnp.concatenate([left, right], axis=1).astype(BF16)
    for unit in range(2):
        hot = one_hot(2 * LANES, index[:, unit * 2 * LANES : (unit + 1) * 2 * LANES])
        pltpu.matmul_push_rhs(hot, 1, unit)
        pltpu.matmul_acc_lhs(point_accs[unit], lhs, 1)


def move_end(tile, pt_ref, res_ref, moved_ref, point_accs):
    for unit in range(2):
        dots = pltpu.matmul_pop(point_accs[unit])
        taken = (dots[6:9] + dots[3:6]) + dots[0:3]
        for q in range(2):
            piece = taken[:, q * LANES : (q + 1) * LANES]
            for a in range(2):
                row = tile * 8 + 2 * (2 * unit + q) + a
                jac = jnp.concatenate([pt_ref[k, pl.ds(row, 1), :] for k in range(3)], axis=0)
                moved = jnp.sum(jac * piece, axis=0, keepdims=True)
                moved_ref[pl.ds(row, 1), :] = moved - res_ref[pl.ds(row, 1), :]


def second_start(offset_ref, index_ref, step_ref, pt_ref, res_ref, moved_ref, pos_ref, cam_ref, line_ref, point_accs, accs):
    for tile in range(2):
        move_start(tile, offset_ref, index_ref, step_ref, point_accs)
        move_end(tile, pt_ref, res_ref, moved_ref, point_accs)
    push_bins(0, pos_ref)
    split_lines(0, moved_ref[0:8, :], cam_ref, line_ref.at[0])


def second_tiles(
    first, last, offset_ref, index_ref, step_ref, pt_ref, res_ref, moved_ref, pos_ref, cam_ref, line_ref, point_accs, accs
):
    tiles = res_ref.shape[0] // 8

    def one_tile(tile, now, later):
        ahead = jnp.minimum(tile + 1, tiles - 1)
        after = jnp.minimum(tile + 2, tiles - 1)
        add_lines(tile, pos_ref, line_ref.at[now], accs)
        move_start(after, offset_ref, index_ref, step_ref, point_accs)
        push_bins(ahead, pos_ref)
        factor = moved_ref[pl.ds(pl.multiple_of(ahead * 8, 8), 8), :]
        split_lines(ahead, factor, cam_ref, line_ref.at[later])
        move_end(after, pt_ref, res_ref, moved_ref, point_accs)

    def some_tiles(k, _):
        for s in range(UNROLL):
            one_tile(UNROLL * k + s, s % 2, 1 - s % 2)
        return 0

    lax.fori_loop(first // UNROLL, last // UNROLL, some_tiles, 0)


def scoped(kernel, shapes):
    def whole(*refs):
        pl.run_scoped(lambda *accs: kernel(*refs, *accs), *shapes())

    return whole


def acc_shapes():
    sums = [pltpu.ACC(unit)((48, 2 * LANES), F32) for unit in range(2)]
    takes = [pltpu.ACC(unit)((16, 2 * LANES), F32) for unit in range(2)]
    return sums + takes + [pltpu.ACC(unit)((BINS, 2 * LANES), F32) for unit in range(2) for _ in range(CAM)]


def row_major(array):
    rows, n_obs = array.shape[1:-1], array.shape[-1]
    blocks = array.reshape(2, *rows, n_obs // LANES, LANES)
    blocks = jnp.moveaxis(blocks, 0, -2)
    return blocks.reshape(*rows, 2 * n_obs // LANES, LANES)


AXES = ("gx_0", "gx_1", "gy_0", "gy_1")
RINGS = ("gx_0", "gy_0", "gy_1")
ORDERS = ((0, 1, 2), (1, 2, 0), (2, 0, 1))
SPOTS = (0, 1, 0)


def neighbours(me, names, sizes):
    total = 1
    for name in names:
        total *= sizes[name]
    place = 0
    for name in names:
        place = place * sizes[name] + me[name]
    found = []
    for k in range(1, total):
        other = lax.rem(place + k, total)
        target = dict(me)
        for name in reversed(names):
            target[name] = lax.rem(other, sizes[name])
            other = other // sizes[name]
        found.append(tuple(target[name] for name in AXES))
    return found


def inside(position, index):
    return (slice(None),) * position + (index,)


def whole_kernel(
    sizes,
    scale,
    offset_ref,
    res_ref,
    cam_ref,
    pt_ref,
    camera_ref,
    slot_ref,
    damp_ref,
    table_ref,
    reduced_ref,
    cost_ref,
    norm_ref,
    pos_ref,
    index_ref,
    feat_ref,
    point_ref,
    step_ref,
    moved_ref,
    line_ref,
    total_ref,
    grad_ref,
    move_ref,
    pair_ref,
    whole_ref,
    in1_ref,
    sum1_ref,
    in2_ref,
    sum2_ref,
    in3_ref,
    mine_ref,
    far_ref,
    plane_ref,
    near_ref,
    pair_send,
    pair_recv,
    ring_send,
    ring_recv,
    far_send,
    far_recv,
    near_send,
    near_recv,
    *accs,
):
    me = {name: lax.axis_index(name) for name in AXES}
    far = neighbours(me, ("gx_0", "gx_1"), sizes)
    near = neighbours(me, ("gy_0", "gy_1"), sizes)
    rings = [neighbours(me, (name,), sizes) for name in RINGS]
    core = me["gx_1"]
    partner = (me["gx_0"], 1 - core, me["gy_0"], me["gy_1"])

    barrier = pltpu.get_barrier_semaphore()
    for target in far + near:
        pl.semaphore_signal(barrier, inc=1, device_id=target, device_id_type=MESH)

    started = []

    def send(source, target_ref, send_sem, recv_sem, device):
        copy = pltpu.make_async_remote_copy(
            src_ref=source,
            dst_ref=target_ref,
            send_sem=send_sem,
            recv_sem=recv_sem,
            device_id=device,
            device_id_type=MESH,
        )
        copy.start()
        started.append(copy)
        return copy

    def spread(source, inbox, job, group, phase, position):
        ring = ORDERS[group][phase]
        name = RINGS[ring]
        copies = []
        for k, device in enumerate(rings[ring]):
            there = device[AXES.index(name)]
            copies.append(
                send(
                    source.at[(job, group) + inside(position, there)],
                    inbox.at[job, group, k],
                    ring_send.at[job, group, phase, k],
                    ring_recv.at[job, group, phase, k],
                    device,
                )
            )
        return copies

    def gather(source, inbox, copies, job, group, phase, position):
        for copy in copies:
            copy.wait_recv()
        here = me[RINGS[ORDERS[group][phase]]]
        kept = source[(job, group) + inside(position, here)]
        return (kept + inbox[job, group, 1]) + (inbox[job, group, 0] + inbox[job, group, 2])

    flight = {}

    def pairs(job, source):
        flight[job] = [
            send(
                source.at[1 - core, g],
                pair_ref.at[job, g],
                pair_send.at[job, g],
                pair_recv.at[job, g],
                partner,
            )
            for g in range(3)
        ]

    def phase_one(job, source):
        copies = flight[job]
        flight[job] = []
        for g in range(3):
            copies[g].wait_recv()
            whole_ref[job, g] = source[core, g] + pair_ref[job, g]
            flight[job].append(spread(whole_ref, in1_ref, job, g, 0, ORDERS[g][0]))

    def phase_two(job):
        copies = flight[job]
        flight[job] = []
        for g in range(3):
            sum1_ref[job, g] = gather(whole_ref, in1_ref, copies[g], job, g, 0, ORDERS[g][0])
            flight[job].append(spread(sum1_ref, in2_ref, job, g, 1, SPOTS[g]))

    def phase_three(job):
        copies = flight[job]
        flight[job] = []
        for g in range(3):
            sum2_ref[job, g] = gather(sum1_ref, in2_ref, copies[g], job, g, 1, SPOTS[g])
            flight[job].append(spread(sum2_ref, in3_ref, job, g, 2, 0))

    def finish(job):
        own = [gather(sum2_ref, in3_ref, flight[job][g], job, g, 2, 0) for g in range(3)]
        return jnp.concatenate(own, axis=0)

    sum_accs, take_accs, accs = accs[:2], accs[2:4], accs[4:]
    empty_accs(sum_accs + take_accs + accs)
    first_tiles(
        offset_ref,
        res_ref,
        cam_ref,
        pt_ref,
        camera_ref,
        slot_ref,
        table_ref,
        pos_ref,
        index_ref,
        feat_ref,
        point_ref,
        line_ref,
        sum_accs,
        accs,
    )
    drain(accs, total_ref)
    regroup_into(grad_ref, total_ref)
    pl.semaphore_wait(barrier, len(far) + len(near))
    pairs(0, grad_ref)
    point_square = solve_points(point_ref, damp_ref, step_ref)
    residual = res_ref[...]
    square = jnp.sum(residual * residual)
    lane = lax.broadcasted_iota(I32, mine_ref.shape, 1)
    refs = (
        offset_ref,
        index_ref,
        step_ref,
        pt_ref,
        res_ref,
        moved_ref,
        pos_ref,
        cam_ref,
        line_ref,
        take_accs,
        accs,
    )
    second_start(*refs)
    second_tiles(0, 8, *refs)
    phase_one(0, grad_ref)
    second_tiles(8, 16, *refs)
    phase_two(0)
    second_tiles(16, 24, *refs)
    phase_three(0)
    second_tiles(24, 32, *refs)
    drain(accs, total_ref)
    regroup_into(move_ref, total_ref)
    pairs(1, move_ref)
    phase_one(1, move_ref)
    grads = finish(0)
    gradient_square = point_square + jnp.sum(grads * grads)
    mine_ref[...] = jnp.where(lane == 0, square, jnp.where(lane == 1, gradient_square, 0.0))
    arrivals = [
        send(mine_ref, far_ref.at[k], far_send.at[k], far_recv.at[k], device)
        for k, device in enumerate(far)
    ]
    phase_two(1)
    for copy in arrivals:
        copy.wait_recv()
    plane_ref[...] = mine_ref[...] + jnp.sum(far_ref[...], axis=0)
    arrivals = [
        send(plane_ref, near_ref.at[k], near_send.at[k], near_recv.at[k], device)
        for k, device in enumerate(near)
    ]
    phase_three(1)
    for copy in arrivals:
        copy.wait_recv()
    totals = plane_ref[...] + jnp.sum(near_ref[...], axis=0)
    first_row = lax.broadcasted_iota(I32, mine_ref.shape, 0) == 0
    cost = totals / scale[0]
    norm = jnp.sqrt(totals / scale[1] + 1e-06)
    cost_ref[0, 0] = jnp.sum(jnp.where(first_row & (lane == 0), cost, 0.0))
    norm_ref[0, 0] = jnp.sum(jnp.where(first_row & (lane == 1), norm, 0.0))
    reduced_ref[...] = finish(1)
    for copy in started:
        copy.wait_send()


def whole(
    residual, cam_jacobian, point_jacobian, obs_camera, obs_slot, tile_offset, damping, camera_slot, sizes, scale
):
    vmem = pl.BlockSpec(memory_space=pltpu.VMEM)
    smem = pl.BlockSpec(memory_space=pltpu.SMEM)
    rows = CAM // 3
    buffer = lambda *lead: pltpu.VMEM(lead + (rows, LANES), F32)
    dma = pltpu.SemaphoreType.DMA
    far = sizes["gx_0"] * sizes["gx_1"] - 1
    near = sizes["gy_0"] * sizes["gy_1"] - 1
    return pl.pallas_call(
        scoped(functools.partial(whole_kernel, sizes, scale), acc_shapes),
        out_shape=(
            jax.ShapeDtypeStruct((CAM, LANES), F32),
            jax.ShapeDtypeStruct((1, 1), F32),
            jax.ShapeDtypeStruct((1, 1), F32),
        ),
        in_specs=[smem] + [vmem] * 7,
        out_specs=(vmem, smem, smem),
        scratch_shapes=[
            pltpu.VMEM(obs_camera.shape, I32),
            pltpu.VMEM(obs_camera.shape, I32),
            pltpu.VMEM((16 * 8, LANES), F32),
            pltpu.VMEM((damping.shape[0] + 1, 16, LANES), F32),
            pltpu.VMEM((damping.shape[0] + 1, 16, LANES), F32),
            pltpu.VMEM(residual.shape, F32),
            pltpu.VMEM((2, 2, CAM, 8, LANES), F32),
            pltpu.VMEM((2, CAM * BINS, LANES), F32),
            buffer(2, 3, 4, 4, 4),
            buffer(2, 3, 4, 4, 4),
            buffer(2, 3, 4, 4, 4),
            buffer(2, 3, 4, 4, 4),
            buffer(2, 3, 3, 4, 4),
            buffer(2, 3, 4, 4),
            buffer(2, 3, 3, 4),
            buffer(2, 3, 4),
            buffer(2, 3, 3),
            pltpu.VMEM((8, LANES), F32),
            pltpu.VMEM((far, 8, LANES), F32),
            pltpu.VMEM((8, LANES), F32),
            pltpu.VMEM((near, 8, LANES), F32),
            dma((2, 3)),
            dma((2, 3)),
            dma((2, 3, 3, 3)),
            dma((2, 3, 3, 3)),
            dma((far,)),
            dma((far,)),
            dma((near,)),
            dma((near,)),
        ],
        compiler_params=pltpu.CompilerParams(collective_id=0, has_side_effects=True),
    )(tile_offset, residual, cam_jacobian, point_jacobian, obs_camera, obs_slot, damping, camera_slot)


def on_device(
    residual, cam_jacobian, point_jacobian, obs_camera, obs_slot, tile_offset, damping, camera_slot
):
    n_obs = residual.shape[1]
    sizes = {name: lax.axis_size(name) for name in AXES}
    devices = lax.axis_size(AXES)
    scale = (2.0 * n_obs * devices, 9.0 * camera_slot.shape[0] + 3.0 * damping.shape[0] * devices)
    lines = lambda array: array.reshape(-1, LANES)
    res, cam, pt = row_major(residual), row_major(cam_jacobian), row_major(point_jacobian)
    reduced, cost, norm = whole(
        res, cam, pt, lines(obs_camera), lines(obs_slot), tile_offset, lines(damping), lines(camera_slot), sizes, scale
    )
    return (reduced, cost.reshape(()), norm.reshape(()))


def solution(mesh):
    finer = Mesh(mesh.devices.reshape(4, 2, 4, 4), AXES)
    in_specs = (
        P(None, AXES),
        P(None, None, AXES),
        P(None, None, AXES),
        P(AXES),
        P(AXES),
        P(AXES),
        P(AXES),
        P(),
    )
    out_specs = (P(None, AXES), P(), P())
    return jax.shard_map(
        on_device, mesh=finer, in_specs=in_specs, out_specs=out_specs, check_vma=False
    )
```

```python
import functools

import jax
import jax.numpy as jnp
from jax import lax
from jax.experimental import pallas as pl
from jax.experimental.pallas import tpu as pltpu
from jax.sharding import Mesh
from jax.sharding import PartitionSpec as P

F32, BF16, I32 = jnp.float32, jnp.bfloat16, jnp.int32
NT = (((1,), (1,)), ((), ()))
MESH = pl.DeviceIdType.MESH
LANES = 128
CAM = 9
BINS = 64
PITCH = 72
UNROLL = 8


def thirds(value):
    high = value.astype(BF16)
    rest = value - high.astype(F32)
    middle = rest.astype(BF16)
    return high, middle, (rest - middle.astype(F32)).astype(BF16)


def row_of(ref, start, count):
    return jnp.concatenate([ref[pl.ds(start + k, 1), :] for k in range(count)], axis=1)


def pair_sum(product):
    return product + pltpu.roll(product, product.shape[0] - 1, 0)


def one_hot(count, index):
    shape = (count, index.shape[1])
    return (lax.broadcasted_iota(I32, shape, 0) == index).astype(F32).astype(BF16)


def push_bins(tile, pos_ref):
    for unit in range(2):
        pos = row_of(pos_ref, tile * 4 + unit * 2, 2)
        lo = (((pos >> 11) & 1) << 7) + (pos & 127)
        pltpu.matmul_push_rhs(one_hot(2 * LANES, lo), 0, unit, transpose=True)


def split_lines(tile, factor, cam_ref, line_ref):
    rows = pl.ds(pl.multiple_of(tile * 8, 8), 8)
    for m in range(CAM):
        value = pair_sum(cam_ref[m, rows, :] * factor)
        high = value.astype(BF16).astype(F32)
        line_ref[0, m] = high
        line_ref[1, m] = value - high


def add_lines(tile, pos_ref, line_ref, accs):
    hots = []
    for unit in range(2):
        owner = row_of(pos_ref, tile * 4 + unit * 2, 2) >> 7
        hots.append(one_hot(BINS, ((owner >> 5) << 4) + (owner & 15)))
    for part in range(2):
        for m in range(CAM):
            for unit in range(2):
                pieces = []
                for q in range(2):
                    row = 2 * (2 * unit + q)
                    line = jnp.broadcast_to(line_ref[part, m, row : row + 1], (16, LANES)).astype(BF16)
                    hot = hots[unit][:, q * LANES : (q + 1) * LANES].reshape(BINS // 16, 16, LANES)
                    pieces.append((hot * line[None]).reshape(BINS, LANES))
                lhs = jnp.concatenate(pieces, axis=1)
                staged = 0 if part == 0 and m == 0 else None
                pltpu.matmul_acc_lhs(accs[unit * CAM + m], lhs, staged)


def empty_accs(accs):
    return [pltpu.matmul_pop(acc) for acc in accs]


def drain(accs, total_ref):
    for unit in range(2):
        pltpu.matmul_acc_lhs(accs[unit * CAM], jnp.zeros((BINS, 2 * LANES), BF16), 0)
    for m in range(CAM):
        total = pltpu.matmul_pop(accs[m]) + pltpu.matmul_pop(accs[CAM + m])
        total_ref[0, m * PITCH : m * PITCH + BINS] = total[:, :LANES]
        total_ref[1, m * PITCH : m * PITCH + BINS] = total[:, LANES:]


def regroup_into(out_ref, total_ref):
    def one(hi, _):
        for side in range(2):
            rows = pl.ds(hi, CAM, stride=PITCH)
            out_ref[side, hi >> 4, (hi >> 2) & 3, hi & 3] = total_ref[side, rows, :]
        return 0

    lax.fori_loop(0, BINS, one, 0, unroll=4)


def is_block(offset, count):
    block = jnp.full((16, LANES), offset >> 7, I32)
    return [block == b for b in range(count)]


def solve_points(point_ref, damp_ref, step_ref):
    blocks = damp_ref.shape[0]
    damping = row_of(damp_ref, 0, blocks)

    def row(k):
        return jnp.concatenate([point_ref[b, k : k + 1, :] for b in range(blocks)], axis=1)

    g = [row(k) for k in range(3)]
    aa, ab, ac, bb, bc, cc = [row(k) for k in range(3, 9)]
    aa, bb, cc = aa + damping, bb + damping, cc + damping
    cof_aa = bb * cc - bc * bc
    cof_ab = ac * bc - ab * cc
    cof_ac = ab * bc - ac * bb
    cof_bb = aa * cc - ac * ac
    cof_bc = ab * ac - aa * bc
    cof_cc = aa * bb - ab * ab
    determ = aa * cof_aa + ab * cof_ab + ac * cof_ac
    steps = [
        (cof_aa * g[0] + cof_ab * g[1] + cof_ac * g[2]) / determ,
        (cof_ab * g[0] + cof_bb * g[1] + cof_bc * g[2]) / determ,
        (cof_ac * g[0] + cof_bc * g[1] + cof_cc * g[2]) / determ,
    ]
    step_ref[...] = jnp.zeros_like(step_ref)
    for k in range(3):
        for p, part in enumerate(thirds(steps[k])):
            value = part.astype(F32)
            for b in range(blocks):
                step_ref[b, 3 * p + k : 3 * p + k + 1, :] = value[:, b * LANES : (b + 1) * LANES]
    return jnp.sum(g[0] * g[0] + g[1] * g[1] + g[2] * g[2])


def first_tiles(
    offset_ref,
    res_ref,
    cam_ref,
    pt_ref,
    camera_ref,
    slot_ref,
    table_ref,
    pos_ref,
    index_ref,
    feat_ref,
    point_ref,
    line_ref,
    point_accs,
    accs,
):
    tiles = res_ref.shape[0] // 8
    blocks = point_ref.shape[0]
    point_ref[...] = jnp.zeros_like(point_ref)
    feat_ref[...] = jnp.zeros_like(feat_ref)

    def find(tile):
        lines = pl.ds(pl.multiple_of(tile * 4, 4), 4)
        camera = camera_ref[lines, :]
        high, low = camera >> 7, camera & 127
        found = [jnp.zeros_like(camera)] * 4
        for k in range(table_ref.shape[0]):
            line = jnp.broadcast_to(table_ref[k : k + 1, :], camera.shape)
            taken = jnp.take_along_axis(line, low, axis=1, mode="promise_in_bounds")
            found[k % 4] = jnp.where(high == k, taken, found[k % 4])
        pos_ref[lines, :] = (found[0] + found[1]) + (found[2] + found[3])

    def residual_of(tile):
        return res_ref[pl.ds(pl.multiple_of(tile * 8, 8), 8), :]

    def add_points(tile):
        rows = pl.ds(pl.multiple_of(tile * 8, 8), 8)
        r = residual_of(tile)
        j = [pt_ref[k, rows, :] for k in range(3)]
        products = [j[0] * r, j[1] * r, j[2] * r]
        products += [j[0] * j[0], j[0] * j[1], j[0] * j[2]]
        products += [j[1] * j[1], j[1] * j[2], j[2] * j[2]]
        for f, product in enumerate(products):
            feat_ref[f * 8 : f * 8 + 8, :] = pair_sum(product)
        offset = offset_ref[tile]
        lines = pl.ds(pl.multiple_of(tile * 4, 4), 4)
        index_ref[lines, :] = slot_ref[lines, :] + (offset & 127)
        index = row_of(index_ref, tile * 4, 4)
        for unit in range(2):
            columns = [feat_ref[pl.ds(4 * unit + 2 * q, 16, stride=8), :] for q in range(2)]
            lhs = jnp.concatenate(thirds(jnp.concatenate(columns, axis=1)), axis=0)
            hot = one_hot(2 * LANES, index[:, unit * 2 * LANES : (unit + 1) * 2 * LANES])
            pltpu.matmul_push_rhs(hot, 1, unit, transpose=True)
            pltpu.matmul_acc_lhs(point_accs[unit], lhs, 1)
        return is_block(offset, blocks - 1)

    find(0)
    push_bins(0, pos_ref)
    split_lines(0, residual_of(0), cam_ref, line_ref.at[0])

    def one_tile(tile, now, later):
        ahead = jnp.minimum(tile + 1, tiles - 1)
        add_lines(tile, pos_ref, line_ref.at[now], accs)
        here = add_points(tile)
        find(ahead)
        push_bins(ahead, pos_ref)
        split_lines(ahead, residual_of(ahead), cam_ref, line_ref.at[later])
        dots = pltpu.matmul_pop(point_accs[0]) + pltpu.matmul_pop(point_accs[1])
        dots = (dots[32:48] + dots[16:32]) + dots[0:16]
        left, right = dots[:, :LANES], dots[:, LANES:]
        for b in range(blocks):
            part = jnp.where(here[b - 1], right, 0.0) if b else jnp.zeros_like(left)
            point_ref[b] += jnp.where(here[b], left, part) if b < blocks - 1 else part

    def some_tiles(k, _):
        for s in range(UNROLL):
            one_tile(UNROLL * k + s, s % 2, 1 - s % 2)
        return 0

    lax.fori_loop(0, tiles // UNROLL, some_tiles, 0)


def move_start(tile, offset_ref, index_ref, step_ref, point_accs):
    index = row_of(index_ref, tile * 4, 4)
    blocks = step_ref.shape[0]
    here = is_block(offset_ref[tile], blocks - 1)
    left = right = jnp.zeros((16, LANES), F32)
    for b in range(blocks - 1):
        left = jnp.where(here[b], step_ref[b], left)
        right = jnp.where(here[b], step_ref[b + 1], right)
    lhs = jnp.concatenate([left, right], axis=1).astype(BF16)
    for unit in range(2):
        hot = one_hot(2 * LANES, index[:, unit * 2 * LANES : (unit + 1) * 2 * LANES])
        pltpu.matmul_push_rhs(hot, 1, unit)
        pltpu.matmul_acc_lhs(point_accs[unit], lhs, 1)


def move_end(tile, pt_ref, res_ref, moved_ref, point_accs):
    for unit in range(2):
        dots = pltpu.matmul_pop(point_accs[unit])
        taken = (dots[6:9] + dots[3:6]) + dots[0:3]
        for q in range(2):
            piece = taken[:, q * LANES : (q + 1) * LANES]
            for a in range(2):
                row = tile * 8 + 2 * (2 * unit + q) + a
                jac = jnp.concatenate([pt_ref[k, pl.ds(row, 1), :] for k in range(3)], axis=0)
                moved = jnp.sum(jac * piece, axis=0, keepdims=True)
                moved_ref[pl.ds(row, 1), :] = moved - res_ref[pl.ds(row, 1), :]


def second_start(offset_ref, index_ref, step_ref, pt_ref, res_ref, moved_ref, pos_ref, cam_ref, line_ref, point_accs, accs):
    for tile in range(2):
        move_start(tile, offset_ref, index_ref, step_ref, point_accs)
        move_end(tile, pt_ref, res_ref, moved_ref, point_accs)
    push_bins(0, pos_ref)
    split_lines(0, moved_ref[0:8, :], cam_ref, line_ref.at[0])


def second_tiles(
    first, last, offset_ref, index_ref, step_ref, pt_ref, res_ref, moved_ref, pos_ref, cam_ref, line_ref, point_accs, accs
):
    tiles = res_ref.shape[0] // 8

    def one_tile(tile, now, later):
        ahead = jnp.minimum(tile + 1, tiles - 1)
        after = jnp.minimum(tile + 2, tiles - 1)
        add_lines(tile, pos_ref, line_ref.at[now], accs)
        move_start(after, offset_ref, index_ref, step_ref, point_accs)
        push_bins(ahead, pos_ref)
        factor = moved_ref[pl.ds(pl.multiple_of(ahead * 8, 8), 8), :]
        split_lines(ahead, factor, cam_ref, line_ref.at[later])
        move_end(after, pt_ref, res_ref, moved_ref, point_accs)

    def some_tiles(k, _):
        for s in range(UNROLL):
            one_tile(UNROLL * k + s, s % 2, 1 - s % 2)
        return 0

    lax.fori_loop(first // UNROLL, last // UNROLL, some_tiles, 0)


def scoped(kernel, shapes):
    def whole(*refs):
        pl.run_scoped(lambda *accs: kernel(*refs, *accs), *shapes())

    return whole


def acc_shapes():
    sums = [pltpu.ACC(unit)((48, 2 * LANES), F32) for unit in range(2)]
    takes = [pltpu.ACC(unit)((16, 2 * LANES), F32) for unit in range(2)]
    return sums + takes + [pltpu.ACC(unit)((BINS, 2 * LANES), F32) for unit in range(2) for _ in range(CAM)]


def row_major(array):
    rows, n_obs = array.shape[1:-1], array.shape[-1]
    blocks = array.reshape(2, *rows, n_obs // LANES, LANES)
    blocks = jnp.moveaxis(blocks, 0, -2)
    return blocks.reshape(*rows, 2 * n_obs // LANES, LANES)


AXES = ("gx_0", "gx_1", "gy_0", "gy_1")
HOPS = (0, 1, 2, 1)
SLABS = (2, 1, 3, 0)


def neighbours(me, names, sizes):
    total = 1
    for name in names:
        total *= sizes[name]
    place = 0
    for name in names:
        place = place * sizes[name] + me[name]
    found = []
    for k in range(1, total):
        other = lax.rem(place + k, total)
        target = dict(me)
        for name in reversed(names):
            target[name] = lax.rem(other, sizes[name])
            other = other // sizes[name]
        found.append(tuple(target[name] for name in AXES))
    return found


def slab_offsets(dx):
    found = [(dx, dy, dz) for dy in range(4) for dz in range(4) if (dx, dy, dz) != (0, 0, 0)]
    return sorted(found, key=lambda offset: -sum(HOPS[d] for d in offset))


def whole_kernel(
    sizes,
    scale,
    offset_ref,
    res_ref,
    cam_ref,
    pt_ref,
    camera_ref,
    slot_ref,
    damp_ref,
    table_ref,
    kept_ref,
    rest_ref,
    cost_ref,
    norm_ref,
    pos_ref,
    index_ref,
    feat_ref,
    point_ref,
    step_ref,
    moved_ref,
    line_ref,
    total_ref,
    grad_ref,
    move_ref,
    pair_ref,
    whole_ref,
    inbox_ref,
    mine_ref,
    far_ref,
    plane_ref,
    near_ref,
    pair_send,
    pair_recv,
    chip_send,
    chip_recv,
    far_send,
    far_recv,
    near_send,
    near_recv,
    *accs,
):
    me = {name: lax.axis_index(name) for name in AXES}
    far = neighbours(me, ("gx_0", "gx_1"), sizes)
    near = neighbours(me, ("gy_0", "gy_1"), sizes)
    core = me["gx_1"]
    partner = (me["gx_0"], 1 - core, me["gy_0"], me["gy_1"])

    barrier = pltpu.get_barrier_semaphore()
    chips = {}
    for dx in SLABS:
        for offset in slab_offsets(dx):
            place = [lax.rem(me[n] + d, sizes[n]) for n, d in zip(("gx_0", "gy_0", "gy_1"), offset)]
            chips[offset] = (place[0], core, place[1], place[2])
    others = [chips[o] for o in chips if o[0] and (o[1] or o[2])]
    for target in far + near + others:
        pl.semaphore_signal(barrier, inc=1, device_id=target, device_id_type=MESH)

    started = []

    def send(source, target_ref, send_sem, recv_sem, device):
        copy = pltpu.make_async_remote_copy(
            src_ref=source,
            dst_ref=target_ref,
            send_sem=send_sem,
            recv_sem=recv_sem,
            device_id=device,
            device_id_type=MESH,
        )
        copy.start()
        started.append(copy)
        return copy

    flight = {}

    def pairs(job, source):
        flight[job] = []
        for k, dx in enumerate(SLABS):
            there = lax.rem(me["gx_0"] + dx, sizes["gx_0"])
            flight[job].append(
                send(
                    source.at[1 - core, there],
                    pair_ref.at[job, there],
                    pair_send.at[job, k],
                    pair_recv.at[job, k],
                    partner,
                )
            )

    def spread(job, source):
        copies = flight[job]
        flight[job] = []
        for k, dx in enumerate(SLABS):
            there = lax.rem(me["gx_0"] + dx, sizes["gx_0"])
            copies[k].wait_recv()
            whole_ref[job, there] = source[core, there] + pair_ref[job, there]
            for offset in slab_offsets(dx):
                slot = (offset[0] * 4 + offset[1]) * 4 + offset[2] - 1
                device = chips[offset]
                flight[job].append(
                    send(
                        whole_ref.at[job, there, device[2], device[3]],
                        inbox_ref.at[job, slot],
                        chip_send.at[job, slot],
                        chip_recv.at[job, slot],
                        device,
                    )
                )

    def finish(job):
        for copy in flight[job]:
            copy.wait_recv()
        kept = whole_ref[job, me["gx_0"], me["gy_0"], me["gy_1"]]
        return kept, jnp.sum(inbox_ref[job], axis=0)

    sum_accs, take_accs, accs = accs[:2], accs[2:4], accs[4:]
    empty_accs(sum_accs + take_accs + accs)
    first_tiles(
        offset_ref,
        res_ref,
        cam_ref,
        pt_ref,
        camera_ref,
        slot_ref,
        table_ref,
        pos_ref,
        index_ref,
        feat_ref,
        point_ref,
        line_ref,
        sum_accs,
        accs,
    )
    drain(accs, total_ref)
    regroup_into(grad_ref, total_ref)
    pl.semaphore_wait(barrier, len(far) + len(near) + len(others))
    pairs(0, grad_ref)
    point_square = solve_points(point_ref, damp_ref, step_ref)
    residual = res_ref[...]
    square = jnp.sum(residual * residual)
    lane = lax.broadcasted_iota(I32, mine_ref.shape, 1)
    refs = (
        offset_ref,
        index_ref,
        step_ref,
        pt_ref,
        res_ref,
        moved_ref,
        pos_ref,
        cam_ref,
        line_ref,
        take_accs,
        accs,
    )
    second_start(*refs)
    second_tiles(0, 8, *refs)
    spread(0, grad_ref)
    second_tiles(8, 24, *refs)
    kept, rest = finish(0)
    grads = kept + rest
    gradient_square = point_square + jnp.sum(grads * grads)
    mine_ref[...] = jnp.where(lane == 0, square, jnp.where(lane == 1, gradient_square, 0.0))
    arrivals = [
        send(mine_ref, far_ref.at[k], far_send.at[k], far_recv.at[k], device)
        for k, device in enumerate(far)
    ]
    second_tiles(24, 32, *refs)
    drain(accs, total_ref)
    regroup_into(move_ref, total_ref)
    pairs(1, move_ref)
    for copy in arrivals:
        copy.wait_recv()
    plane_ref[...] = mine_ref[...] + jnp.sum(far_ref[...], axis=0)
    arrivals = [
        send(plane_ref, near_ref.at[k], near_send.at[k], near_recv.at[k], device)
        for k, device in enumerate(near)
    ]
    spread(1, move_ref)
    for copy in arrivals:
        copy.wait_recv()
    totals = plane_ref[...] + jnp.sum(near_ref[...], axis=0)
    first_row = lax.broadcasted_iota(I32, mine_ref.shape, 0) == 0
    cost = totals / scale[0]
    norm = jnp.sqrt(totals / scale[1] + 1e-06)
    cost_ref[0, 0] = jnp.sum(jnp.where(first_row & (lane == 0), cost, 0.0))
    norm_ref[0, 0] = jnp.sum(jnp.where(first_row & (lane == 1), norm, 0.0))
    kept_ref[...], rest_ref[...] = finish(1)
    for copy in started:
        copy.wait_send()


def whole(
    residual, cam_jacobian, point_jacobian, obs_camera, obs_slot, tile_offset, damping, camera_slot, sizes, scale
):
    vmem = pl.BlockSpec(memory_space=pltpu.VMEM)
    smem = pl.BlockSpec(memory_space=pltpu.SMEM)
    buffer = lambda *lead: pltpu.VMEM(lead + (CAM, LANES), F32)
    chips = sizes["gx_0"] * sizes["gy_0"] * sizes["gy_1"] - 1
    dma = pltpu.SemaphoreType.DMA
    far = sizes["gx_0"] * sizes["gx_1"] - 1
    near = sizes["gy_0"] * sizes["gy_1"] - 1
    return pl.pallas_call(
        scoped(functools.partial(whole_kernel, sizes, scale), acc_shapes),
        out_shape=(
            jax.ShapeDtypeStruct((CAM, LANES), F32),
            jax.ShapeDtypeStruct((CAM, LANES), F32),
            jax.ShapeDtypeStruct((1, 1), F32),
            jax.ShapeDtypeStruct((1, 1), F32),
        ),
        in_specs=[smem] + [vmem] * 7,
        out_specs=(vmem, vmem, smem, smem),
        scratch_shapes=[
            pltpu.VMEM(obs_camera.shape, I32),
            pltpu.VMEM(obs_camera.shape, I32),
            pltpu.VMEM((16 * 8, LANES), F32),
            pltpu.VMEM((damping.shape[0] + 1, 16, LANES), F32),
            pltpu.VMEM((damping.shape[0] + 1, 16, LANES), F32),
            pltpu.VMEM(residual.shape, F32),
            pltpu.VMEM((2, 2, CAM, 8, LANES), F32),
            pltpu.VMEM((2, CAM * PITCH, LANES), F32),
            buffer(2, 4, 4, 4),
            buffer(2, 4, 4, 4),
            buffer(2, 4, 4, 4),
            buffer(2, 4, 4, 4),
            buffer(2, chips),
            pltpu.VMEM((8, LANES), F32),
            pltpu.VMEM((far, 8, LANES), F32),
            pltpu.VMEM((8, LANES), F32),
            pltpu.VMEM((near, 8, LANES), F32),
            dma((2, 4)),
            dma((2, 4)),
            dma((2, chips)),
            dma((2, chips)),
            dma((far,)),
            dma((far,)),
            dma((near,)),
            dma((near,)),
        ],
        compiler_params=pltpu.CompilerParams(collective_id=0, has_side_effects=True),
    )(tile_offset, residual, cam_jacobian, point_jacobian, obs_camera, obs_slot, damping, camera_slot)


def on_device(
    residual, cam_jacobian, point_jacobian, obs_camera, obs_slot, tile_offset, damping, camera_slot
):
    n_obs = residual.shape[1]
    sizes = {name: lax.axis_size(name) for name in AXES}
    devices = lax.axis_size(AXES)
    scale = (2.0 * n_obs * devices, 9.0 * camera_slot.shape[0] + 3.0 * damping.shape[0] * devices)
    lines = lambda array: array.reshape(-1, LANES)
    res, cam, pt = row_major(residual), row_major(cam_jacobian), row_major(point_jacobian)
    kept, rest, cost, norm = whole(
        res, cam, pt, lines(obs_camera), lines(obs_slot), tile_offset, lines(damping), lines(camera_slot), sizes, scale
    )
    return (kept + rest, cost.reshape(()), norm.reshape(()))


def solution(mesh):
    finer = Mesh(mesh.devices.reshape(4, 2, 4, 4), AXES)
    in_specs = (
        P(None, AXES),
        P(None, None, AXES),
        P(None, None, AXES),
        P(AXES),
        P(AXES),
        P(AXES),
        P(AXES),
        P(),
    )
    out_specs = (P(None, AXES), P(), P())
    return jax.shard_map(
        on_device, mesh=finer, in_specs=in_specs, out_specs=out_specs, check_vma=False
    )
```

```python
import functools

import jax
import jax.numpy as jnp
from jax import lax
from jax.experimental import pallas as pl
from jax.experimental.pallas import tpu as pltpu
from jax.sharding import Mesh
from jax.sharding import PartitionSpec as P

F32, BF16, I32 = jnp.float32, jnp.bfloat16, jnp.int32
NT = (((1,), (1,)), ((), ()))
MESH = pl.DeviceIdType.MESH
LANES = 128
CAM = 9
BINS = 64
PITCH = 72
UNROLL = 8


def thirds(value):
    high = value.astype(BF16)
    rest = value - high.astype(F32)
    middle = rest.astype(BF16)
    return high, middle, (rest - middle.astype(F32)).astype(BF16)


def row_of(ref, start, count):
    return jnp.concatenate([ref[pl.ds(start + k, 1), :] for k in range(count)], axis=1)


def pair_sum(product):
    return product + pltpu.roll(product, product.shape[0] - 1, 0)


def one_hot(count, index):
    shape = (count, index.shape[1])
    return (lax.broadcasted_iota(I32, shape, 0) == index).astype(F32).astype(BF16)


def push_bins(tile, pos_ref):
    for unit in range(2):
        pos = row_of(pos_ref, tile * 4 + unit * 2, 2)
        lo = (((pos >> 11) & 1) << 7) + (pos & 127)
        pltpu.matmul_push_rhs(one_hot(2 * LANES, lo), 0, unit, transpose=True)


def split_lines(tile, factor, cam_ref, line_ref):
    rows = pl.ds(pl.multiple_of(tile * 8, 8), 8)
    for m in range(CAM):
        value = pair_sum(cam_ref[m, rows, :] * factor)
        high = value.astype(BF16).astype(F32)
        line_ref[0, m] = high
        line_ref[1, m] = value - high


def add_lines(tile, pos_ref, line_ref, accs):
    hots = []
    for unit in range(2):
        owner = row_of(pos_ref, tile * 4 + unit * 2, 2) >> 7
        hots.append(one_hot(BINS, ((owner >> 5) << 4) + (owner & 15)))
    for part in range(2):
        for m in range(CAM):
            for unit in range(2):
                pieces = []
                for q in range(2):
                    row = 2 * (2 * unit + q)
                    line = jnp.broadcast_to(line_ref[part, m, row : row + 1], (16, LANES)).astype(BF16)
                    hot = hots[unit][:, q * LANES : (q + 1) * LANES].reshape(BINS // 16, 16, LANES)
                    pieces.append((hot * line[None]).reshape(BINS, LANES))
                lhs = jnp.concatenate(pieces, axis=1)
                staged = 0 if part == 0 and m == 0 else None
                pltpu.matmul_acc_lhs(accs[unit * CAM + m], lhs, staged)


def empty_accs(accs):
    return [pltpu.matmul_pop(acc) for acc in accs]


def drain(accs, total_ref):
    for unit in range(2):
        pltpu.matmul_acc_lhs(accs[unit * CAM], jnp.zeros((BINS, 2 * LANES), BF16), 0)
    for m in range(CAM):
        total = pltpu.matmul_pop(accs[m]) + pltpu.matmul_pop(accs[CAM + m])
        total_ref[0, m * PITCH : m * PITCH + BINS] = total[:, :LANES]
        total_ref[1, m * PITCH : m * PITCH + BINS] = total[:, LANES:]


def regroup_into(out_ref, total_ref):
    def one(hi, _):
        for side in range(2):
            rows = pl.ds(hi, CAM, stride=PITCH)
            out_ref[side, hi >> 4, (hi >> 2) & 3, hi & 3] = total_ref[side, rows, :]
        return 0

    lax.fori_loop(0, BINS, one, 0, unroll=4)


def is_block(offset, count):
    block = jnp.full((16, LANES), offset >> 7, I32)
    return [block == b for b in range(count)]


def solve_points(point_ref, damp_ref, step_ref):
    blocks = damp_ref.shape[0]
    damping = row_of(damp_ref, 0, blocks)

    def row(k):
        return jnp.concatenate([point_ref[b, k : k + 1, :] for b in range(blocks)], axis=1)

    g = [row(k) for k in range(3)]
    aa, ab, ac, bb, bc, cc = [row(k) for k in range(3, 9)]
    aa, bb, cc = aa + damping, bb + damping, cc + damping
    cof_aa = bb * cc - bc * bc
    cof_ab = ac * bc - ab * cc
    cof_ac = ab * bc - ac * bb
    cof_bb = aa * cc - ac * ac
    cof_bc = ab * ac - aa * bc
    cof_cc = aa * bb - ab * ab
    determ = aa * cof_aa + ab * cof_ab + ac * cof_ac
    steps = [
        (cof_aa * g[0] + cof_ab * g[1] + cof_ac * g[2]) / determ,
        (cof_ab * g[0] + cof_bb * g[1] + cof_bc * g[2]) / determ,
        (cof_ac * g[0] + cof_bc * g[1] + cof_cc * g[2]) / determ,
    ]
    step_ref[...] = jnp.zeros_like(step_ref)
    for k in range(3):
        for p, part in enumerate(thirds(steps[k])):
            value = part.astype(F32)
            for b in range(blocks):
                step_ref[b, 3 * p + k : 3 * p + k + 1, :] = value[:, b * LANES : (b + 1) * LANES]
    return jnp.sum(g[0] * g[0] + g[1] * g[1] + g[2] * g[2])


def first_tiles(
    offset_ref,
    res_ref,
    cam_ref,
    pt_ref,
    camera_ref,
    slot_ref,
    table_ref,
    pos_ref,
    index_ref,
    feat_ref,
    point_ref,
    line_ref,
    point_accs,
    accs,
    loads,
):
    tiles = res_ref.shape[0] // 8
    blocks = point_ref.shape[0]
    point_ref[...] = jnp.zeros_like(point_ref)
    feat_ref[...] = jnp.zeros_like(feat_ref)

    def find(tile):
        lines = pl.ds(pl.multiple_of(tile * 4, 4), 4)
        camera = camera_ref[lines, :]
        high, low = camera >> 7, camera & 127
        found = [jnp.zeros_like(camera)] * 4
        for k in range(table_ref.shape[0]):
            line = jnp.broadcast_to(table_ref[k : k + 1, :], camera.shape)
            taken = jnp.take_along_axis(line, low, axis=1, mode="promise_in_bounds")
            found[k % 4] = jnp.where(high == k, taken, found[k % 4])
        pos_ref[lines, :] = (found[0] + found[1]) + (found[2] + found[3])

    def residual_of(tile):
        return res_ref[pl.ds(pl.multiple_of(tile * 8, 8), 8), :]

    def add_points(tile):
        rows = pl.ds(pl.multiple_of(tile * 8, 8), 8)
        r = residual_of(tile)
        j = [pt_ref[k, rows, :] for k in range(3)]
        products = [j[0] * r, j[1] * r, j[2] * r]
        products += [j[0] * j[0], j[0] * j[1], j[0] * j[2]]
        products += [j[1] * j[1], j[1] * j[2], j[2] * j[2]]
        for f, product in enumerate(products):
            feat_ref[f * 8 : f * 8 + 8, :] = pair_sum(product)
        offset = offset_ref[tile]
        lines = pl.ds(pl.multiple_of(tile * 4, 4), 4)
        index_ref[lines, :] = slot_ref[lines, :] + (offset & 127)
        index = row_of(index_ref, tile * 4, 4)
        for unit in range(2):
            columns = [feat_ref[pl.ds(4 * unit + 2 * q, 16, stride=8), :] for q in range(2)]
            lhs = jnp.concatenate(thirds(jnp.concatenate(columns, axis=1)), axis=0)
            hot = one_hot(2 * LANES, index[:, unit * 2 * LANES : (unit + 1) * 2 * LANES])
            pltpu.matmul_push_rhs(hot, 1, unit, transpose=True)
            pltpu.matmul_acc_lhs(point_accs[unit], lhs, 1)
        return is_block(offset, blocks - 1)

    for load in loads[:2]:
        load.wait()
    find(0)
    for load in loads[2:]:
        load.wait()
    push_bins(0, pos_ref)
    split_lines(0, residual_of(0), cam_ref, line_ref.at[0])

    def one_tile(tile, now, later):
        ahead = jnp.minimum(tile + 1, tiles - 1)
        add_lines(tile, pos_ref, line_ref.at[now], accs)
        here = add_points(tile)
        find(ahead)
        push_bins(ahead, pos_ref)
        split_lines(ahead, residual_of(ahead), cam_ref, line_ref.at[later])
        dots = pltpu.matmul_pop(point_accs[0]) + pltpu.matmul_pop(point_accs[1])
        dots = (dots[32:48] + dots[16:32]) + dots[0:16]
        left, right = dots[:, :LANES], dots[:, LANES:]
        for b in range(blocks):
            part = jnp.where(here[b - 1], right, 0.0) if b else jnp.zeros_like(left)
            point_ref[b] += jnp.where(here[b], left, part) if b < blocks - 1 else part

    def some_tiles(k, _):
        for s in range(UNROLL):
            one_tile(UNROLL * k + s, s % 2, 1 - s % 2)
        return 0

    lax.fori_loop(0, tiles // UNROLL, some_tiles, 0)


def move_start(tile, offset_ref, index_ref, step_ref, point_accs):
    index = row_of(index_ref, tile * 4, 4)
    blocks = step_ref.shape[0]
    here = is_block(offset_ref[tile], blocks - 1)
    left = right = jnp.zeros((16, LANES), F32)
    for b in range(blocks - 1):
        left = jnp.where(here[b], step_ref[b], left)
        right = jnp.where(here[b], step_ref[b + 1], right)
    lhs = jnp.concatenate([left, right], axis=1).astype(BF16)
    for unit in range(2):
        hot = one_hot(2 * LANES, index[:, unit * 2 * LANES : (unit + 1) * 2 * LANES])
        pltpu.matmul_push_rhs(hot, 1, unit)
        pltpu.matmul_acc_lhs(point_accs[unit], lhs, 1)


def move_end(tile, pt_ref, res_ref, moved_ref, point_accs):
    for unit in range(2):
        dots = pltpu.matmul_pop(point_accs[unit])
        taken = (dots[6:9] + dots[3:6]) + dots[0:3]
        for q in range(2):
            piece = taken[:, q * LANES : (q + 1) * LANES]
            for a in range(2):
                row = tile * 8 + 2 * (2 * unit + q) + a
                jac = jnp.concatenate([pt_ref[k, pl.ds(row, 1), :] for k in range(3)], axis=0)
                moved = jnp.sum(jac * piece, axis=0, keepdims=True)
                moved_ref[pl.ds(row, 1), :] = moved - res_ref[pl.ds(row, 1), :]


def second_start(offset_ref, index_ref, step_ref, pt_ref, res_ref, moved_ref, pos_ref, cam_ref, line_ref, point_accs, accs):
    for tile in range(2):
        move_start(tile, offset_ref, index_ref, step_ref, point_accs)
        move_end(tile, pt_ref, res_ref, moved_ref, point_accs)
    push_bins(0, pos_ref)
    split_lines(0, moved_ref[0:8, :], cam_ref, line_ref.at[0])


def second_tiles(
    first, last, offset_ref, index_ref, step_ref, pt_ref, res_ref, moved_ref, pos_ref, cam_ref, line_ref, point_accs, accs
):
    tiles = res_ref.shape[0] // 8

    def one_tile(tile, now, later):
        ahead = jnp.minimum(tile + 1, tiles - 1)
        after = jnp.minimum(tile + 2, tiles - 1)
        add_lines(tile, pos_ref, line_ref.at[now], accs)
        move_start(after, offset_ref, index_ref, step_ref, point_accs)
        push_bins(ahead, pos_ref)
        factor = moved_ref[pl.ds(pl.multiple_of(ahead * 8, 8), 8), :]
        split_lines(ahead, factor, cam_ref, line_ref.at[later])
        move_end(after, pt_ref, res_ref, moved_ref, point_accs)

    def some_tiles(k, _):
        for s in range(UNROLL):
            one_tile(UNROLL * k + s, s % 2, 1 - s % 2)
        return 0

    lax.fori_loop(first // UNROLL, last // UNROLL, some_tiles, 0)


def scoped(kernel, shapes):
    def whole(*refs):
        pl.run_scoped(lambda *accs: kernel(*refs, *accs), *shapes())

    return whole


def acc_shapes():
    sums = [pltpu.ACC(unit)((48, 2 * LANES), F32) for unit in range(2)]
    takes = [pltpu.ACC(unit)((16, 2 * LANES), F32) for unit in range(2)]
    return sums + takes + [pltpu.ACC(unit)((BINS, 2 * LANES), F32) for unit in range(2) for _ in range(CAM)]


def row_major(array):
    rows, n_obs = array.shape[1:-1], array.shape[-1]
    blocks = array.reshape(2, *rows, n_obs // LANES, LANES)
    blocks = jnp.moveaxis(blocks, 0, -2)
    return blocks.reshape(*rows, 2 * n_obs // LANES, LANES)


AXES = ("gx_0", "gx_1", "gy_0", "gy_1")
HOPS = (0, 1, 2, 1)
SLABS = (2, 1, 3, 0)


def neighbours(me, names, sizes):
    total = 1
    for name in names:
        total *= sizes[name]
    place = 0
    for name in names:
        place = place * sizes[name] + me[name]
    found = []
    for k in range(1, total):
        other = lax.rem(place + k, total)
        target = dict(me)
        for name in reversed(names):
            target[name] = lax.rem(other, sizes[name])
            other = other // sizes[name]
        found.append(tuple(target[name] for name in AXES))
    return found


def slab_offsets(dx):
    found = [(dx, dy, dz) for dy in range(4) for dz in range(4) if (dx, dy, dz) != (0, 0, 0)]
    return sorted(found, key=lambda offset: -sum(HOPS[d] for d in offset))


def whole_kernel(
    sizes,
    scale,
    offset_ref,
    res_hbm,
    cam_hbm,
    pt_hbm,
    camera_hbm,
    slot_hbm,
    damp_hbm,
    table_hbm,
    kept_ref,
    rest_ref,
    cost_ref,
    res_ref,
    cam_ref,
    pt_ref,
    camera_ref,
    slot_ref,
    damp_ref,
    table_ref,
    load_sem,
    pos_ref,
    index_ref,
    feat_ref,
    point_ref,
    step_ref,
    moved_ref,
    line_ref,
    total_ref,
    grad_ref,
    move_ref,
    pair_ref,
    whole_ref,
    inbox_ref,
    mine_ref,
    far_ref,
    plane_ref,
    near_ref,
    pair_send,
    pair_recv,
    chip_send,
    chip_recv,
    far_send,
    far_recv,
    near_send,
    near_recv,
    *accs,
):
    loads = [
        pltpu.make_async_copy(source, target, load_sem.at[k])
        for k, (source, target) in enumerate(
            (
                (camera_hbm, camera_ref),
                (table_hbm, table_ref),
                (res_hbm, res_ref),
                (pt_hbm, pt_ref),
                (slot_hbm, slot_ref),
                (cam_hbm, cam_ref),
                (damp_hbm, damp_ref),
            )
        )
    ]
    for load in loads:
        load.start()
    me = {name: lax.axis_index(name) for name in AXES}
    far = neighbours(me, ("gx_0", "gx_1"), sizes)
    near = neighbours(me, ("gy_0", "gy_1"), sizes)
    core = me["gx_1"]
    partner = (me["gx_0"], 1 - core, me["gy_0"], me["gy_1"])

    barrier = pltpu.get_barrier_semaphore()
    chips = {}
    for dx in SLABS:
        for offset in slab_offsets(dx):
            place = [lax.rem(me[n] + d, sizes[n]) for n, d in zip(("gx_0", "gy_0", "gy_1"), offset)]
            chips[offset] = (place[0], core, place[1], place[2])
    others = [chips[o] for o in chips if o[0] and (o[1] or o[2])]
    for target in far + near + others:
        pl.semaphore_signal(barrier, inc=1, device_id=target, device_id_type=MESH)

    started = []

    def send(source, target_ref, send_sem, recv_sem, device):
        copy = pltpu.make_async_remote_copy(
            src_ref=source,
            dst_ref=target_ref,
            send_sem=send_sem,
            recv_sem=recv_sem,
            device_id=device,
            device_id_type=MESH,
        )
        copy.start()
        started.append(copy)
        return copy

    flight = {}

    def pairs(job, source):
        flight[job] = []
        for k, dx in enumerate(SLABS):
            there = lax.rem(me["gx_0"] + dx, sizes["gx_0"])
            flight[job].append(
                send(
                    source.at[1 - core, there],
                    pair_ref.at[job, there],
                    pair_send.at[job, k],
                    pair_recv.at[job, k],
                    partner,
                )
            )

    def spread(job, source):
        copies = flight[job]
        flight[job] = []
        for k, dx in enumerate(SLABS):
            there = lax.rem(me["gx_0"] + dx, sizes["gx_0"])
            copies[k].wait_recv()
            whole_ref[job, there] = source[core, there] + pair_ref[job, there]
            for offset in slab_offsets(dx):
                slot = (offset[0] * 4 + offset[1]) * 4 + offset[2] - 1
                device = chips[offset]
                flight[job].append(
                    send(
                        whole_ref.at[job, there, device[2], device[3]],
                        inbox_ref.at[job, slot],
                        chip_send.at[job, slot],
                        chip_recv.at[job, slot],
                        device,
                    )
                )

    def finish(job):
        for copy in flight[job]:
            copy.wait_recv()
        kept = whole_ref[job, me["gx_0"], me["gy_0"], me["gy_1"]]
        return kept, jnp.sum(inbox_ref[job], axis=0)

    sum_accs, take_accs, accs = accs[:2], accs[2:4], accs[4:]
    empty_accs(sum_accs + take_accs + accs)
    first_tiles(
        offset_ref,
        res_ref,
        cam_ref,
        pt_ref,
        camera_ref,
        slot_ref,
        table_ref,
        pos_ref,
        index_ref,
        feat_ref,
        point_ref,
        line_ref,
        sum_accs,
        accs,
        loads,
    )
    drain(accs, total_ref)
    regroup_into(grad_ref, total_ref)
    pl.semaphore_wait(barrier, len(far) + len(near) + len(others))
    pairs(0, grad_ref)
    point_square = solve_points(point_ref, damp_ref, step_ref)
    residual = res_ref[...]
    square = jnp.sum(residual * residual)
    lane = lax.broadcasted_iota(I32, mine_ref.shape, 1)
    refs = (
        offset_ref,
        index_ref,
        step_ref,
        pt_ref,
        res_ref,
        moved_ref,
        pos_ref,
        cam_ref,
        line_ref,
        take_accs,
        accs,
    )
    second_start(*refs)
    second_tiles(0, 8, *refs)
    spread(0, grad_ref)
    second_tiles(8, 24, *refs)
    kept, rest = finish(0)
    grads = kept + rest
    gradient_square = point_square + jnp.sum(grads * grads)
    mine_ref[...] = jnp.where(lane == 0, square, jnp.where(lane == 1, gradient_square, 0.0))
    arrivals = [
        send(mine_ref, far_ref.at[k], far_send.at[k], far_recv.at[k], device)
        for k, device in enumerate(far)
    ]
    second_tiles(24, 32, *refs)
    drain(accs, total_ref)
    regroup_into(move_ref, total_ref)
    pairs(1, move_ref)
    for copy in arrivals:
        copy.wait_recv()
    plane_ref[...] = mine_ref[...] + jnp.sum(far_ref[...], axis=0)
    arrivals = [
        send(plane_ref, near_ref.at[k], near_send.at[k], near_recv.at[k], device)
        for k, device in enumerate(near)
    ]
    spread(1, move_ref)
    for copy in arrivals:
        copy.wait_recv()
    totals = plane_ref[...] + jnp.sum(near_ref[...], axis=0)
    first_row = lax.broadcasted_iota(I32, mine_ref.shape, 0) == 0
    cost = totals / scale[0]
    norm = jnp.sqrt(totals / scale[1] + 1e-06)
    cost_ref[...] = jnp.where(lane == 0, cost, norm)
    kept_ref[...], rest_ref[...] = finish(1)
    for copy in started:
        copy.wait_send()


def whole(
    residual, cam_jacobian, point_jacobian, obs_camera, obs_slot, tile_offset, damping, camera_slot, sizes, scale
):
    vmem = pl.BlockSpec(memory_space=pltpu.VMEM)
    smem = pl.BlockSpec(memory_space=pltpu.SMEM)
    buffer = lambda *lead: pltpu.VMEM(lead + (CAM, LANES), F32)
    chips = sizes["gx_0"] * sizes["gy_0"] * sizes["gy_1"] - 1
    dma = pltpu.SemaphoreType.DMA
    far = sizes["gx_0"] * sizes["gx_1"] - 1
    near = sizes["gy_0"] * sizes["gy_1"] - 1
    return pl.pallas_call(
        scoped(functools.partial(whole_kernel, sizes, scale), acc_shapes),
        out_shape=(
            jax.ShapeDtypeStruct((CAM, LANES), F32),
            jax.ShapeDtypeStruct((CAM, LANES), F32),
            jax.ShapeDtypeStruct((8, LANES), F32),
        ),
        in_specs=[smem] + [pl.BlockSpec(memory_space=pl.ANY)] * 7,
        out_specs=(vmem, vmem, vmem),
        scratch_shapes=[
            pltpu.VMEM(residual.shape, F32),
            pltpu.VMEM(cam_jacobian.shape, F32),
            pltpu.VMEM(point_jacobian.shape, F32),
            pltpu.VMEM(obs_camera.shape, I32),
            pltpu.VMEM(obs_slot.shape, I32),
            pltpu.VMEM(damping.shape, F32),
            pltpu.VMEM(camera_slot.shape, I32),
            dma((7,)),
            pltpu.VMEM(obs_camera.shape, I32),
            pltpu.VMEM(obs_camera.shape, I32),
            pltpu.VMEM((16 * 8, LANES), F32),
            pltpu.VMEM((damping.shape[0] + 1, 16, LANES), F32),
            pltpu.VMEM((damping.shape[0] + 1, 16, LANES), F32),
            pltpu.VMEM(residual.shape, F32),
            pltpu.VMEM((2, 2, CAM, 8, LANES), F32),
            pltpu.VMEM((2, CAM * PITCH, LANES), F32),
            buffer(2, 4, 4, 4),
            buffer(2, 4, 4, 4),
            buffer(2, 4, 4, 4),
            buffer(2, 4, 4, 4),
            buffer(2, chips),
            pltpu.VMEM((8, LANES), F32),
            pltpu.VMEM((far, 8, LANES), F32),
            pltpu.VMEM((8, LANES), F32),
            pltpu.VMEM((near, 8, LANES), F32),
            dma((2, 4)),
            dma((2, 4)),
            dma((2, chips)),
            dma((2, chips)),
            dma((far,)),
            dma((far,)),
            dma((near,)),
            dma((near,)),
        ],
        compiler_params=pltpu.CompilerParams(collective_id=0, has_side_effects=True),
    )(tile_offset, residual, cam_jacobian, point_jacobian, obs_camera, obs_slot, damping, camera_slot)


def on_device(
    residual, cam_jacobian, point_jacobian, obs_camera, obs_slot, tile_offset, damping, camera_slot
):
    n_obs = residual.shape[1]
    sizes = {name: lax.axis_size(name) for name in AXES}
    devices = lax.axis_size(AXES)
    scale = (2.0 * n_obs * devices, 9.0 * camera_slot.shape[0] + 3.0 * damping.shape[0] * devices)
    lines = lambda array: array.reshape(-1, LANES)
    res, cam, pt = row_major(residual), row_major(cam_jacobian), row_major(point_jacobian)
    kept, rest, ends = whole(
        res, cam, pt, lines(obs_camera), lines(obs_slot), tile_offset, lines(damping), lines(camera_slot), sizes, scale
    )
    return (kept + rest, ends[0, 0], ends[0, 1])


def solution(mesh):
    finer = Mesh(mesh.devices.reshape(4, 2, 4, 4), AXES)
    in_specs = (
        P(None, AXES),
        P(None, None, AXES),
        P(None, None, AXES),
        P(AXES),
        P(AXES),
        P(AXES),
        P(AXES),
        P(),
    )
    out_specs = (P(None, AXES), P(), P())
    return jax.shard_map(
        on_device, mesh=finer, in_specs=in_specs, out_specs=out_specs, check_vma=False
    )
```

```python
import functools

import jax
import jax.numpy as jnp
from jax import lax
from jax.experimental import pallas as pl
from jax.experimental.pallas import tpu as pltpu
from jax.sharding import Mesh
from jax.sharding import PartitionSpec as P

F32, BF16, I32 = jnp.float32, jnp.bfloat16, jnp.int32
NT = (((1,), (1,)), ((), ()))
MESH = pl.DeviceIdType.MESH
LANES = 128
CAM = 9
BINS = 64
PITCH = 72
UNROLL = 8


def thirds(value):
    high = value.astype(BF16)
    rest = value - high.astype(F32)
    middle = rest.astype(BF16)
    return high, middle, (rest - middle.astype(F32)).astype(BF16)


def row_of(ref, start, count):
    return jnp.concatenate([ref[pl.ds(start + k, 1), :] for k in range(count)], axis=1)


def pair_sum(product):
    return product + pltpu.roll(product, product.shape[0] - 1, 0)


def one_hot(count, index):
    shape = (count, index.shape[1])
    return (lax.broadcasted_iota(I32, shape, 0) == index).astype(F32).astype(BF16)


def push_bins(tile, pos_ref):
    for unit in range(2):
        pos = row_of(pos_ref, tile * 4 + unit * 2, 2)
        lo = (((pos >> 11) & 1) << 7) + (pos & 127)
        pltpu.matmul_push_rhs(one_hot(2 * LANES, lo), 0, unit, transpose=True)


def split_lines(tile, factor, cam_ref, line_ref):
    rows = pl.ds(pl.multiple_of(tile * 8, 8), 8)
    for m in range(CAM):
        value = pair_sum(cam_ref[m, rows, :] * factor)
        high = value.astype(BF16).astype(F32)
        line_ref[0, m] = high
        line_ref[1, m] = value - high


def add_lines(tile, pos_ref, line_ref, accs):
    hots = []
    for unit in range(2):
        owner = row_of(pos_ref, tile * 4 + unit * 2, 2) >> 7
        hots.append(one_hot(BINS, ((owner >> 5) << 4) + (owner & 15)))
    for part in range(2):
        for m in range(CAM):
            for unit in range(2):
                pieces = []
                for q in range(2):
                    row = 2 * (2 * unit + q)
                    line = jnp.broadcast_to(line_ref[part, m, row : row + 1], (16, LANES)).astype(BF16)
                    hot = hots[unit][:, q * LANES : (q + 1) * LANES].reshape(BINS // 16, 16, LANES)
                    pieces.append((hot * line[None]).reshape(BINS, LANES))
                lhs = jnp.concatenate(pieces, axis=1)
                staged = 0 if part == 0 and m == 0 else None
                pltpu.matmul_acc_lhs(accs[unit * CAM + m], lhs, staged)


def empty_accs(accs):
    return [pltpu.matmul_pop(acc) for acc in accs]


def drain(accs, total_ref):
    for unit in range(2):
        pltpu.matmul_acc_lhs(accs[unit * CAM], jnp.zeros((BINS, 2 * LANES), BF16), 0)
    for m in range(CAM):
        total = pltpu.matmul_pop(accs[m]) + pltpu.matmul_pop(accs[CAM + m])
        total_ref[0, m * PITCH : m * PITCH + BINS] = total[:, :LANES]
        total_ref[1, m * PITCH : m * PITCH + BINS] = total[:, LANES:]


def regroup_into(out_ref, total_ref):
    def one(hi, _):
        for side in range(2):
            rows = pl.ds(hi, CAM, stride=PITCH)
            out_ref[side, hi >> 4, (hi >> 2) & 3, hi & 3] = total_ref[side, rows, :]
        return 0

    lax.fori_loop(0, BINS, one, 0, unroll=4)


def is_block(offset, count):
    block = jnp.full((16, LANES), offset >> 7, I32)
    return [block == b for b in range(count)]


def solve_points(point_ref, damp_ref, step_ref):
    blocks = damp_ref.shape[0]
    damping = row_of(damp_ref, 0, blocks)

    def row(k):
        return jnp.concatenate([point_ref[b, k : k + 1, :] for b in range(blocks)], axis=1)

    g = [row(k) for k in range(3)]
    aa, ab, ac, bb, bc, cc = [row(k) for k in range(3, 9)]
    aa, bb, cc = aa + damping, bb + damping, cc + damping
    cof_aa = bb * cc - bc * bc
    cof_ab = ac * bc - ab * cc
    cof_ac = ab * bc - ac * bb
    cof_bb = aa * cc - ac * ac
    cof_bc = ab * ac - aa * bc
    cof_cc = aa * bb - ab * ab
    determ = aa * cof_aa + ab * cof_ab + ac * cof_ac
    steps = [
        (cof_aa * g[0] + cof_ab * g[1] + cof_ac * g[2]) / determ,
        (cof_ab * g[0] + cof_bb * g[1] + cof_bc * g[2]) / determ,
        (cof_ac * g[0] + cof_bc * g[1] + cof_cc * g[2]) / determ,
    ]
    step_ref[...] = jnp.zeros_like(step_ref)
    for k in range(3):
        for p, part in enumerate(thirds(steps[k])):
            value = part.astype(F32)
            for b in range(blocks):
                step_ref[b, 3 * p + k : 3 * p + k + 1, :] = value[:, b * LANES : (b + 1) * LANES]
    return jnp.sum(g[0] * g[0] + g[1] * g[1] + g[2] * g[2])


def first_tiles(
    offset_ref,
    res_ref,
    cam_ref,
    pt_ref,
    camera_ref,
    slot_ref,
    table_ref,
    pos_ref,
    index_ref,
    feat_ref,
    point_ref,
    line_ref,
    point_accs,
    accs,
    loads,
):
    tiles = res_ref.shape[0] // 8
    blocks = point_ref.shape[0]
    point_ref[...] = jnp.zeros_like(point_ref)
    feat_ref[...] = jnp.zeros_like(feat_ref)

    def find(tile):
        lines = pl.ds(pl.multiple_of(tile * 4, 4), 4)
        camera = camera_ref[lines, :]
        high, low = camera >> 7, camera & 127
        found = [jnp.zeros_like(camera)] * 4
        for k in range(table_ref.shape[0]):
            line = jnp.broadcast_to(table_ref[k : k + 1, :], camera.shape)
            taken = jnp.take_along_axis(line, low, axis=1, mode="promise_in_bounds")
            found[k % 4] = jnp.where(high == k, taken, found[k % 4])
        pos_ref[lines, :] = (found[0] + found[1]) + (found[2] + found[3])

    def residual_of(tile):
        return res_ref[pl.ds(pl.multiple_of(tile * 8, 8), 8), :]

    def add_points(tile):
        rows = pl.ds(pl.multiple_of(tile * 8, 8), 8)
        r = residual_of(tile)
        j = [pt_ref[k, rows, :] for k in range(3)]
        products = [j[0] * r, j[1] * r, j[2] * r]
        products += [j[0] * j[0], j[0] * j[1], j[0] * j[2]]
        products += [j[1] * j[1], j[1] * j[2], j[2] * j[2]]
        for f, product in enumerate(products):
            feat_ref[f * 8 : f * 8 + 8, :] = pair_sum(product)
        offset = offset_ref[tile]
        lines = pl.ds(pl.multiple_of(tile * 4, 4), 4)
        index_ref[lines, :] = slot_ref[lines, :] + (offset & 127)
        index = row_of(index_ref, tile * 4, 4)
        for unit in range(2):
            columns = [feat_ref[pl.ds(4 * unit + 2 * q, 16, stride=8), :] for q in range(2)]
            lhs = jnp.concatenate(thirds(jnp.concatenate(columns, axis=1)), axis=0)
            hot = one_hot(2 * LANES, index[:, unit * 2 * LANES : (unit + 1) * 2 * LANES])
            pltpu.matmul_push_rhs(hot, 1, unit, transpose=True)
            pltpu.matmul_acc_lhs(point_accs[unit], lhs, 1)
        return is_block(offset, blocks - 1)

    for load in loads[:2]:
        load.wait()
    find(0)
    for load in loads[2:]:
        load.wait()
    push_bins(0, pos_ref)
    split_lines(0, residual_of(0), cam_ref, line_ref.at[0])

    def one_tile(tile, now, later):
        ahead = jnp.minimum(tile + 1, tiles - 1)
        add_lines(tile, pos_ref, line_ref.at[now], accs)
        here = add_points(tile)
        find(ahead)
        push_bins(ahead, pos_ref)
        split_lines(ahead, residual_of(ahead), cam_ref, line_ref.at[later])
        dots = pltpu.matmul_pop(point_accs[0]) + pltpu.matmul_pop(point_accs[1])
        dots = (dots[32:48] + dots[16:32]) + dots[0:16]
        left, right = dots[:, :LANES], dots[:, LANES:]
        for b in range(blocks):
            part = jnp.where(here[b - 1], right, 0.0) if b else jnp.zeros_like(left)
            point_ref[b] += jnp.where(here[b], left, part) if b < blocks - 1 else part

    def some_tiles(k, _):
        for s in range(UNROLL):
            one_tile(UNROLL * k + s, s % 2, 1 - s % 2)
        return 0

    lax.fori_loop(0, tiles // UNROLL, some_tiles, 0)


def move_start(tile, offset_ref, index_ref, step_ref, point_accs):
    index = row_of(index_ref, tile * 4, 4)
    blocks = step_ref.shape[0]
    here = is_block(offset_ref[tile], blocks - 1)
    left = right = jnp.zeros((16, LANES), F32)
    for b in range(blocks - 1):
        left = jnp.where(here[b], step_ref[b], left)
        right = jnp.where(here[b], step_ref[b + 1], right)
    lhs = jnp.concatenate([left, right], axis=1).astype(BF16)
    for unit in range(2):
        hot = one_hot(2 * LANES, index[:, unit * 2 * LANES : (unit + 1) * 2 * LANES])
        pltpu.matmul_push_rhs(hot, 1, unit)
        pltpu.matmul_acc_lhs(point_accs[unit], lhs, 1)


def move_end(tile, pt_ref, res_ref, moved_ref, point_accs):
    for unit in range(2):
        dots = pltpu.matmul_pop(point_accs[unit])
        taken = (dots[6:9] + dots[3:6]) + dots[0:3]
        for q in range(2):
            piece = taken[:, q * LANES : (q + 1) * LANES]
            for a in range(2):
                row = tile * 8 + 2 * (2 * unit + q) + a
                jac = jnp.concatenate([pt_ref[k, pl.ds(row, 1), :] for k in range(3)], axis=0)
                moved = jnp.sum(jac * piece, axis=0, keepdims=True)
                moved_ref[pl.ds(row, 1), :] = moved - res_ref[pl.ds(row, 1), :]


def second_start(offset_ref, index_ref, step_ref, pt_ref, res_ref, moved_ref, pos_ref, cam_ref, line_ref, point_accs, accs):
    for tile in range(2):
        move_start(tile, offset_ref, index_ref, step_ref, point_accs)
        move_end(tile, pt_ref, res_ref, moved_ref, point_accs)
    push_bins(0, pos_ref)
    split_lines(0, moved_ref[0:8, :], cam_ref, line_ref.at[0])


def second_tiles(
    first, last, offset_ref, index_ref, step_ref, pt_ref, res_ref, moved_ref, pos_ref, cam_ref, line_ref, point_accs, accs
):
    tiles = res_ref.shape[0] // 8

    def one_tile(tile, now, later):
        ahead = jnp.minimum(tile + 1, tiles - 1)
        after = jnp.minimum(tile + 2, tiles - 1)
        add_lines(tile, pos_ref, line_ref.at[now], accs)
        move_start(after, offset_ref, index_ref, step_ref, point_accs)
        push_bins(ahead, pos_ref)
        factor = moved_ref[pl.ds(pl.multiple_of(ahead * 8, 8), 8), :]
        split_lines(ahead, factor, cam_ref, line_ref.at[later])
        move_end(after, pt_ref, res_ref, moved_ref, point_accs)

    def some_tiles(k, _):
        for s in range(UNROLL):
            one_tile(UNROLL * k + s, s % 2, 1 - s % 2)
        return 0

    lax.fori_loop(first // UNROLL, last // UNROLL, some_tiles, 0)


def scoped(kernel, shapes):
    def whole(*refs):
        pl.run_scoped(lambda *accs: kernel(*refs, *accs), *shapes())

    return whole


def acc_shapes():
    sums = [pltpu.ACC(unit)((48, 2 * LANES), F32) for unit in range(2)]
    takes = [pltpu.ACC(unit)((16, 2 * LANES), F32) for unit in range(2)]
    return sums + takes + [pltpu.ACC(unit)((BINS, 2 * LANES), F32) for unit in range(2) for _ in range(CAM)]


def row_major(array):
    rows, n_obs = array.shape[1:-1], array.shape[-1]
    blocks = array.reshape(2, *rows, n_obs // LANES, LANES)
    blocks = jnp.moveaxis(blocks, 0, -2)
    return blocks.reshape(*rows, 2 * n_obs // LANES, LANES)


AXES = ("gx_0", "gx_1", "gy_0", "gy_1")
HOPS = (0, 1, 2, 1)
SLABS = (2, 1, 3, 0)


def neighbours(me, names, sizes):
    total = 1
    for name in names:
        total *= sizes[name]
    place = 0
    for name in names:
        place = place * sizes[name] + me[name]
    found = []
    for k in range(1, total):
        other = lax.rem(place + k, total)
        target = dict(me)
        for name in reversed(names):
            target[name] = lax.rem(other, sizes[name])
            other = other // sizes[name]
        found.append(tuple(target[name] for name in AXES))
    return found


def slab_offsets(dx):
    found = [(dx, dy, dz) for dy in range(4) for dz in range(4) if (dx, dy, dz) != (0, 0, 0)]
    return sorted(found, key=lambda offset: -sum(HOPS[d] for d in offset))


def whole_kernel(
    sizes,
    scale,
    offset_ref,
    res_hbm,
    cam_hbm,
    pt_hbm,
    camera_hbm,
    slot_hbm,
    damp_hbm,
    table_hbm,
    kept_ref,
    rest_ref,
    cost_ref,
    res_ref,
    cam_ref,
    pt_ref,
    camera_ref,
    slot_ref,
    damp_ref,
    table_ref,
    load_sem,
    pos_ref,
    index_ref,
    feat_ref,
    point_ref,
    step_ref,
    moved_ref,
    line_ref,
    total_ref,
    grad_ref,
    move_ref,
    pair_ref,
    whole_ref,
    inbox_ref,
    mine_ref,
    far_ref,
    plane_ref,
    near_ref,
    pair_send,
    pair_recv,
    chip_send,
    chip_recv,
    far_send,
    far_recv,
    near_send,
    near_recv,
    *accs,
):
    loads = [
        pltpu.make_async_copy(source, target, load_sem.at[k])
        for k, (source, target) in enumerate(
            (
                (camera_hbm, camera_ref),
                (table_hbm, table_ref),
                (res_hbm, res_ref),
                (pt_hbm, pt_ref),
                (slot_hbm, slot_ref),
                (cam_hbm, cam_ref),
                (damp_hbm, damp_ref),
            )
        )
    ]
    for load in loads:
        load.start()
    me = {name: lax.axis_index(name) for name in AXES}
    far = neighbours(me, ("gx_0", "gx_1"), sizes)
    near = neighbours(me, ("gy_0", "gy_1"), sizes)
    core = me["gx_1"]
    partner = (me["gx_0"], 1 - core, me["gy_0"], me["gy_1"])

    barrier = pltpu.get_barrier_semaphore()
    chips = {}
    for dx in SLABS:
        for offset in slab_offsets(dx):
            place = [lax.rem(me[n] + d, sizes[n]) for n, d in zip(("gx_0", "gy_0", "gy_1"), offset)]
            chips[offset] = (place[0], core, place[1], place[2])
    others = [chips[o] for o in chips if o[0] and (o[1] or o[2])]
    for target in far + near + others:
        pl.semaphore_signal(barrier, inc=1, device_id=target, device_id_type=MESH)

    started = []

    def send(source, target_ref, send_sem, recv_sem, device):
        copy = pltpu.make_async_remote_copy(
            src_ref=source,
            dst_ref=target_ref,
            send_sem=send_sem,
            recv_sem=recv_sem,
            device_id=device,
            device_id_type=MESH,
        )
        copy.start()
        started.append(copy)
        return copy

    flight = {}

    def pairs(job, source):
        flight[job] = []
        for k, dx in enumerate(SLABS):
            there = lax.rem(me["gx_0"] + dx, sizes["gx_0"])
            flight[job].append(
                send(
                    source.at[1 - core, there],
                    pair_ref.at[job, there],
                    pair_send.at[job, k],
                    pair_recv.at[job, k],
                    partner,
                )
            )

    def spread(job, source):
        copies = flight[job]
        flight[job] = []
        for k, dx in enumerate(SLABS):
            there = lax.rem(me["gx_0"] + dx, sizes["gx_0"])
            copies[k].wait_recv()
            whole_ref[job, there] = source[core, there] + pair_ref[job, there]
            for offset in slab_offsets(dx):
                slot = (offset[0] * 4 + offset[1]) * 4 + offset[2] - 1
                device = chips[offset]
                flight[job].append(
                    send(
                        whole_ref.at[job, there, device[2], device[3]],
                        inbox_ref.at[job, slot],
                        chip_send.at[job, slot],
                        chip_recv.at[job, slot],
                        device,
                    )
                )

    def finish(job):
        for copy in flight[job]:
            copy.wait_recv()
        kept = whole_ref[job, me["gx_0"], me["gy_0"], me["gy_1"]]
        return kept, jnp.sum(inbox_ref[job], axis=0)

    sum_accs, take_accs, accs = accs[:2], accs[2:4], accs[4:]
    empty_accs(sum_accs + take_accs + accs)
    first_tiles(
        offset_ref,
        res_ref,
        cam_ref,
        pt_ref,
        camera_ref,
        slot_ref,
        table_ref,
        pos_ref,
        index_ref,
        feat_ref,
        point_ref,
        line_ref,
        sum_accs,
        accs,
        loads,
    )
    drain(accs, total_ref)
    regroup_into(grad_ref, total_ref)
    pl.semaphore_wait(barrier, len(far) + len(near) + len(others))
    pairs(0, grad_ref)
    point_square = solve_points(point_ref, damp_ref, step_ref)
    residual = res_ref[...]
    square = jnp.sum(residual * residual)
    lane = lax.broadcasted_iota(I32, mine_ref.shape, 1)
    refs = (
        offset_ref,
        index_ref,
        step_ref,
        pt_ref,
        res_ref,
        moved_ref,
        pos_ref,
        cam_ref,
        line_ref,
        take_accs,
        accs,
    )
    second_start(*refs)
    second_tiles(0, 8, *refs)
    spread(0, grad_ref)
    second_tiles(8, 24, *refs)
    kept, rest = finish(0)
    grads = kept + rest
    gradient_square = point_square + jnp.sum(grads * grads)
    mine_ref[...] = jnp.where(lane == 0, square, jnp.where(lane == 1, gradient_square, 0.0))
    arrivals = [
        send(mine_ref, far_ref.at[k], far_send.at[k], far_recv.at[k], device)
        for k, device in enumerate(far)
    ]
    second_tiles(24, 32, *refs)
    drain(accs, total_ref)
    regroup_into(move_ref, total_ref)
    pairs(1, move_ref)
    for copy in arrivals:
        copy.wait_recv()
    plane_ref[...] = mine_ref[...] + jnp.sum(far_ref[...], axis=0)
    arrivals = [
        send(plane_ref, near_ref.at[k], near_send.at[k], near_recv.at[k], device)
        for k, device in enumerate(near)
    ]
    spread(1, move_ref)
    for copy in arrivals:
        copy.wait_recv()
    totals = plane_ref[...] + jnp.sum(near_ref[...], axis=0)
    first_row = lax.broadcasted_iota(I32, mine_ref.shape, 0) == 0
    cost = totals / scale[0]
    norm = jnp.sqrt(totals / scale[1] + 1e-06)
    cost_ref[...] = jnp.where(lane == 0, cost, norm)
    kept_ref[...], rest_ref[...] = finish(1)
    for copy in started:
        copy.wait_send()


def whole(
    residual, cam_jacobian, point_jacobian, obs_camera, obs_slot, tile_offset, damping, camera_slot, sizes, scale
):
    vmem = pl.BlockSpec(memory_space=pltpu.VMEM)
    smem = pl.BlockSpec(memory_space=pltpu.SMEM)
    buffer = lambda *lead: pltpu.VMEM(lead + (CAM, LANES), F32)
    chips = sizes["gx_0"] * sizes["gy_0"] * sizes["gy_1"] - 1
    dma = pltpu.SemaphoreType.DMA
    far = sizes["gx_0"] * sizes["gx_1"] - 1
    near = sizes["gy_0"] * sizes["gy_1"] - 1
    return pl.pallas_call(
        scoped(functools.partial(whole_kernel, sizes, scale), acc_shapes),
        out_shape=(
            jax.ShapeDtypeStruct((CAM, LANES), F32),
            jax.ShapeDtypeStruct((CAM, LANES), F32),
            jax.ShapeDtypeStruct((8, LANES), F32),
        ),
        in_specs=[smem] + [pl.BlockSpec(memory_space=pl.ANY)] * 7,
        out_specs=(vmem, vmem, vmem),
        scratch_shapes=[
            pltpu.VMEM(residual.shape, F32),
            pltpu.VMEM(cam_jacobian.shape, F32),
            pltpu.VMEM(point_jacobian.shape, F32),
            pltpu.VMEM(obs_camera.shape, I32),
            pltpu.VMEM(obs_slot.shape, I32),
            pltpu.VMEM(damping.shape, F32),
            pltpu.VMEM(camera_slot.shape, I32),
            dma((7,)),
            pltpu.VMEM(obs_camera.shape, I32),
            pltpu.VMEM(obs_camera.shape, I32),
            pltpu.VMEM((16 * 8, LANES), F32),
            pltpu.VMEM((damping.shape[0] + 1, 16, LANES), F32),
            pltpu.VMEM((damping.shape[0] + 1, 16, LANES), F32),
            pltpu.VMEM(residual.shape, F32),
            pltpu.VMEM((2, 2, CAM, 8, LANES), F32),
            pltpu.VMEM((2, CAM * PITCH, LANES), F32),
            buffer(2, 4, 4, 4),
            buffer(2, 4, 4, 4),
            buffer(2, 4, 4, 4),
            buffer(2, 4, 4, 4),
            buffer(2, chips),
            pltpu.VMEM((8, LANES), F32),
            pltpu.VMEM((far, 8, LANES), F32),
            pltpu.VMEM((8, LANES), F32),
            pltpu.VMEM((near, 8, LANES), F32),
            dma((2, 4)),
            dma((2, 4)),
            dma((2, chips)),
            dma((2, chips)),
            dma((far,)),
            dma((far,)),
            dma((near,)),
            dma((near,)),
        ],
        compiler_params=pltpu.CompilerParams(collective_id=0, has_side_effects=True),
    )(tile_offset, residual, cam_jacobian, point_jacobian, obs_camera, obs_slot, damping, camera_slot)


def close_kernel(kept_ref, rest_ref, ends_ref, reduced_ref, cost_ref, norm_ref):
    reduced_ref[...] = kept_ref[...] + rest_ref[...]
    lane = lax.broadcasted_iota(I32, (1, LANES), 1)
    ends = ends_ref[0:1, :]
    cost_ref[0, 0] = jnp.sum(jnp.where(lane == 0, ends, 0.0))
    norm_ref[0, 0] = jnp.sum(jnp.where(lane == 1, ends, 0.0))


def close(kept, rest, ends):
    vmem = pl.BlockSpec(memory_space=pltpu.VMEM)
    smem = pl.BlockSpec(memory_space=pltpu.SMEM)
    scalar = jax.ShapeDtypeStruct((1, 1), F32)
    return pl.pallas_call(
        close_kernel,
        out_shape=(jax.ShapeDtypeStruct(kept.shape, F32), scalar, scalar),
        in_specs=[vmem] * 3,
        out_specs=(vmem, smem, smem),
    )(kept, rest, ends)


def on_device(
    residual, cam_jacobian, point_jacobian, obs_camera, obs_slot, tile_offset, damping, camera_slot
):
    n_obs = residual.shape[1]
    sizes = {name: lax.axis_size(name) for name in AXES}
    devices = lax.axis_size(AXES)
    scale = (2.0 * n_obs * devices, 9.0 * camera_slot.shape[0] + 3.0 * damping.shape[0] * devices)
    lines = lambda array: array.reshape(-1, LANES)
    res, cam, pt = row_major(residual), row_major(cam_jacobian), row_major(point_jacobian)
    kept, rest, ends = whole(
        res, cam, pt, lines(obs_camera), lines(obs_slot), tile_offset, lines(damping), lines(camera_slot), sizes, scale
    )
    reduced, cost, norm = close(kept, rest, ends)
    return (reduced, cost.reshape(()), norm.reshape(()))


def solution(mesh):
    finer = Mesh(mesh.devices.reshape(4, 2, 4, 4), AXES)
    in_specs = (
        P(None, AXES),
        P(None, None, AXES),
        P(None, None, AXES),
        P(AXES),
        P(AXES),
        P(AXES),
        P(AXES),
        P(),
    )
    out_specs = (P(None, AXES), P(), P())
    return jax.shard_map(
        on_device, mesh=finer, in_specs=in_specs, out_specs=out_specs, check_vma=False
    )
```

```python
import functools

import jax
import jax.numpy as jnp
from jax import lax
from jax.experimental import pallas as pl
from jax.experimental.pallas import tpu as pltpu
from jax.sharding import Mesh
from jax.sharding import PartitionSpec as P

F32, BF16, I32 = jnp.float32, jnp.bfloat16, jnp.int32
NT = (((1,), (1,)), ((), ()))
MESH = pl.DeviceIdType.MESH
LANES = 128
CAM = 9
BINS = 64
PITCH = 72
UNROLL = 8


def thirds(value):
    high = value.astype(BF16)
    rest = value - high.astype(F32)
    middle = rest.astype(BF16)
    return high, middle, (rest - middle.astype(F32)).astype(BF16)


def row_of(ref, start, count):
    return jnp.concatenate([ref[pl.ds(start + k, 1), :] for k in range(count)], axis=1)


def pair_sum(product):
    return product + pltpu.roll(product, product.shape[0] - 1, 0)


def one_hot(count, index):
    shape = (count, index.shape[1])
    return (lax.broadcasted_iota(I32, shape, 0) == index).astype(F32).astype(BF16)


def push_bins(tile, pos_ref):
    for unit in range(2):
        pos = row_of(pos_ref, tile * 4 + unit * 2, 2)
        lo = (((pos >> 11) & 1) << 7) + (pos & 127)
        pltpu.matmul_push_rhs(one_hot(2 * LANES, lo), 0, unit, transpose=True)


def split_lines(tile, factor, cam_ref, line_ref):
    rows = pl.ds(pl.multiple_of(tile * 8, 8), 8)
    for m in range(CAM):
        value = pair_sum(cam_ref[m, rows, :] * factor)
        high = value.astype(BF16).astype(F32)
        line_ref[0, m] = high
        line_ref[1, m] = value - high


def add_lines(tile, pos_ref, line_ref, accs):
    hots = []
    for unit in range(2):
        owner = row_of(pos_ref, tile * 4 + unit * 2, 2) >> 7
        hots.append(one_hot(BINS, ((owner >> 5) << 4) + (owner & 15)))
    for part in range(2):
        for m in range(CAM):
            for unit in range(2):
                pieces = []
                for q in range(2):
                    row = 2 * (2 * unit + q)
                    line = jnp.broadcast_to(line_ref[part, m, row : row + 1], (16, LANES)).astype(BF16)
                    hot = hots[unit][:, q * LANES : (q + 1) * LANES].reshape(BINS // 16, 16, LANES)
                    pieces.append((hot * line[None]).reshape(BINS, LANES))
                lhs = jnp.concatenate(pieces, axis=1)
                staged = 0 if part == 0 and m == 0 else None
                pltpu.matmul_acc_lhs(accs[unit * CAM + m], lhs, staged)


def empty_accs(accs):
    return [pltpu.matmul_pop(acc) for acc in accs]


def drain(accs, total_ref):
    for unit in range(2):
        pltpu.matmul_acc_lhs(accs[unit * CAM], jnp.zeros((BINS, 2 * LANES), BF16), 0)
    for m in range(CAM):
        total = pltpu.matmul_pop(accs[m]) + pltpu.matmul_pop(accs[CAM + m])
        total_ref[0, m * PITCH : m * PITCH + BINS] = total[:, :LANES]
        total_ref[1, m * PITCH : m * PITCH + BINS] = total[:, LANES:]


def regroup_slab(out_ref, total_ref, slab):
    def one(k, _):
        hi = slab * 16 + k
        for side in range(2):
            rows = pl.ds(hi, CAM, stride=PITCH)
            out_ref[side, slab, k >> 2, k & 3] = total_ref[side, rows, :]
        return 0

    lax.fori_loop(0, 16, one, 0, unroll=4)


def is_block(offset, count):
    block = jnp.full((16, LANES), offset >> 7, I32)
    return [block == b for b in range(count)]


def solve_points(point_ref, damp_ref, step_ref):
    blocks = damp_ref.shape[0]
    damping = row_of(damp_ref, 0, blocks)

    def row(k):
        return jnp.concatenate([point_ref[b, k : k + 1, :] for b in range(blocks)], axis=1)

    g = [row(k) for k in range(3)]
    aa, ab, ac, bb, bc, cc = [row(k) for k in range(3, 9)]
    aa, bb, cc = aa + damping, bb + damping, cc + damping
    cof_aa = bb * cc - bc * bc
    cof_ab = ac * bc - ab * cc
    cof_ac = ab * bc - ac * bb
    cof_bb = aa * cc - ac * ac
    cof_bc = ab * ac - aa * bc
    cof_cc = aa * bb - ab * ab
    determ = aa * cof_aa + ab * cof_ab + ac * cof_ac
    steps = [
        (cof_aa * g[0] + cof_ab * g[1] + cof_ac * g[2]) / determ,
        (cof_ab * g[0] + cof_bb * g[1] + cof_bc * g[2]) / determ,
        (cof_ac * g[0] + cof_bc * g[1] + cof_cc * g[2]) / determ,
    ]
    step_ref[...] = jnp.zeros_like(step_ref)
    for k in range(3):
        for p, part in enumerate(thirds(steps[k])):
            value = part.astype(F32)
            for b in range(blocks):
                step_ref[b, 3 * p + k : 3 * p + k + 1, :] = value[:, b * LANES : (b + 1) * LANES]
    return jnp.sum(g[0] * g[0] + g[1] * g[1] + g[2] * g[2])


def first_tiles(
    offset_ref,
    res_ref,
    cam_ref,
    pt_ref,
    camera_ref,
    slot_ref,
    table_ref,
    pos_ref,
    index_ref,
    feat_ref,
    point_ref,
    line_ref,
    point_accs,
    accs,
    loads,
):
    tiles = res_ref.shape[0] // 8
    blocks = point_ref.shape[0]
    point_ref[...] = jnp.zeros_like(point_ref)
    feat_ref[...] = jnp.zeros_like(feat_ref)

    def find(tile):
        lines = pl.ds(pl.multiple_of(tile * 4, 4), 4)
        camera = camera_ref[lines, :]
        high, low = camera >> 7, camera & 127
        found = [jnp.zeros_like(camera)] * 4
        for k in range(table_ref.shape[0]):
            line = jnp.broadcast_to(table_ref[k : k + 1, :], camera.shape)
            taken = jnp.take_along_axis(line, low, axis=1, mode="promise_in_bounds")
            found[k % 4] = jnp.where(high == k, taken, found[k % 4])
        pos_ref[lines, :] = (found[0] + found[1]) + (found[2] + found[3])

    def residual_of(tile):
        return res_ref[pl.ds(pl.multiple_of(tile * 8, 8), 8), :]

    def add_points(tile):
        rows = pl.ds(pl.multiple_of(tile * 8, 8), 8)
        r = residual_of(tile)
        j = [pt_ref[k, rows, :] for k in range(3)]
        products = [j[0] * r, j[1] * r, j[2] * r]
        products += [j[0] * j[0], j[0] * j[1], j[0] * j[2]]
        products += [j[1] * j[1], j[1] * j[2], j[2] * j[2]]
        for f, product in enumerate(products):
            feat_ref[f * 8 : f * 8 + 8, :] = pair_sum(product)
        offset = offset_ref[tile]
        lines = pl.ds(pl.multiple_of(tile * 4, 4), 4)
        index_ref[lines, :] = slot_ref[lines, :] + (offset & 127)
        index = row_of(index_ref, tile * 4, 4)
        for unit in range(2):
            columns = [feat_ref[pl.ds(4 * unit + 2 * q, 16, stride=8), :] for q in range(2)]
            lhs = jnp.concatenate(thirds(jnp.concatenate(columns, axis=1)), axis=0)
            hot = one_hot(2 * LANES, index[:, unit * 2 * LANES : (unit + 1) * 2 * LANES])
            pltpu.matmul_push_rhs(hot, 1, unit, transpose=True)
            pltpu.matmul_acc_lhs(point_accs[unit], lhs, 1)
        return is_block(offset, blocks - 1)

    for load in loads[:2]:
        load.wait()
    find(0)
    for load in loads[2:]:
        load.wait()
    push_bins(0, pos_ref)
    split_lines(0, residual_of(0), cam_ref, line_ref.at[0])

    def one_tile(tile, now, later):
        ahead = jnp.minimum(tile + 1, tiles - 1)
        add_lines(tile, pos_ref, line_ref.at[now], accs)
        here = add_points(tile)
        find(ahead)
        push_bins(ahead, pos_ref)
        split_lines(ahead, residual_of(ahead), cam_ref, line_ref.at[later])
        dots = pltpu.matmul_pop(point_accs[0]) + pltpu.matmul_pop(point_accs[1])
        dots = (dots[32:48] + dots[16:32]) + dots[0:16]
        left, right = dots[:, :LANES], dots[:, LANES:]
        for b in range(blocks):
            part = jnp.where(here[b - 1], right, 0.0) if b else jnp.zeros_like(left)
            point_ref[b] += jnp.where(here[b], left, part) if b < blocks - 1 else part

    def some_tiles(k, _):
        for s in range(UNROLL):
            one_tile(UNROLL * k + s, s % 2, 1 - s % 2)
        return 0

    lax.fori_loop(0, tiles // UNROLL, some_tiles, 0)


def move_start(tile, offset_ref, index_ref, step_ref, point_accs):
    index = row_of(index_ref, tile * 4, 4)
    blocks = step_ref.shape[0]
    here = is_block(offset_ref[tile], blocks - 1)
    left = right = jnp.zeros((16, LANES), F32)
    for b in range(blocks - 1):
        left = jnp.where(here[b], step_ref[b], left)
        right = jnp.where(here[b], step_ref[b + 1], right)
    lhs = jnp.concatenate([left, right], axis=1).astype(BF16)
    for unit in range(2):
        hot = one_hot(2 * LANES, index[:, unit * 2 * LANES : (unit + 1) * 2 * LANES])
        pltpu.matmul_push_rhs(hot, 1, unit)
        pltpu.matmul_acc_lhs(point_accs[unit], lhs, 1)


def move_end(tile, pt_ref, res_ref, moved_ref, point_accs):
    for unit in range(2):
        dots = pltpu.matmul_pop(point_accs[unit])
        taken = (dots[6:9] + dots[3:6]) + dots[0:3]
        for q in range(2):
            piece = taken[:, q * LANES : (q + 1) * LANES]
            for a in range(2):
                row = tile * 8 + 2 * (2 * unit + q) + a
                jac = jnp.concatenate([pt_ref[k, pl.ds(row, 1), :] for k in range(3)], axis=0)
                moved = jnp.sum(jac * piece, axis=0, keepdims=True)
                moved_ref[pl.ds(row, 1), :] = moved - res_ref[pl.ds(row, 1), :]


def second_start(offset_ref, index_ref, step_ref, pt_ref, res_ref, moved_ref, pos_ref, cam_ref, line_ref, point_accs, accs):
    for tile in range(2):
        move_start(tile, offset_ref, index_ref, step_ref, point_accs)
        move_end(tile, pt_ref, res_ref, moved_ref, point_accs)
    push_bins(0, pos_ref)
    split_lines(0, moved_ref[0:8, :], cam_ref, line_ref.at[0])


def second_tiles(
    first, last, offset_ref, index_ref, step_ref, pt_ref, res_ref, moved_ref, pos_ref, cam_ref, line_ref, point_accs, accs
):
    tiles = res_ref.shape[0] // 8

    def one_tile(tile, now, later):
        ahead = jnp.minimum(tile + 1, tiles - 1)
        after = jnp.minimum(tile + 2, tiles - 1)
        add_lines(tile, pos_ref, line_ref.at[now], accs)
        move_start(after, offset_ref, index_ref, step_ref, point_accs)
        push_bins(ahead, pos_ref)
        factor = moved_ref[pl.ds(pl.multiple_of(ahead * 8, 8), 8), :]
        split_lines(ahead, factor, cam_ref, line_ref.at[later])
        move_end(after, pt_ref, res_ref, moved_ref, point_accs)

    def some_tiles(k, _):
        for s in range(UNROLL):
            one_tile(UNROLL * k + s, s % 2, 1 - s % 2)
        return 0

    lax.fori_loop(first // UNROLL, last // UNROLL, some_tiles, 0)


def scoped(kernel, shapes):
    def whole(*refs):
        pl.run_scoped(lambda *accs: kernel(*refs, *accs), *shapes())

    return whole


def acc_shapes():
    sums = [pltpu.ACC(unit)((48, 2 * LANES), F32) for unit in range(2)]
    takes = [pltpu.ACC(unit)((16, 2 * LANES), F32) for unit in range(2)]
    return sums + takes + [pltpu.ACC(unit)((BINS, 2 * LANES), F32) for unit in range(2) for _ in range(CAM)]


def row_major(array):
    rows, n_obs = array.shape[1:-1], array.shape[-1]
    blocks = array.reshape(2, *rows, n_obs // LANES, LANES)
    blocks = jnp.moveaxis(blocks, 0, -2)
    return blocks.reshape(*rows, 2 * n_obs // LANES, LANES)


AXES = ("gx_0", "gx_1", "gy_0", "gy_1")
HOPS = (0, 1, 2, 1)
SLABS = (2, 1, 3, 0)


def neighbours(me, names, sizes):
    total = 1
    for name in names:
        total *= sizes[name]
    place = 0
    for name in names:
        place = place * sizes[name] + me[name]
    found = []
    for k in range(1, total):
        other = lax.rem(place + k, total)
        target = dict(me)
        for name in reversed(names):
            target[name] = lax.rem(other, sizes[name])
            other = other // sizes[name]
        found.append(tuple(target[name] for name in AXES))
    return found


def slab_offsets(dx):
    found = [(dx, dy, dz) for dy in range(4) for dz in range(4) if (dx, dy, dz) != (0, 0, 0)]
    return sorted(found, key=lambda offset: -sum(HOPS[d] for d in offset))


def whole_kernel(
    sizes,
    scale,
    offset_ref,
    res_hbm,
    cam_hbm,
    pt_hbm,
    camera_hbm,
    slot_hbm,
    damp_hbm,
    table_hbm,
    kept_ref,
    rest_ref,
    cost_ref,
    res_ref,
    cam_ref,
    pt_ref,
    camera_ref,
    slot_ref,
    damp_ref,
    table_ref,
    load_sem,
    pos_ref,
    index_ref,
    feat_ref,
    point_ref,
    step_ref,
    moved_ref,
    line_ref,
    total_ref,
    grad_ref,
    move_ref,
    pair_ref,
    whole_ref,
    inbox_ref,
    mine_ref,
    far_ref,
    plane_ref,
    near_ref,
    pair_send,
    pair_recv,
    chip_send,
    chip_recv,
    far_send,
    far_recv,
    near_send,
    near_recv,
    *accs,
):
    loads = [
        pltpu.make_async_copy(source, target, load_sem.at[k])
        for k, (source, target) in enumerate(
            (
                (camera_hbm, camera_ref),
                (table_hbm, table_ref),
                (res_hbm, res_ref),
                (pt_hbm, pt_ref),
                (slot_hbm, slot_ref),
                (cam_hbm, cam_ref),
                (damp_hbm, damp_ref),
            )
        )
    ]
    for load in loads:
        load.start()
    me = {name: lax.axis_index(name) for name in AXES}
    far = neighbours(me, ("gx_0", "gx_1"), sizes)
    near = neighbours(me, ("gy_0", "gy_1"), sizes)
    core = me["gx_1"]
    partner = (me["gx_0"], 1 - core, me["gy_0"], me["gy_1"])

    barrier = pltpu.get_barrier_semaphore()
    chips = {}
    for dx in SLABS:
        for offset in slab_offsets(dx):
            place = [lax.rem(me[n] + d, sizes[n]) for n, d in zip(("gx_0", "gy_0", "gy_1"), offset)]
            chips[offset] = (place[0], core, place[1], place[2])
    others = [chips[o] for o in chips if o[0] and (o[1] or o[2])]
    for target in far + near + others:
        pl.semaphore_signal(barrier, inc=1, device_id=target, device_id_type=MESH)

    started = []

    def send(source, target_ref, send_sem, recv_sem, device):
        copy = pltpu.make_async_remote_copy(
            src_ref=source,
            dst_ref=target_ref,
            send_sem=send_sem,
            recv_sem=recv_sem,
            device_id=device,
            device_id_type=MESH,
        )
        copy.start()
        started.append(copy)
        return copy

    flight = {}

    def pairs(job, source):
        flight[job] = []
        for k, dx in enumerate(SLABS):
            there = lax.rem(me["gx_0"] + dx, sizes["gx_0"])
            regroup_slab(source, total_ref, there)
            flight[job].append(
                send(
                    source.at[1 - core, there],
                    pair_ref.at[job, there],
                    pair_send.at[job, k],
                    pair_recv.at[job, k],
                    partner,
                )
            )

    def spread(job, source):
        copies = flight[job]
        flight[job] = []
        for k, dx in enumerate(SLABS):
            there = lax.rem(me["gx_0"] + dx, sizes["gx_0"])
            copies[k].wait_recv()
            whole_ref[job, there] = source[core, there] + pair_ref[job, there]
            for offset in slab_offsets(dx):
                slot = (offset[0] * 4 + offset[1]) * 4 + offset[2] - 1
                device = chips[offset]
                flight[job].append(
                    send(
                        whole_ref.at[job, there, device[2], device[3]],
                        inbox_ref.at[job, slot],
                        chip_send.at[job, slot],
                        chip_recv.at[job, slot],
                        device,
                    )
                )

    def finish(job):
        for copy in flight[job]:
            copy.wait_recv()
        kept = whole_ref[job, me["gx_0"], me["gy_0"], me["gy_1"]]
        return kept, jnp.sum(inbox_ref[job], axis=0)

    sum_accs, take_accs, accs = accs[:2], accs[2:4], accs[4:]
    empty_accs(sum_accs + take_accs + accs)
    first_tiles(
        offset_ref,
        res_ref,
        cam_ref,
        pt_ref,
        camera_ref,
        slot_ref,
        table_ref,
        pos_ref,
        index_ref,
        feat_ref,
        point_ref,
        line_ref,
        sum_accs,
        accs,
        loads,
    )
    drain(accs, total_ref)
    pl.semaphore_wait(barrier, len(far) + len(near) + len(others))
    pairs(0, grad_ref)
    point_square = solve_points(point_ref, damp_ref, step_ref)
    residual = res_ref[...]
    square = jnp.sum(residual * residual)
    lane = lax.broadcasted_iota(I32, mine_ref.shape, 1)
    refs = (
        offset_ref,
        index_ref,
        step_ref,
        pt_ref,
        res_ref,
        moved_ref,
        pos_ref,
        cam_ref,
        line_ref,
        take_accs,
        accs,
    )
    second_start(*refs)
    second_tiles(0, 8, *refs)
    spread(0, grad_ref)
    second_tiles(8, 24, *refs)
    kept, rest = finish(0)
    grads = kept + rest
    gradient_square = point_square + jnp.sum(grads * grads)
    mine_ref[...] = jnp.where(lane == 0, square, jnp.where(lane == 1, gradient_square, 0.0))
    arrivals = [
        send(mine_ref, far_ref.at[k], far_send.at[k], far_recv.at[k], device)
        for k, device in enumerate(far)
    ]
    second_tiles(24, 32, *refs)
    drain(accs, total_ref)
    pairs(1, move_ref)
    for copy in arrivals:
        copy.wait_recv()
    plane_ref[...] = mine_ref[...] + jnp.sum(far_ref[...], axis=0)
    arrivals = [
        send(plane_ref, near_ref.at[k], near_send.at[k], near_recv.at[k], device)
        for k, device in enumerate(near)
    ]
    spread(1, move_ref)
    for copy in arrivals:
        copy.wait_recv()
    totals = plane_ref[...] + jnp.sum(near_ref[...], axis=0)
    first_row = lax.broadcasted_iota(I32, mine_ref.shape, 0) == 0
    cost = totals / scale[0]
    norm = jnp.sqrt(totals / scale[1] + 1e-06)
    cost_ref[...] = jnp.where(lane == 0, cost, norm)
    kept_ref[...], rest_ref[...] = finish(1)
    for copy in started:
        copy.wait_send()


def whole(
    residual, cam_jacobian, point_jacobian, obs_camera, obs_slot, tile_offset, damping, camera_slot, sizes, scale
):
    vmem = pl.BlockSpec(memory_space=pltpu.VMEM)
    smem = pl.BlockSpec(memory_space=pltpu.SMEM)
    buffer = lambda *lead: pltpu.VMEM(lead + (CAM, LANES), F32)
    chips = sizes["gx_0"] * sizes["gy_0"] * sizes["gy_1"] - 1
    dma = pltpu.SemaphoreType.DMA
    far = sizes["gx_0"] * sizes["gx_1"] - 1
    near = sizes["gy_0"] * sizes["gy_1"] - 1
    return pl.pallas_call(
        scoped(functools.partial(whole_kernel, sizes, scale), acc_shapes),
        out_shape=(
            jax.ShapeDtypeStruct((CAM, LANES), F32),
            jax.ShapeDtypeStruct((CAM, LANES), F32),
            jax.ShapeDtypeStruct((8, LANES), F32),
        ),
        in_specs=[smem] + [pl.BlockSpec(memory_space=pl.ANY)] * 7,
        out_specs=(vmem, vmem, vmem),
        scratch_shapes=[
            pltpu.VMEM(residual.shape, F32),
            pltpu.VMEM(cam_jacobian.shape, F32),
            pltpu.VMEM(point_jacobian.shape, F32),
            pltpu.VMEM(obs_camera.shape, I32),
            pltpu.VMEM(obs_slot.shape, I32),
            pltpu.VMEM(damping.shape, F32),
            pltpu.VMEM(camera_slot.shape, I32),
            dma((7,)),
            pltpu.VMEM(obs_camera.shape, I32),
            pltpu.VMEM(obs_camera.shape, I32),
            pltpu.VMEM((16 * 8, LANES), F32),
            pltpu.VMEM((damping.shape[0] + 1, 16, LANES), F32),
            pltpu.VMEM((damping.shape[0] + 1, 16, LANES), F32),
            pltpu.VMEM(residual.shape, F32),
            pltpu.VMEM((2, 2, CAM, 8, LANES), F32),
            pltpu.VMEM((2, CAM * PITCH, LANES), F32),
            buffer(2, 4, 4, 4),
            buffer(2, 4, 4, 4),
            buffer(2, 4, 4, 4),
            buffer(2, 4, 4, 4),
            buffer(2, chips),
            pltpu.VMEM((8, LANES), F32),
            pltpu.VMEM((far, 8, LANES), F32),
            pltpu.VMEM((8, LANES), F32),
            pltpu.VMEM((near, 8, LANES), F32),
            dma((2, 4)),
            dma((2, 4)),
            dma((2, chips)),
            dma((2, chips)),
            dma((far,)),
            dma((far,)),
            dma((near,)),
            dma((near,)),
        ],
        compiler_params=pltpu.CompilerParams(collective_id=0, has_side_effects=True),
    )(tile_offset, residual, cam_jacobian, point_jacobian, obs_camera, obs_slot, damping, camera_slot)


def close_kernel(kept_ref, rest_ref, ends_ref, reduced_ref, cost_ref, norm_ref):
    reduced_ref[...] = kept_ref[...] + rest_ref[...]
    lane = lax.broadcasted_iota(I32, (1, LANES), 1)
    ends = ends_ref[0:1, :]
    cost_ref[0, 0] = jnp.sum(jnp.where(lane == 0, ends, 0.0))
    norm_ref[0, 0] = jnp.sum(jnp.where(lane == 1, ends, 0.0))


def close(kept, rest, ends):
    vmem = pl.BlockSpec(memory_space=pltpu.VMEM)
    smem = pl.BlockSpec(memory_space=pltpu.SMEM)
    scalar = jax.ShapeDtypeStruct((1, 1), F32)
    return pl.pallas_call(
        close_kernel,
        out_shape=(jax.ShapeDtypeStruct(kept.shape, F32), scalar, scalar),
        in_specs=[vmem] * 3,
        out_specs=(vmem, smem, smem),
    )(kept, rest, ends)


def on_device(
    residual, cam_jacobian, point_jacobian, obs_camera, obs_slot, tile_offset, damping, camera_slot
):
    n_obs = residual.shape[1]
    sizes = {name: lax.axis_size(name) for name in AXES}
    devices = lax.axis_size(AXES)
    scale = (2.0 * n_obs * devices, 9.0 * camera_slot.shape[0] + 3.0 * damping.shape[0] * devices)
    lines = lambda array: array.reshape(-1, LANES)
    res, cam, pt = row_major(residual), row_major(cam_jacobian), row_major(point_jacobian)
    kept, rest, ends = whole(
        res, cam, pt, lines(obs_camera), lines(obs_slot), tile_offset, lines(damping), lines(camera_slot), sizes, scale
    )
    reduced, cost, norm = close(kept, rest, ends)
    return (reduced, cost.reshape(()), norm.reshape(()))


def solution(mesh):
    finer = Mesh(mesh.devices.reshape(4, 2, 4, 4), AXES)
    in_specs = (
        P(None, AXES),
        P(None, None, AXES),
        P(None, None, AXES),
        P(AXES),
        P(AXES),
        P(AXES),
        P(AXES),
        P(),
    )
    out_specs = (P(None, AXES), P(), P())
    return jax.shard_map(
        on_device, mesh=finer, in_specs=in_specs, out_specs=out_specs, check_vma=False
    )
```

```python
import functools

import jax
import jax.numpy as jnp
from jax import lax
from jax.experimental import pallas as pl
from jax.experimental.pallas import tpu as pltpu
from jax.sharding import Mesh
from jax.sharding import PartitionSpec as P

F32, BF16, I32 = jnp.float32, jnp.bfloat16, jnp.int32
NT = (((1,), (1,)), ((), ()))
MESH = pl.DeviceIdType.MESH
LANES = 128
CAM = 9
BINS = 64
PITCH = 72
UNROLL = 8


def thirds(value):
    high = value.astype(BF16)
    rest = value - high.astype(F32)
    middle = rest.astype(BF16)
    return high, middle, (rest - middle.astype(F32)).astype(BF16)


def row_of(ref, start, count):
    return jnp.concatenate([ref[pl.ds(start + k, 1), :] for k in range(count)], axis=1)


def pair_sum(product):
    return product + pltpu.roll(product, product.shape[0] - 1, 0)


def one_hot(count, index):
    shape = (count, index.shape[1])
    return (lax.broadcasted_iota(I32, shape, 0) == index).astype(F32).astype(BF16)


def push_bins(tile, pos_ref):
    for unit in range(2):
        pos = row_of(pos_ref, tile * 4 + unit * 2, 2)
        lo = (((pos >> 11) & 1) << 7) + (pos & 127)
        pltpu.matmul_push_rhs(one_hot(2 * LANES, lo), 0, unit, transpose=True)


def split_lines(tile, factor, cam_ref, line_ref):
    rows = pl.ds(pl.multiple_of(tile * 8, 8), 8)
    for m in range(CAM):
        value = pair_sum(cam_ref[m, rows, :] * factor)
        high = value.astype(BF16).astype(F32)
        line_ref[0, m] = high
        line_ref[1, m] = value - high


def add_lines(tile, pos_ref, line_ref, accs):
    hots = []
    for unit in range(2):
        owner = row_of(pos_ref, tile * 4 + unit * 2, 2) >> 7
        hots.append(one_hot(BINS, ((owner >> 5) << 4) + (owner & 15)))
    for part in range(2):
        for m in range(CAM):
            for unit in range(2):
                pieces = []
                for q in range(2):
                    row = 2 * (2 * unit + q)
                    line = jnp.broadcast_to(line_ref[part, m, row : row + 1], (16, LANES)).astype(BF16)
                    hot = hots[unit][:, q * LANES : (q + 1) * LANES].reshape(BINS // 16, 16, LANES)
                    pieces.append((hot * line[None]).reshape(BINS, LANES))
                lhs = jnp.concatenate(pieces, axis=1)
                staged = 0 if part == 0 and m == 0 else None
                pltpu.matmul_acc_lhs(accs[unit * CAM + m], lhs, staged)


def empty_accs(accs):
    return [pltpu.matmul_pop(acc) for acc in accs]


def drain(accs, total_ref):
    for unit in range(2):
        pltpu.matmul_acc_lhs(accs[unit * CAM], jnp.zeros((BINS, 2 * LANES), BF16), 0)
    for m in range(CAM):
        total = pltpu.matmul_pop(accs[m]) + pltpu.matmul_pop(accs[CAM + m])
        total_ref[0, m * PITCH : m * PITCH + BINS] = total[:, :LANES]
        total_ref[1, m * PITCH : m * PITCH + BINS] = total[:, LANES:]


def regroup_into(out_ref, total_ref):
    def one(hi, _):
        for side in range(2):
            rows = pl.ds(hi, CAM, stride=PITCH)
            out_ref[side, hi >> 4, (hi >> 2) & 3, hi & 3] = total_ref[side, rows, :]
        return 0

    lax.fori_loop(0, BINS, one, 0, unroll=4)


def is_block(offset, count):
    block = jnp.full((16, LANES), offset >> 7, I32)
    return [block == b for b in range(count)]


def solve_points(point_ref, damp_ref, step_ref):
    blocks = damp_ref.shape[0]
    damping = row_of(damp_ref, 0, blocks)

    def row(k):
        return jnp.concatenate([point_ref[b, k : k + 1, :] for b in range(blocks)], axis=1)

    g = [row(k) for k in range(3)]
    aa, ab, ac, bb, bc, cc = [row(k) for k in range(3, 9)]
    aa, bb, cc = aa + damping, bb + damping, cc + damping
    cof_aa = bb * cc - bc * bc
    cof_ab = ac * bc - ab * cc
    cof_ac = ab * bc - ac * bb
    cof_bb = aa * cc - ac * ac
    cof_bc = ab * ac - aa * bc
    cof_cc = aa * bb - ab * ab
    determ = aa * cof_aa + ab * cof_ab + ac * cof_ac
    steps = [
        (cof_aa * g[0] + cof_ab * g[1] + cof_ac * g[2]) / determ,
        (cof_ab * g[0] + cof_bb * g[1] + cof_bc * g[2]) / determ,
        (cof_ac * g[0] + cof_bc * g[1] + cof_cc * g[2]) / determ,
    ]
    step_ref[...] = jnp.zeros_like(step_ref)
    for k in range(3):
        for p, part in enumerate(thirds(steps[k])):
            value = part.astype(F32)
            for b in range(blocks):
                step_ref[b, 3 * p + k : 3 * p + k + 1, :] = value[:, b * LANES : (b + 1) * LANES]
    return jnp.sum(g[0] * g[0] + g[1] * g[1] + g[2] * g[2])


def first_tiles(
    offset_ref,
    res_ref,
    cam_ref,
    pt_ref,
    camera_ref,
    slot_ref,
    table_ref,
    pos_ref,
    index_ref,
    feat_ref,
    point_ref,
    line_ref,
    point_accs,
    accs,
    loads,
):
    tiles = res_ref.shape[0] // 8
    blocks = point_ref.shape[0]
    point_ref[...] = jnp.zeros_like(point_ref)
    feat_ref[...] = jnp.zeros_like(feat_ref)

    def find(tile):
        lines = pl.ds(pl.multiple_of(tile * 4, 4), 4)
        camera = camera_ref[lines, :]
        high, low = camera >> 7, camera & 127
        found = [jnp.zeros_like(camera)] * 4
        for k in range(table_ref.shape[0]):
            line = jnp.broadcast_to(table_ref[k : k + 1, :], camera.shape)
            taken = jnp.take_along_axis(line, low, axis=1, mode="promise_in_bounds")
            found[k % 4] = jnp.where(high == k, taken, found[k % 4])
        pos_ref[lines, :] = (found[0] + found[1]) + (found[2] + found[3])

    def residual_of(tile):
        return res_ref[pl.ds(pl.multiple_of(tile * 8, 8), 8), :]

    def add_points(tile):
        rows = pl.ds(pl.multiple_of(tile * 8, 8), 8)
        r = residual_of(tile)
        j = [pt_ref[k, rows, :] for k in range(3)]
        products = [j[0] * r, j[1] * r, j[2] * r]
        products += [j[0] * j[0], j[0] * j[1], j[0] * j[2]]
        products += [j[1] * j[1], j[1] * j[2], j[2] * j[2]]
        for f, product in enumerate(products):
            feat_ref[f * 8 : f * 8 + 8, :] = pair_sum(product)
        offset = offset_ref[tile]
        lines = pl.ds(pl.multiple_of(tile * 4, 4), 4)
        index_ref[lines, :] = slot_ref[lines, :] + (offset & 127)
        index = row_of(index_ref, tile * 4, 4)
        for unit in range(2):
            columns = [feat_ref[pl.ds(4 * unit + 2 * q, 16, stride=8), :] for q in range(2)]
            lhs = jnp.concatenate(thirds(jnp.concatenate(columns, axis=1)), axis=0)
            hot = one_hot(2 * LANES, index[:, unit * 2 * LANES : (unit + 1) * 2 * LANES])
            pltpu.matmul_push_rhs(hot, 1, unit, transpose=True)
            pltpu.matmul_acc_lhs(point_accs[unit], lhs, 1)
        return is_block(offset, blocks - 1)

    for load in loads[:2]:
        load.wait()
    find(0)
    for load in loads[2:]:
        load.wait()
    push_bins(0, pos_ref)
    split_lines(0, residual_of(0), cam_ref, line_ref.at[0])

    def one_tile(tile, now, later):
        ahead = jnp.minimum(tile + 1, tiles - 1)
        add_lines(tile, pos_ref, line_ref.at[now], accs)
        here = add_points(tile)
        find(ahead)
        push_bins(ahead, pos_ref)
        split_lines(ahead, residual_of(ahead), cam_ref, line_ref.at[later])
        dots = pltpu.matmul_pop(point_accs[0]) + pltpu.matmul_pop(point_accs[1])
        dots = (dots[32:48] + dots[16:32]) + dots[0:16]
        left, right = dots[:, :LANES], dots[:, LANES:]
        for b in range(blocks):
            part = jnp.where(here[b - 1], right, 0.0) if b else jnp.zeros_like(left)
            point_ref[b] += jnp.where(here[b], left, part) if b < blocks - 1 else part

    def some_tiles(k, _):
        for s in range(UNROLL):
            one_tile(UNROLL * k + s, s % 2, 1 - s % 2)
        return 0

    lax.fori_loop(0, tiles // UNROLL, some_tiles, 0)


def move_start(tile, offset_ref, index_ref, step_ref, point_accs):
    index = row_of(index_ref, tile * 4, 4)
    blocks = step_ref.shape[0]
    here = is_block(offset_ref[tile], blocks - 1)
    left = right = jnp.zeros((16, LANES), F32)
    for b in range(blocks - 1):
        left = jnp.where(here[b], step_ref[b], left)
        right = jnp.where(here[b], step_ref[b + 1], right)
    lhs = jnp.concatenate([left, right], axis=1).astype(BF16)
    for unit in range(2):
        hot = one_hot(2 * LANES, index[:, unit * 2 * LANES : (unit + 1) * 2 * LANES])
        pltpu.matmul_push_rhs(hot, 1, unit)
        pltpu.matmul_acc_lhs(point_accs[unit], lhs, 1)


def move_end(tile, pt_ref, res_ref, moved_ref, point_accs):
    for unit in range(2):
        dots = pltpu.matmul_pop(point_accs[unit])
        taken = (dots[6:9] + dots[3:6]) + dots[0:3]
        for q in range(2):
            piece = taken[:, q * LANES : (q + 1) * LANES]
            for a in range(2):
                row = tile * 8 + 2 * (2 * unit + q) + a
                jac = jnp.concatenate([pt_ref[k, pl.ds(row, 1), :] for k in range(3)], axis=0)
                moved = jnp.sum(jac * piece, axis=0, keepdims=True)
                moved_ref[pl.ds(row, 1), :] = moved - res_ref[pl.ds(row, 1), :]


def second_start(offset_ref, index_ref, step_ref, pt_ref, res_ref, moved_ref, pos_ref, cam_ref, line_ref, point_accs, accs):
    for tile in range(2):
        move_start(tile, offset_ref, index_ref, step_ref, point_accs)
        move_end(tile, pt_ref, res_ref, moved_ref, point_accs)
    push_bins(0, pos_ref)
    split_lines(0, moved_ref[0:8, :], cam_ref, line_ref.at[0])


def second_tiles(
    first, last, offset_ref, index_ref, step_ref, pt_ref, res_ref, moved_ref, pos_ref, cam_ref, line_ref, point_accs, accs
):
    tiles = res_ref.shape[0] // 8

    def one_tile(tile, now, later):
        ahead = jnp.minimum(tile + 1, tiles - 1)
        after = jnp.minimum(tile + 2, tiles - 1)
        add_lines(tile, pos_ref, line_ref.at[now], accs)
        move_start(after, offset_ref, index_ref, step_ref, point_accs)
        push_bins(ahead, pos_ref)
        factor = moved_ref[pl.ds(pl.multiple_of(ahead * 8, 8), 8), :]
        split_lines(ahead, factor, cam_ref, line_ref.at[later])
        move_end(after, pt_ref, res_ref, moved_ref, point_accs)

    def some_tiles(k, _):
        for s in range(UNROLL):
            one_tile(UNROLL * k + s, s % 2, 1 - s % 2)
        return 0

    lax.fori_loop(first // UNROLL, last // UNROLL, some_tiles, 0)


def scoped(kernel, shapes):
    def whole(*refs):
        pl.run_scoped(lambda *accs: kernel(*refs, *accs), *shapes())

    return whole


def acc_shapes():
    sums = [pltpu.ACC(unit)((48, 2 * LANES), F32) for unit in range(2)]
    takes = [pltpu.ACC(unit)((16, 2 * LANES), F32) for unit in range(2)]
    return sums + takes + [pltpu.ACC(unit)((BINS, 2 * LANES), F32) for unit in range(2) for _ in range(CAM)]


def row_major(array):
    rows, n_obs = array.shape[1:-1], array.shape[-1]
    blocks = array.reshape(2, *rows, n_obs // LANES, LANES)
    blocks = jnp.moveaxis(blocks, 0, -2)
    return blocks.reshape(*rows, 2 * n_obs // LANES, LANES)


AXES = ("gx_0", "gx_1", "gy_0", "gy_1")
HOPS = (0, 1, 2, 1)
SLABS = (2, 1, 3, 0)


def neighbours(me, names, sizes):
    total = 1
    for name in names:
        total *= sizes[name]
    place = 0
    for name in names:
        place = place * sizes[name] + me[name]
    found = []
    for k in range(1, total):
        other = lax.rem(place + k, total)
        target = dict(me)
        for name in reversed(names):
            target[name] = lax.rem(other, sizes[name])
            other = other // sizes[name]
        found.append(tuple(target[name] for name in AXES))
    return found


def slab_offsets(dx):
    found = [(dx, dy, dz) for dy in range(4) for dz in range(4) if (dx, dy, dz) != (0, 0, 0)]
    return sorted(found, key=lambda offset: -sum(HOPS[d] for d in offset))


def whole_kernel(
    sizes,
    scale,
    offset_ref,
    res_hbm,
    cam_hbm,
    pt_hbm,
    camera_hbm,
    slot_hbm,
    damp_hbm,
    table_hbm,
    kept_ref,
    rest_ref,
    cost_ref,
    res_ref,
    cam_ref,
    pt_ref,
    camera_ref,
    slot_ref,
    damp_ref,
    table_ref,
    load_sem,
    pos_ref,
    index_ref,
    feat_ref,
    point_ref,
    step_ref,
    moved_ref,
    line_ref,
    total_ref,
    grad_ref,
    move_ref,
    pair_ref,
    whole_ref,
    inbox_ref,
    mine_ref,
    far_ref,
    plane_ref,
    near_ref,
    pair_send,
    pair_recv,
    chip_send,
    chip_recv,
    far_send,
    far_recv,
    near_send,
    near_recv,
    *accs,
):
    loads = [
        pltpu.make_async_copy(source, target, load_sem.at[k])
        for k, (source, target) in enumerate(
            (
                (camera_hbm, camera_ref),
                (table_hbm, table_ref),
                (res_hbm, res_ref),
                (pt_hbm, pt_ref),
                (slot_hbm, slot_ref),
                (cam_hbm, cam_ref),
                (damp_hbm, damp_ref),
            )
        )
    ]
    for load in loads:
        load.start()
    me = {name: lax.axis_index(name) for name in AXES}
    far = neighbours(me, ("gx_0", "gx_1"), sizes)
    near = neighbours(me, ("gy_0", "gy_1"), sizes)
    core = me["gx_1"]
    partner = (me["gx_0"], 1 - core, me["gy_0"], me["gy_1"])

    barrier = pltpu.get_barrier_semaphore()
    chips = {}
    for dx in SLABS:
        for offset in slab_offsets(dx):
            place = [lax.rem(me[n] + d, sizes[n]) for n, d in zip(("gx_0", "gy_0", "gy_1"), offset)]
            chips[offset] = (place[0], core, place[1], place[2])
    others = [chips[o] for o in chips if o[0] and (o[1] or o[2])]
    for target in far + near + others:
        pl.semaphore_signal(barrier, inc=1, device_id=target, device_id_type=MESH)

    started = []

    def send(source, target_ref, send_sem, recv_sem, device):
        copy = pltpu.make_async_remote_copy(
            src_ref=source,
            dst_ref=target_ref,
            send_sem=send_sem,
            recv_sem=recv_sem,
            device_id=device,
            device_id_type=MESH,
        )
        copy.start()
        started.append(copy)
        return copy

    flight = {}

    def pairs(job, source):
        flight[job] = []
        for k, dx in enumerate(SLABS):
            there = lax.rem(me["gx_0"] + dx, sizes["gx_0"])
            flight[job].append(
                send(
                    source.at[1 - core, there],
                    pair_ref.at[job, there],
                    pair_send.at[job, k],
                    pair_recv.at[job, k],
                    partner,
                )
            )

    def spread(job, source):
        copies = flight[job]
        flight[job] = []
        for k, dx in enumerate(SLABS):
            there = lax.rem(me["gx_0"] + dx, sizes["gx_0"])
            copies[k].wait_recv()
            whole_ref[job, there] = source[core, there] + pair_ref[job, there]
            for offset in slab_offsets(dx):
                slot = (offset[0] * 4 + offset[1]) * 4 + offset[2] - 1
                device = chips[offset]
                flight[job].append(
                    send(
                        whole_ref.at[job, there, device[2], device[3]],
                        inbox_ref.at[job, slot],
                        chip_send.at[job, slot],
                        chip_recv.at[job, slot],
                        device,
                    )
                )

    def finish(job):
        for copy in flight[job]:
            copy.wait_recv()
        kept = whole_ref[job, me["gx_0"], me["gy_0"], me["gy_1"]]
        return kept, jnp.sum(inbox_ref[job], axis=0)

    sum_accs, take_accs, accs = accs[:2], accs[2:4], accs[4:]
    empty_accs(sum_accs + take_accs + accs)
    first_tiles(
        offset_ref,
        res_ref,
        cam_ref,
        pt_ref,
        camera_ref,
        slot_ref,
        table_ref,
        pos_ref,
        index_ref,
        feat_ref,
        point_ref,
        line_ref,
        sum_accs,
        accs,
        loads,
    )
    drain(accs, total_ref)
    regroup_into(grad_ref, total_ref)
    pl.semaphore_wait(barrier, len(far) + len(near) + len(others))
    pairs(0, grad_ref)
    point_square = solve_points(point_ref, damp_ref, step_ref)
    residual = res_ref[...]
    square = jnp.sum(residual * residual)
    lane = lax.broadcasted_iota(I32, mine_ref.shape, 1)
    refs = (
        offset_ref,
        index_ref,
        step_ref,
        pt_ref,
        res_ref,
        moved_ref,
        pos_ref,
        cam_ref,
        line_ref,
        take_accs,
        accs,
    )
    second_start(*refs)
    second_tiles(0, 8, *refs)
    spread(0, grad_ref)
    second_tiles(8, 24, *refs)
    kept, rest = finish(0)
    grads = kept + rest
    gradient_square = point_square + jnp.sum(grads * grads)
    mine_ref[...] = jnp.where(lane == 0, square, jnp.where(lane == 1, gradient_square, 0.0))
    arrivals = [
        send(mine_ref, far_ref.at[k], far_send.at[k], far_recv.at[k], device)
        for k, device in enumerate(far)
    ]
    second_tiles(24, 32, *refs)
    for copy in arrivals:
        copy.wait_recv()
    plane_ref[...] = mine_ref[...] + jnp.sum(far_ref[...], axis=0)
    arrivals = [
        send(plane_ref, near_ref.at[k], near_send.at[k], near_recv.at[k], device)
        for k, device in enumerate(near)
    ]
    drain(accs, total_ref)
    regroup_into(move_ref, total_ref)
    pairs(1, move_ref)
    spread(1, move_ref)
    for copy in arrivals:
        copy.wait_recv()
    totals = plane_ref[...] + jnp.sum(near_ref[...], axis=0)
    first_row = lax.broadcasted_iota(I32, mine_ref.shape, 0) == 0
    cost = totals / scale[0]
    norm = jnp.sqrt(totals / scale[1] + 1e-06)
    cost_ref[...] = jnp.where(lane == 0, cost, norm)
    kept_ref[...], rest_ref[...] = finish(1)
    for copy in started:
        copy.wait_send()


def whole(
    residual, cam_jacobian, point_jacobian, obs_camera, obs_slot, tile_offset, damping, camera_slot, sizes, scale
):
    vmem = pl.BlockSpec(memory_space=pltpu.VMEM)
    smem = pl.BlockSpec(memory_space=pltpu.SMEM)
    buffer = lambda *lead: pltpu.VMEM(lead + (CAM, LANES), F32)
    chips = sizes["gx_0"] * sizes["gy_0"] * sizes["gy_1"] - 1
    dma = pltpu.SemaphoreType.DMA
    far = sizes["gx_0"] * sizes["gx_1"] - 1
    near = sizes["gy_0"] * sizes["gy_1"] - 1
    return pl.pallas_call(
        scoped(functools.partial(whole_kernel, sizes, scale), acc_shapes),
        out_shape=(
            jax.ShapeDtypeStruct((CAM, LANES), F32),
            jax.ShapeDtypeStruct((CAM, LANES), F32),
            jax.ShapeDtypeStruct((8, LANES), F32),
        ),
        in_specs=[smem] + [pl.BlockSpec(memory_space=pl.ANY)] * 7,
        out_specs=(vmem, vmem, vmem),
        scratch_shapes=[
            pltpu.VMEM(residual.shape, F32),
            pltpu.VMEM(cam_jacobian.shape, F32),
            pltpu.VMEM(point_jacobian.shape, F32),
            pltpu.VMEM(obs_camera.shape, I32),
            pltpu.VMEM(obs_slot.shape, I32),
            pltpu.VMEM(damping.shape, F32),
            pltpu.VMEM(camera_slot.shape, I32),
            dma((7,)),
            pltpu.VMEM(obs_camera.shape, I32),
            pltpu.VMEM(obs_camera.shape, I32),
            pltpu.VMEM((16 * 8, LANES), F32),
            pltpu.VMEM((damping.shape[0] + 1, 16, LANES), F32),
            pltpu.VMEM((damping.shape[0] + 1, 16, LANES), F32),
            pltpu.VMEM(residual.shape, F32),
            pltpu.VMEM((2, 2, CAM, 8, LANES), F32),
            pltpu.VMEM((2, CAM * PITCH, LANES), F32),
            buffer(2, 4, 4, 4),
            buffer(2, 4, 4, 4),
            buffer(2, 4, 4, 4),
            buffer(2, 4, 4, 4),
            buffer(2, chips),
            pltpu.VMEM((8, LANES), F32),
            pltpu.VMEM((far, 8, LANES), F32),
            pltpu.VMEM((8, LANES), F32),
            pltpu.VMEM((near, 8, LANES), F32),
            dma((2, 4)),
            dma((2, 4)),
            dma((2, chips)),
            dma((2, chips)),
            dma((far,)),
            dma((far,)),
            dma((near,)),
            dma((near,)),
        ],
        compiler_params=pltpu.CompilerParams(collective_id=0, has_side_effects=True),
    )(tile_offset, residual, cam_jacobian, point_jacobian, obs_camera, obs_slot, damping, camera_slot)


def close_kernel(kept_ref, rest_ref, ends_ref, reduced_ref, cost_ref, norm_ref):
    reduced_ref[...] = kept_ref[...] + rest_ref[...]
    lane = lax.broadcasted_iota(I32, (1, LANES), 1)
    ends = ends_ref[0:1, :]
    cost_ref[0, 0] = jnp.sum(jnp.where(lane == 0, ends, 0.0))
    norm_ref[0, 0] = jnp.sum(jnp.where(lane == 1, ends, 0.0))


def close(kept, rest, ends):
    vmem = pl.BlockSpec(memory_space=pltpu.VMEM)
    smem = pl.BlockSpec(memory_space=pltpu.SMEM)
    scalar = jax.ShapeDtypeStruct((1, 1), F32)
    return pl.pallas_call(
        close_kernel,
        out_shape=(jax.ShapeDtypeStruct(kept.shape, F32), scalar, scalar),
        in_specs=[vmem] * 3,
        out_specs=(vmem, smem, smem),
    )(kept, rest, ends)


def on_device(
    residual, cam_jacobian, point_jacobian, obs_camera, obs_slot, tile_offset, damping, camera_slot
):
    n_obs = residual.shape[1]
    sizes = {name: lax.axis_size(name) for name in AXES}
    devices = lax.axis_size(AXES)
    scale = (2.0 * n_obs * devices, 9.0 * camera_slot.shape[0] + 3.0 * damping.shape[0] * devices)
    lines = lambda array: array.reshape(-1, LANES)
    res, cam, pt = row_major(residual), row_major(cam_jacobian), row_major(point_jacobian)
    kept, rest, ends = whole(
        res, cam, pt, lines(obs_camera), lines(obs_slot), tile_offset, lines(damping), lines(camera_slot), sizes, scale
    )
    reduced, cost, norm = close(kept, rest, ends)
    return (reduced, cost.reshape(()), norm.reshape(()))


def solution(mesh):
    finer = Mesh(mesh.devices.reshape(4, 2, 4, 4), AXES)
    in_specs = (
        P(None, AXES),
        P(None, None, AXES),
        P(None, None, AXES),
        P(AXES),
        P(AXES),
        P(AXES),
        P(AXES),
        P(),
    )
    out_specs = (P(None, AXES), P(), P())
    return jax.shard_map(
        on_device, mesh=finer, in_specs=in_specs, out_specs=out_specs, check_vma=False
    )
```
